128 devices in a mesh: dp: 2 (over core), ep: 64 (over x, y, z).
Axes of the slice: x: 4, y: 4, z: 4, core: 2. Of those that a mesh axis runs over, the one named last changes fastest.
Arguments:
- x: bfloat16 [2, 64, 256, 1792], P('dp', 'ep'), parts along dimension 0
- expert: int32 [2, 64, 256, 8], P('dp', 'ep'), parts along dimension 0
- slot: int32 [2, 64, 256, 8], P('dp', 'ep'), parts along dimension 0
- gate: float32 [2, 64, 256, 8], P('dp', 'ep'), parts along dimension 0
- w_gate: bfloat16 [64, 1792, 2560], P('ep')
- w_up: bfloat16 [64, 1792, 2560], P('ep')
- w_down: bfloat16 [64, 2560, 1792], P('ep')
- s_gate: bfloat16 [1792, 20480], replicated
- s_up: bfloat16 [1792, 20480], replicated
- s_down: bfloat16 [20480, 1792], replicated
Outputs:
- y: bfloat16 [2, 64, 256, 1792], P('dp', 'ep'), parts along dimension 0
There are 2 independent parts. The reference program is written for one: setup_inputs(seed, part) draws one part's arguments, and reference() takes and returns one part's arrays. A program takes and returns all parts, laid end to end along the dimension named above; an argument that names none is the same for every part.
All inputs are finite; a program needn't handle non-finite values.
Results may differ from the reference program's by a relative error of at most 0.009.
Values are sent between devices in bfloat16 or wider.
A program may use at most 1.5 GiB of HBM per device.

```python
import jax
import jax.numpy as jnp

MEMBERS = 64
TOKENS = 256
D = 1792
FF = 2560
TOP = 8
EXPERTS = 64
SHARED_FF = 20480
SLOTS = 5 * TOKENS * TOP // (4 * EXPERTS)


def setup_inputs(seed: int = 0, part: int = 0) -> dict:
    own, k1, k2, k3, k4, k5, k6 = jax.random.split(jax.random.key(seed), 7)
    kx, ke, kl, kg = jax.random.split(jax.random.fold_in(own, part), 4)
    devices = (1, MEMBERS)
    place = jax.random.permutation(kl, jnp.arange(EXPERTS, dtype=jnp.uint32))
    slow = ((EXPERTS + (9 * place) % EXPERTS) << ((9 * place) // EXPERTS)) // EXPERTS
    wait = (jax.random.bits(ke, (*devices, TOKENS, EXPERTS), jnp.uint32) >> 10) * slow
    expert = jnp.argsort(wait, axis=-1)[..., :TOP].astype(jnp.int32)
    chosen = jax.nn.one_hot(expert, EXPERTS, dtype=jnp.int32)
    in_line = jnp.cumsum(chosen.reshape(*devices, TOKENS * TOP, EXPERTS), axis=2) - 1
    slot = jnp.sum(in_line.reshape(chosen.shape) * chosen, axis=-1)

    def one(key, rows, columns):
        return (jax.random.normal(key, (rows, columns), jnp.float32) * rows**-0.5).astype(jnp.bfloat16)

    def weights(key, rows, columns):
        return jax.lax.map(lambda k: one(k, rows, columns), jax.random.split(key, EXPERTS))

    return {
        "x": jax.random.normal(kx, (*devices, TOKENS, D), jnp.float32).astype(jnp.bfloat16),
        "expert": expert,
        "slot": slot,
        "gate": jax.nn.softmax(jax.random.normal(kg, expert.shape, jnp.float32)),
        "w_gate": weights(k1, D, FF),
        "w_up": weights(k2, D, FF),
        "w_down": weights(k3, FF, D),
        "s_gate": one(k4, D, SHARED_FF),
        "s_up": one(k5, D, SHARED_FF),
        "s_down": one(k6, SHARED_FF, D),
    }


def einsum(form, a, b):
    return jnp.einsum(form, a.astype(jnp.float32), b.astype(jnp.float32))


def for_all(x, s_gate, s_up, s_down):
    h = jax.nn.silu(einsum("...d,df->...f", x, s_gate)) * einsum("...d,df->...f", x, s_up)
    return einsum("...f,fd->...d", h.astype(jnp.bfloat16), s_down)


def reference(x, expert, slot, gate, w_gate, w_up, w_down, s_gate, s_up, s_down):
    to_expert = jax.nn.one_hot(expert, EXPERTS, dtype=jnp.bfloat16)
    to_slot = jax.nn.one_hot(slot, SLOTS, dtype=jnp.bfloat16)
    weighted = to_expert * gate[..., None].astype(jnp.bfloat16)
    dispatch = einsum("abtke,abtkc->abtec", to_expert, to_slot).astype(jnp.bfloat16)
    combine = einsum("abtke,abtkc->abtec", weighted, to_slot).astype(jnp.bfloat16)
    z = einsum("abtec,abtd->aebcd", dispatch, x).astype(jnp.bfloat16)
    h = jax.nn.silu(einsum("aebcd,edf->aebcf", z, w_gate))
    h = (h * einsum("aebcd,edf->aebcf", z, w_up)).astype(jnp.bfloat16)
    out = einsum("aebcf,efd->aebcd", h, w_down).astype(jnp.bfloat16)
    y = einsum("abtec,aebcd->abtd", combine, out)
    return (y + for_all(x, s_gate, s_up, s_down)).astype(jnp.bfloat16)
```

```python
import functools

import jax
import jax.numpy as jnp
from jax import lax
from jax.experimental import pallas as pl
from jax.experimental.pallas import tpu as pltpu
from jax.sharding import PartitionSpec as P

MESH = pl.DeviceIdType.MESH
N = 4
STRIDE = (16, 4, 1)
TURNS = ((0, 1, 2), (1, 2, 0), (2, 0, 1))
SUB = 8
F32, BF16 = jnp.float32, jnp.bfloat16


def dot(a, b):
    return jnp.dot(a, b, preferred_element_type=F32)


def kernel(cfg, *refs):
    tokens, chunks, cols, ff, f_tile, d_tile, units, u_tile, top, slots = (
        cfg["tokens"], cfg["chunks"], cfg["cols"], cfg["ff"], cfg["f_tile"], cfg["d_tile"],
        cfg["units"], cfg["u_tile"], cfg["top"], cfg["slots"])
    it = iter(refs)
    take = lambda n: [next(it) for _ in range(n)]
    x_hbm, meta, wg_hbm, wu_hbm, wd_hbm, sg_hbm, su_hbm, sd_hbm = take(8)
    (y_ref,) = take(1)
    made, bl, ecl, ebl = take(3), take(3), take(3), take(3)
    xv, = take(1)
    al = take(3)
    eal = take(3)
    met, stage, wg, wu, wd, z, h, acc, sg, su, sd = take(11)
    (x_sem, w_sem, s_sem, st_sem, a_send, a_recv, m_send, m_recv, b_send, b_recv, b_self, c_send, c_recv, c_self,
     ec_send, ec_recv, ec_self, eb_send, eb_recv, ld_sem, ea_send, ea_recv) = take(22)

    me = lax.axis_index("ep")
    co = (me // 16, lax.rem(me // 4, 4), lax.rem(me, 4))
    starts = [sum(cols[:r]) for r in range(3)]
    span = [pl.ds(starts[r], cols[r]) for r in range(3)]
    d = sum(cols)

    def hop(c, s):
        return lax.rem(c + s, N)

    def peer(axis, s):
        return {"ep": me + (hop(co[axis], s) - co[axis]) * STRIDE[axis]}

    def remote(src, dst, send, recv, to):
        return pltpu.make_async_remote_copy(
            src_ref=src, dst_ref=dst, send_sem=send, recv_sem=recv, device_id=to, device_id_type=MESH)

    def at_b(ref, r, k, b):
        return ref.at[k, :, b] if TURNS[r] == (2, 0, 1) else ref.at[k, :, :, b]

    def at_c(ref, r, k, c):
        axis = TURNS[r][2]
        if axis == 0:
            return ref.at[k, c, :, :, :, span[r]]
        if axis == 1:
            return ref.at[k, :, c, :, :, span[r]]
        return ref.at[k, :, :, c, :, span[r]]

    def a_copy(r, s):
        return remote(x_hbm.at[:, span[r]], al[r].at[3 - s], a_send.at[r, 3 - s], a_recv.at[r, 3 - s], peer(TURNS[r][0], s))

    def m_copy(axis, s):
        return remote(meta, met.at[axis, 3 - s], m_send.at[axis, 3 - s], m_recv.at[axis, 3 - s], peer(axis, s))

    def stage_copy(r, k):
        return pltpu.make_async_copy(stage.at[:, :, :, :, span[r]], made[r].at[k], st_sem.at[r])

    def b_own(r, k):
        b = co[TURNS[r][1]]
        return pltpu.make_async_copy(stage.at[b, :, :, :, span[r]], at_b(bl[r], r, k, b), b_self.at[r])

    def b_copy(r, k, s):
        b = co[TURNS[r][1]]
        return remote(made[r].at[k, hop(b, s)], at_b(bl[r], r, k, b), b_send.at[r, k, s - 1], b_recv.at[r, k, s - 1], peer(TURNS[r][1], s))

    def c_own(r, k):
        c = co[TURNS[r][2]]
        return pltpu.make_async_copy(bl[r].at[k, c], at_c(z, r, k, c), c_self.at[r, k])

    def c_copy(r, k, s):
        c = co[TURNS[r][2]]
        return remote(bl[r].at[k, hop(c, s)], at_c(z, r, k, c), c_send.at[r, k, s - 1], c_recv.at[r, k, s - 1], peer(TURNS[r][2], s))

    def ec_own(r, k):
        c = co[TURNS[r][2]]
        return pltpu.make_async_copy(at_c(z, r, k, c), ecl[r].at[k, c], ec_self.at[r, k])

    def ec_copy(r, k, s):
        c = co[TURNS[r][2]]
        return remote(at_c(z, r, k, hop(c, s)), ecl[r].at[k, c], ec_send.at[r, k, s - 1], ec_recv.at[r, k, s - 1], peer(TURNS[r][2], s))

    def eb_copy(r, k, s):
        b = co[TURNS[r][1]]
        return remote(at_b(ecl[r], r, k, hop(b, s)), ebl[r].at[k, b], eb_send.at[r, k, s - 1], eb_recv.at[r, k, s - 1], peer(TURNS[r][1], s))

    def ea_copy(r, s):
        return remote(al[r].at[s - 1], eal[r].at[3 - s], ea_send.at[r, 3 - s], ea_recv.at[r, 3 - s], peer(TURNS[r][0], s))

    def load(r, k, o):
        b = co[TURNS[r][1]]
        src = at_b(ecl[r], r, k, b) if o == 0 else ebl[r].at[k, hop(b, o)]
        return pltpu.make_async_copy(src, wd.at[k, hop(b, o), :, :, :, span[r]], ld_sem.at[r, k, o])

    hops = [(r, s) for r in range(3) for s in (1, 3, 2)]

    def s_copies(u):
        i = lax.rem(u, 2)
        w = pl.ds(pl.multiple_of(u * u_tile, u_tile), u_tile)
        return [pltpu.make_async_copy(sg_hbm.at[:, w], sg.at[i], s_sem.at[i, 0]),
                pltpu.make_async_copy(su_hbm.at[:, w], su.at[i], s_sem.at[i, 1]),
                pltpu.make_async_copy(sd_hbm.at[w, :], sd.at[i], s_sem.at[i, 2])]

    def shared(lo, hi):
        def unit(u, _):
            @pl.when(u + 1 < units)
            def _():
                for c in s_copies(u + 1):
                    c.start()
            for c in s_copies(u):
                c.wait()
            i = lax.rem(u, 2)
            g = dot(xv[...], sg[i])
            act = (jax.nn.silu(g) * dot(xv[...], su[i])).astype(BF16)
            acc[...] += dot(act, sd[i])
            return 0
        lax.fori_loop(lo, hi, unit, 0)

    def matches(r, o, first, count, weight):
        a_axis, b_axis, c_axis = TURNS[r]
        m = meta if o == 0 else met.at[a_axis, o - 1]
        i = lax.broadcasted_iota(jnp.int32, (count, tokens), 0)
        expert = co[a_axis] * STRIDE[a_axis] + ((i // 32) % 4) * STRIDE[b_axis] + ((i // 8) % 4) * STRIDE[c_axis]
        code = (expert * slots + (i // 128 + first) * SUB + i % 8).astype(F32)
        out = jnp.zeros((count, tokens), F32)
        for j in range(top):
            out = jnp.where(m[j : j + 1, :] == code, m[top + j : top + j + 1, :] if weight else 1.0, out)
        return out.astype(BF16)

    def gather(k):
        for r in range(3):
            for o in range(4):
                src = xv[:, span[r]] if o == 0 else al[r][o - 1]
                rows = dot(matches(r, o, k, 128, False), src).astype(BF16)
                stage[:, :, hop(co[TURNS[r][0]], o), :, span[r]] = rows.reshape(4, 4, SUB, cols[r])

    def forward_c(k):
        for r in range(3):
            for s in (1, 2, 3):
                b_copy(r, k, s).wait_recv()
        for r, s in hops:
            c_copy(r, k, s).start()
        for r in range(3):
            c_own(r, k).start()

    def forward_eb(k):
        for r in range(3):
            for s in (1, 2, 3):
                ec_copy(r, k, s).wait_recv()
            ec_own(r, k).wait()
        for r, s in hops:
            eb_copy(r, k, s).start()

    def weights():
        return [pltpu.make_async_copy(wg_hbm, wg, w_sem.at[0]), pltpu.make_async_copy(wu_hbm, wu, w_sem.at[1]),
                pltpu.make_async_copy(wd_hbm, wd, w_sem.at[2])]

    rows = N * N * N * SUB

    def expert(k):
        for r in range(3):
            for s in (1, 2, 3):
                c_copy(r, k, s).wait_recv()
            c_own(r, k).wait()

        def up(f, _):
            w = pl.ds(pl.multiple_of(f * f_tile, f_tile), f_tile)
            zk = z[k].reshape(rows, d)
            h[:, w] = (jax.nn.silu(dot(zk, wg[:, w])) * dot(zk, wu[:, w])).astype(BF16)
            return 0
        lax.fori_loop(0, ff // f_tile, up, 0)

        @pl.when(k >= 1)
        def _():
            forward_eb(k - 1)

        def down(n, _):
            w = pl.ds(pl.multiple_of(n * d_tile, d_tile), d_tile)
            out = dot(h[...], wd[:, :, :, :, :, w].reshape(ff, d_tile))
            z[k, :, :, :, :, w] = out.astype(BF16).reshape(N, N, N, SUB, d_tile)
            return 0
        lax.fori_loop(0, d // d_tile, down, 0)
        for r, s in hops:
            ec_copy(r, k, s).start()
        for r in range(3):
            ec_own(r, k).start()

    for c in s_copies(0):
        c.start()
    x_in = pltpu.make_async_copy(x_hbm, xv, x_sem)
    x_in.start()
    barrier = pltpu.get_barrier_semaphore()
    for axis in range(3):
        for s in (1, 2, 3):
            pl.semaphore_signal(barrier, inc=1, device_id=peer(axis, s), device_id_type=MESH)
    pl.semaphore_wait(barrier, 9)
    for axis in range(3):
        for s in (1, 3, 2):
            m_copy(axis, s).start()
    for r, s in hops:
        a_copy(r, s).start()
    acc[...] = jnp.zeros_like(acc)
    for c in weights():
        c.start()
    x_in.wait()
    plan = cfg["plan"]
    shared(0, plan[0])
    for axis in range(3):
        for s in (1, 2, 3):
            m_copy(axis, s).wait_recv()
    for r, s in hops:
        a_copy(r, s).wait_recv()

    def dispatch(k, _):
        gather(k)
        for r in range(3):
            stage_copy(r, k).start()
            b_own(r, k).start()
        for r in range(3):
            stage_copy(r, k).wait()
            b_own(r, k).wait()
        for r, s in hops:
            b_copy(r, k, s).start()
        return 0
    early = min(3, chunks)
    lax.fori_loop(0, early, dispatch, 0)

    def later(k, _):
        forward_c(k)
        @pl.when(k + early < chunks)
        def _():
            dispatch(k + early, 0)
        shared(plan[0] + k * plan[1], plan[0] + (k + 1) * plan[1])
        return 0
    lax.fori_loop(0, chunks, later, 0)
    for c in weights():
        c.wait()
    lax.fori_loop(0, chunks, lambda k, _: (expert(k), 0)[1], 0)
    done = plan[0] + chunks * plan[1]
    shared(done, done + plan[2])
    for k in range(chunks - 1):
        for r in range(3):
            for s in (1, 2, 3):
                eb_copy(r, k, s).wait_recv()
            for o in range(4):
                load(r, k, o).start()
    forward_eb(chunks - 1)
    shared(done + plan[2], units)
    for k in range(chunks - 1, chunks):
        for r in range(3):
            for s in (1, 2, 3):
                eb_copy(r, k, s).wait_recv()
            for o in range(4):
                load(r, k, o).start()
    for r in range(3):
        for k in range(chunks):
            for o in range(4):
                load(r, k, o).wait()
    for o in (2, 1, 3, 0):
        for r in range(3):
            src = wd[:, :, :, hop(co[TURNS[r][0]], o), :, span[r]]
            part = lax.dot_general(
                matches(r, o, 0, 128 * chunks, True), src.reshape(128 * chunks, cols[r]),
                (((0,), (0,)), ((), ())), preferred_element_type=F32)
            if o == 0:
                acc[:, span[r]] += part
            else:
                al[r][o - 1] = part.astype(BF16)
                ea_copy(r, o).start()
    for r, s in hops:
        ea_copy(r, s).wait_recv()
    for r in range(3):
        total = acc[:, span[r]]
        for o in range(3):
            total += eal[r][o].astype(F32)
        y_ref[:, span[r]] = total.astype(BF16)

    for axis in range(3):
        for s in (1, 2, 3):
            m_copy(axis, s).wait_send()
    for r, s in hops:
        a_copy(r, s).wait_send()
        ea_copy(r, s).wait_send()

    def drain(k, _):
        for r, s in hops:
            b_copy(r, k, s).wait_send()
            c_copy(r, k, s).wait_send()
            ec_copy(r, k, s).wait_send()
            eb_copy(r, k, s).wait_send()
        return 0
    lax.fori_loop(0, chunks, drain, 0)


def layer(x, meta, w_gate, w_up, w_down, s_gate, s_up, s_down, cfg):
    tokens, chunks, cols, ff, units, u_tile = (cfg[n] for n in ("tokens", "chunks", "cols", "ff", "units", "u_tile"))
    d, rows = sum(cols), N * N * N * SUB
    any_ = pl.BlockSpec(memory_space=pl.ANY)
    vm = pl.BlockSpec(memory_space=pltpu.VMEM)
    block = lambda w: jax.ShapeDtypeStruct((chunks, N, N, N, SUB, w), BF16)
    dma = pltpu.SemaphoreType.DMA
    phase = [dma((3, chunks, 3)), dma((3, chunks, 3))]
    outs = pl.pallas_call(
        functools.partial(kernel, cfg),
        out_shape=[jax.ShapeDtypeStruct((tokens, d), BF16)] + [block(w) for _ in range(4) for w in cols],
        in_specs=[any_, vm] + [any_] * 6,
        out_specs=[vm] + [any_] * 12,
        scratch_shapes=[
            pltpu.VMEM((tokens, d), BF16),
            *[pltpu.VMEM((3, tokens, w), BF16) for w in cols],
            *[pltpu.VMEM((3, tokens, w), BF16) for w in cols],
            pltpu.VMEM((3, 3, *meta.shape), F32),
            pltpu.VMEM((N, N, N, SUB, d), BF16),
            pltpu.VMEM((d, ff), BF16),
            pltpu.VMEM((d, ff), BF16),
            pltpu.VMEM((chunks, N, N, N, SUB, d), BF16),
            pltpu.VMEM((chunks, N, N, N, SUB, d), BF16),
            pltpu.VMEM((rows, ff), BF16),
            pltpu.VMEM((tokens, d), F32),
            pltpu.VMEM((2, d, u_tile), BF16),
            pltpu.VMEM((2, d, u_tile), BF16),
            pltpu.VMEM((2, u_tile, d), BF16),
            dma(()), dma((3,)), dma((2, 3)), dma((3,)),
            dma((3, 3)), dma((3, 3)), dma((3, 3)), dma((3, 3)),
            *phase, dma((3,)),
            *phase, dma((3, chunks)),
            *phase, dma((3, chunks)),
            *phase, dma((3, chunks, 4)),
            dma((3, 3)), dma((3, 3)),
        ],
        compiler_params=pltpu.CompilerParams(collective_id=0, has_side_effects=True, vmem_limit_bytes=cfg["vmem"]),
        name="moe_layer",
    )(x, meta, w_gate, w_up, w_down.reshape(chunks, N, N, N, SUB, d), s_gate, s_up, s_down)
    return outs[0]


def configure(x, expert, w_gate, s_gate):
    tokens, d = x.shape[-2:]
    top, ff, width, experts = expert.shape[-1], w_gate.shape[-1], s_gate.shape[-1], N * N * N
    slots = 5 * tokens * top // (4 * experts)
    lanes = d // 128
    cols = tuple(128 * ((lanes + 2 - r) // 3) for r in range(3))
    return dict(tokens=tokens, top=top, slots=slots, chunks=slots // SUB, cols=cols, ff=ff, f_tile=512, d_tile=256,
                units=width // 512, u_tile=512, plan=(6, 3, 8), vmem=67043328)


def solution(mesh):
    def step(x, expert, slot, gate, w_gate, w_up, w_down, s_gate, s_up, s_down):
        cfg = configure(x, expert, w_gate, s_gate)
        kept = slot[0, 0] < cfg["slots"]
        code = jnp.where(kept, expert[0, 0] * cfg["slots"] + slot[0, 0], -1).astype(F32)
        weight = gate[0, 0].astype(BF16).astype(F32)
        meta = jnp.concatenate([code.T, weight.T])
        y = layer(x[0, 0], meta, w_gate[0], w_up[0], w_down[0], s_gate, s_up, s_down, cfg)
        return y[None, None]

    tok, own, whole = P("dp", "ep", None, None), P("ep", None, None), P(None, None)
    return jax.shard_map(step, mesh=mesh, in_specs=(tok,) * 4 + (own,) * 3 + (whole,) * 3, out_specs=tok, check_vma=False)
```

```python
import functools

import jax
import jax.numpy as jnp
from jax import lax
from jax.experimental import pallas as pl
from jax.experimental.pallas import tpu as pltpu
from jax.sharding import PartitionSpec as P

MESH = pl.DeviceIdType.MESH
N = 4
STRIDE = (16, 4, 1)
TURNS = ((0, 1, 2), (1, 2, 0), (2, 0, 1))
SUB = 8
ORDER = (2, 1, 3, 0)
HOPS = tuple((r, s) for s in (1, 3, 2) for r in range(3))
F32, BF16 = jnp.float32, jnp.bfloat16


def dot(a, b):
    return jnp.dot(a, b, preferred_element_type=F32)


def any_of(i, places):
    hit = i == places[0]
    for p in places[1:]:
        hit = hit | (i == p)
    return hit


def before(i, places):
    return sum((i > p).astype(jnp.int32) for p in places)


def kernel(cfg, *refs):
    tokens, chunks, cols, ff, f_tile, units, u_tile, top, slots, plan = (
        cfg[n] for n in ("tokens", "chunks", "cols", "ff", "f_tile", "units", "u_tile", "top", "slots", "plan"))
    it = iter(refs)
    take = lambda n: [next(it) for _ in range(n)]
    x_hbm, expert_ref, slot_ref, gate_ref, wg_hbm, wu_hbm, wd_hbm, sg_hbm, su_hbm, sd_hbm = take(10)
    sum_hbm, eal = take(2)
    made, bl, ecl, ebl = take(3), take(3), take(3), take(3)
    (xv,) = take(1)
    al = take(3)
    met, stage, wg, wu, wd, z, h, acc, sg, su, sd, act = take(12)
    (x_sem, w_sem, s_sem, st_sem, out_sem, a_send, a_recv, m_send, m_recv, b0_send, b0_recv, b_send, b_recv, b_self,
     c_send, c_recv, c_self, ec_send, ec_recv, ec_self, ecx_send, ecx_recv, ecx_self, eb_send, eb_recv,
     ebx_send, ebx_recv, ebx_self, ld_sem, ea_send, ea_recv) = take(31)

    me = lax.axis_index("ep")
    co = (me // 16, lax.rem(me // 4, 4), lax.rem(me, 4))
    starts = [sum(cols[:r]) for r in range(3)]
    span = [pl.ds(starts[r], cols[r]) for r in range(3)]
    d, last = sum(cols), chunks - 1
    a_axis, b_axis, c_axis = ([t[i] for t in TURNS] for i in range(3))

    def hop(c, s):
        return lax.rem(c + s, N)

    def peer(axis, s):
        return {"ep": me + (hop(co[axis], s) - co[axis]) * STRIDE[axis]}

    def remote(src, dst, send, recv, to):
        return pltpu.make_async_remote_copy(
            src_ref=src, dst_ref=dst, send_sem=send, recv_sem=recv, device_id=to, device_id_type=MESH)

    def ab(ref, r, k, a, b):
        return ref.at[k, b, a] if a_axis[r] > b_axis[r] else ref.at[k, a, b]

    def at_c(ref, r, k, c):
        if c_axis[r] == 0:
            return ref.at[k, c, :, :, :, span[r]]
        if c_axis[r] == 1:
            return ref.at[k, :, c, :, :, span[r]]
        return ref.at[k, :, :, c, :, span[r]]

    def at_ca(ref, r, k, c, a):
        ix = {c_axis[r]: c, a_axis[r]: a, b_axis[r]: slice(None)}
        return ref.at[k, ix[0], ix[1], ix[2], :, span[r]]

    every, others = slice(None), pl.ds(1, 3)

    def a_copy(r, s):
        return remote(x_hbm.at[:, span[r]], al[r].at[3 - s], a_send.at[r, 3 - s], a_recv.at[r, 3 - s], peer(a_axis[r], s))

    def m_copy(axis, s):
        return remote(met.at[axis, 0], met.at[axis, N - s], m_send.at[axis, 3 - s], m_recv.at[axis, 3 - s], peer(axis, s))

    def early_copies(r):
        return [pltpu.make_async_copy(stage.at[pl.ds(0, chunks), :, :, :, span[r]], made[r].at[:, 0], st_sem.at[r, 0]),
                pltpu.make_async_copy(stage.at[pl.ds(0, chunks), 0, :, :, span[r]], ab(bl[r], r, every, 0, 0), st_sem.at[r, 1])]

    def b0_copy(r, s):
        return remote(made[r].at[:, 0, s], ab(bl[r], r, every, 0, N - s), b0_send.at[r, s - 1], b0_recv.at[r, s - 1], peer(b_axis[r], s))

    def stage_copies(r, k):
        return [pltpu.make_async_copy(stage.at[others, :, :, :, span[r]], made[r].at[k, others], st_sem.at[r, 0]),
                pltpu.make_async_copy(stage.at[others, 0, :, :, span[r]], ab(bl[r], r, k, others, 0), st_sem.at[r, 1])]

    def b_copy(r, k, s):
        return remote(made[r].at[k, others, s], ab(bl[r], r, k, others, N - s), b_send.at[r, k, s - 1], b_recv.at[r, k, s - 1],
                      peer(b_axis[r], s))

    def c_own(r, k):
        return pltpu.make_async_copy(bl[r].at[k, :, :, 0], at_c(z, r, k, 0), c_self.at[r, k])

    def c_copy(r, k, s):
        return remote(bl[r].at[k, :, :, s], at_c(z, r, k, N - s), c_send.at[r, k, s - 1], c_recv.at[r, k, s - 1], peer(c_axis[r], s))

    def ec_own(r, k):
        return pltpu.make_async_copy(at_c(z, r, k, 0), ecl[r].at[k, :, :, 0], ec_self.at[r, k])

    def ec_copy(r, k, s):
        return remote(at_c(z, r, k, s), ecl[r].at[k, :, :, N - s], ec_send.at[r, k, s - 1], ec_recv.at[r, k, s - 1], peer(c_axis[r], s))

    def ecx_own(r, o):
        return pltpu.make_async_copy(at_ca(z, r, last, 0, o), ab(ecl[r], r, last, o, every).at[:, 0], ecx_self.at[r, o])

    def ecx_copy(r, o, s):
        return remote(at_ca(z, r, last, s, o), ab(ecl[r], r, last, o, every).at[:, N - s], ecx_send.at[r, o, s - 1],
                      ecx_recv.at[r, o, s - 1], peer(c_axis[r], s))

    def eb_copy(r, k, s):
        return remote(ab(ecl[r], r, k, every, s), ebl[r].at[k, :, N - s], eb_send.at[r, k, s - 1], eb_recv.at[r, k, s - 1],
                      peer(b_axis[r], s))

    def ebx_own(r, o):
        return pltpu.make_async_copy(ab(ecl[r], r, last, o, 0), stage.at[o, 0, :, :, span[r]], ebx_self.at[r, o])

    def ebx_copy(r, o, s):
        return remote(ab(ecl[r], r, last, o, s), stage.at[o, N - s, :, :, span[r]], ebx_send.at[r, o, s - 1], ebx_recv.at[r, o, s - 1],
                      peer(b_axis[r], s))

    def ea_copy(r, o):
        return remote(al[r].at[o - 1], eal.at[3 - o, :, span[r]], ea_send.at[r, 3 - o], ea_recv.at[r, 3 - o], peer(a_axis[r], o))

    def load(r, k, b):
        src = ab(ecl[r], r, k, every, 0) if b == 0 else ebl[r].at[k, :, b]
        return pltpu.make_async_copy(src, wd.at[k, :, b, :, :, span[r]], ld_sem.at[r, k, b])

    def up_copies(u):
        i, w = lax.rem(u, 2), pl.ds(pl.multiple_of(u * u_tile, u_tile), u_tile)
        return [pltpu.make_async_copy(sg_hbm.at[:, w], sg.at[i], s_sem.at[i, 0]),
                pltpu.make_async_copy(su_hbm.at[:, w], su.at[i], s_sem.at[i, 1])]

    def down_copy(u):
        i, w = lax.rem(u, 2), pl.ds(pl.multiple_of(u * u_tile, u_tile), u_tile)
        return pltpu.make_async_copy(sd_hbm.at[w, :], sd.at[i], s_sem.at[i, 2])

    def shared(u):
        @pl.when(u + 1 < units)
        def _():
            for c in up_copies(u + 1):
                c.start()
        down_copy(u).start()
        for c in up_copies(u):
            c.wait()
        @pl.when(u > 0)
        def _():
            down_copy(u - 1).wait()
        i, j = lax.rem(u, 2), lax.rem(u + 1, 2)
        g = dot(xv[...], sg[i])
        up = dot(xv[...], su[i])
        acc[...] += dot(act[j], sd[j])
        act[i] = (jax.nn.silu(g) * up).astype(BF16)

    def matches(r, o, first, count, weight):
        wide = min(tokens, 128)
        i = lax.broadcasted_iota(jnp.int32, (128, wide), 0)
        b, c = (co[b_axis[r]] + (i >> 5)) & 3, (co[c_axis[r]] + (i >> 3)) & 3
        expert = co[a_axis[r]] * STRIDE[a_axis[r]] + b * STRIDE[b_axis[r]] + c * STRIDE[c_axis[r]]
        base = (expert * slots + first * SUB + (i & 7)).astype(F32)
        m = met.at[a_axis[r], o]
        out = []
        for k in range(count):
            code, line = base + float(k * SUB), []
            for t in range(0, tokens, wide):
                hit = jnp.zeros((128, wide), F32)
                for j in range(top):
                    new = m[top + j : top + j + 1, t : t + wide] if weight else 1.0
                    hit = jnp.where(m[j : j + 1, t : t + wide] == code, new, hit)
                line.append(hit.astype(BF16))
            out.append(jnp.concatenate(line, axis=1))
        return jnp.concatenate(out)

    def dispatch(k):
        for r in range(3):
            for o in (1, 3, 2):
                rows = dot(matches(r, o, k, 1, False), al[r][o - 1]).astype(BF16)
                stage[o, :, :, :, span[r]] = rows.reshape(N, N, SUB, cols[r])
        for r in range(3):
            for c in stage_copies(r, k):
                c.start()
        for r in range(3):
            for c in stage_copies(r, k):
                c.wait()
        for r, s in HOPS:
            b_copy(r, k, s).start()

    def forward_c(k):
        for r in range(3):
            for s in (1, 2, 3):
                b_copy(r, k, s).wait_recv()
        for r, s in HOPS:
            c_copy(r, k, s).start()
        for r in range(3):
            c_own(r, k).start()

    def forward_eb(k):
        for r in range(3):
            for s in (1, 2, 3):
                ec_copy(r, k, s).wait_recv()
            ec_own(r, k).wait()
        for r, s in HOPS:
            eb_copy(r, k, s).start()

    def forward_ebx(o):
        for r in range(3):
            for s in (1, 2, 3):
                ecx_copy(r, o, s).wait_recv()
            ecx_own(r, o).wait()
        for r, s in HOPS:
            ebx_copy(r, o, s).start()
        for r in range(3):
            ebx_own(r, o).start()

    rows = N * N * N * SUB

    def expert(k):
        for r in range(3):
            for s in (1, 2, 3):
                c_copy(r, k, s).wait_recv()
            c_own(r, k).wait()

        def up(f, _):
            for (ek, ef), event, arg in plan["main"]:
                pl.when((k == ek) & (f == ef))(functools.partial({"C": forward_c, "F": forward_eb}[event], arg))
            w = pl.ds(pl.multiple_of(f * f_tile, f_tile), f_tile)
            zk = z[k].reshape(rows, d)
            h[:, w] = (jax.nn.silu(dot(zk, wg[:, w])) * dot(zk, wu[:, w])).astype(BF16)
            return 0
        lax.fori_loop(0, ff // f_tile, up, 0)

        at = 0
        for r in range(3):
            w = pl.ds(at, cfg["down"][r])
            at += cfg["down"][r]
            out = dot(h[...], wd[:, :, :, :, :, w].reshape(ff, cfg["down"][r]))
            z[k, :, :, :, :, w] = out.astype(BF16).reshape(N, N, N, SUB, cfg["down"][r])

            @pl.when(k < last)
            def _():
                for s in (1, 3, 2):
                    ec_copy(r, k, s).start()
                ec_own(r, k).start()

            @pl.when(k == last)
            def _():
                for o in ORDER:
                    for s in (1, 3, 2):
                        ecx_copy(r, o, s).start()
                    ecx_own(r, o).start()

    def held(r, o):
        return (pl.ds(pl.multiple_of(lax.rem(o, 2) * (128 * chunks), 128), 128 * chunks),
                pl.ds(pl.multiple_of((2 * r + o // 2) * tokens, 128 if tokens % 128 == 0 else tokens), tokens))

    def weigh(i):
        o = ordered(i)
        for r in range(3):
            wg[held(r, o)] = matches(r, o, 0, chunks, True)

    def ordered(i):
        return jnp.where(i == 0, ORDER[0], jnp.where(i == 1, ORDER[1], jnp.where(i == 2, ORDER[2], ORDER[3])))

    def combine(i, _):
        o = ordered(i)
        for r in range(3):
            for s in (1, 2, 3):
                ebx_copy(r, o, s).wait_recv()
            ebx_own(r, o).wait()
        for r in range(3):
            weight = wg[held(r, o)]
            early = wd[0:last, pl.ds(o, 1), :, :, :, span[r]].reshape(128 * last, cols[r])
            late = stage[pl.ds(o, 1), :, :, :, span[r]].reshape(128, cols[r])
            across = (((0,), (0,)), ((), ()))
            part = lax.dot_general(weight[: 128 * last], early, across, preferred_element_type=F32)
            part += lax.dot_general(weight[128 * last :], late, across, preferred_element_type=F32)

            @pl.when(o == 0)
            def _():
                acc[:, span[r]] += part

            @pl.when(o > 0)
            def _():
                al[r][pl.ds(o - 1, 1)] = part.astype(BF16)[None]
                ea_copy(r, o).start()
        return 0

    x_in = pltpu.make_async_copy(x_hbm, xv, x_sem)
    x_in.start()
    for c in up_copies(0):
        c.start()
    code = jnp.where(slot_ref[...] < slots, expert_ref[...] * slots + slot_ref[...], -1).astype(F32)
    for axis in range(3):
        met[axis, 0, :top] = code
        met[axis, 0, top:] = gate_ref[...]
    barrier = pltpu.get_barrier_semaphore()
    for axis in range(3):
        for s in (1, 2, 3):
            pl.semaphore_signal(barrier, inc=1, device_id=peer(axis, s), device_id_type=MESH)
    acc[...] = jnp.zeros_like(acc)
    act[...] = jnp.zeros_like(act)
    sd[1] = jnp.zeros_like(sd[1])
    pl.semaphore_wait(barrier, 9)
    for s in (1, 3, 2):
        for axis in range(3):
            m_copy(axis, s).start()
        for r in range(3):
            a_copy(r, s).start()
    x_in.wait()
    for r in range(3):
        mine = dot(matches(r, 0, 0, chunks, False), xv[:, span[r]]).astype(BF16)
        stage[0:chunks, :, :, :, span[r]] = mine.reshape(chunks, N, N, SUB, cols[r])
    for r in range(3):
        for c in early_copies(r):
            c.start()
    for r in range(3):
        for c in early_copies(r):
            c.wait()
    for r, s in HOPS:
        b0_copy(r, s).start()

    def weight_copy(which, k):
        if which == 2:
            return pltpu.make_async_copy(wd_hbm.at[k], wd.at[k], w_sem.at[2, k])
        w = pl.ds(pl.multiple_of(k * (d // 4), d // 4), d // 4)
        return pltpu.make_async_copy((wg_hbm, wu_hbm)[which].at[w], (wg, wu)[which].at[w], w_sem.at[which, k])

    pieces = (4, 4, chunks)
    if plan["weights"] < 0:
        for which in range(3):
            for k in range(pieces[which]):
                weight_copy(which, k).start()

    def pre(i, _):
        first, gathers, forwards = plan["weights"], plan["gather"], plan["forward"]
        if first >= 0:
            for which in range(3):
                at = first + sum(pieces[:which])

                @pl.when((i >= at) & (i < at + pieces[which]))
                def _():
                    weight_copy(which, i - at).start()

        @pl.when(i == gathers[0])
        def _():
            for axis in range(3):
                for s in (1, 2, 3):
                    m_copy(axis, s).wait_recv()
            for r, s in HOPS:
                a_copy(r, s).wait_recv()

        @pl.when(i == forwards[0])
        def _():
            for r, s in HOPS:
                b0_copy(r, s).wait_recv()

        @pl.when(any_of(i, forwards))
        def _():
            forward_c(before(i, forwards))

        @pl.when(any_of(i, gathers))
        def _():
            dispatch(before(i, gathers))

        shared(i)
        return 0
    lax.fori_loop(0, plan["pre"], pre, 0)
    for which in range(3):
        for k in range(pieces[which]):
            weight_copy(which, k).wait()
    lax.fori_loop(0, chunks, lambda k, _: (expert(k), 0)[1], 0)

    def fetch(ks):
        for k in ks:
            for r in range(3):
                for s in (1, 2, 3):
                    eb_copy(r, k, s).wait_recv()
                for b in range(4):
                    load(r, k, b).start()

    def tail(i, _):
        @pl.when(i < 4)
        def _():
            weigh(i)

        @pl.when(i == plan["eb"])
        def _():
            forward_eb(last - 1)

        @pl.when(i == plan["fetch"])
        def _():
            fetch(range(last - 1))

        for p, o in zip(plan["ebx"], ORDER, strict=True):
            pl.when(i == p)(functools.partial(forward_ebx, o))

        @pl.when(i == plan["sums"])
        def _():
            fetch([last - 1])
            for k in range(last):
                for r in range(3):
                    for b in range(4):
                        load(r, k, b).wait()
            lax.fori_loop(0, 4, combine, 0)

        shared(i + plan["pre"])
        return 0
    lax.fori_loop(0, units - plan["pre"], tail, 0)
    down_copy(units - 1).wait()
    acc[...] += dot(act[(units - 1) % 2], sd[(units - 1) % 2])
    out = pltpu.make_async_copy(acc, sum_hbm, out_sem)
    out.start()
    for r, s in HOPS:
        ea_copy(r, s).wait_recv()

    for axis in range(3):
        for s in (1, 2, 3):
            m_copy(axis, s).wait_send()
    for r, s in HOPS:
        a_copy(r, s).wait_send()
        b0_copy(r, s).wait_send()
        ea_copy(r, s).wait_send()
        for o in range(4):
            ecx_copy(r, o, s).wait_send()
            ebx_copy(r, o, s).wait_send()

    def drain(k, _):
        for r, s in HOPS:
            b_copy(r, k, s).wait_send()
            c_copy(r, k, s).wait_send()
            @pl.when(k < last)
            def _():
                ec_copy(r, k, s).wait_send()
                eb_copy(r, k, s).wait_send()
        return 0
    lax.fori_loop(0, chunks, drain, 0)
    out.wait()


def layer(x, expert, slot, gate, w_gate, w_up, w_down, s_gate, s_up, s_down, cfg):
    tokens, chunks, cols, ff, u_tile, top = (cfg[n] for n in ("tokens", "chunks", "cols", "ff", "u_tile", "top"))
    d, rows = sum(cols), N * N * N * SUB
    hbm, vm = pl.BlockSpec(memory_space=pl.ANY), pl.BlockSpec(memory_space=pltpu.VMEM)
    block = lambda w: jax.ShapeDtypeStruct((chunks, N, N, N, SUB, w), BF16)
    dma = pltpu.SemaphoreType.DMA
    phase, single, quarter = [dma((3, chunks, 3))] * 2, [dma((3, 3))] * 2, [dma((3, 4, 3))] * 2
    outs = pl.pallas_call(
        functools.partial(kernel, cfg),
        out_shape=[jax.ShapeDtypeStruct((tokens, d), F32), jax.ShapeDtypeStruct((3, tokens, d), BF16)]
        + [block(w) for _ in range(4) for w in cols],
        in_specs=[hbm] + [vm] * 3 + [hbm] * 6,
        out_specs=[hbm] * 14,
        scratch_shapes=[
            pltpu.VMEM((tokens, d), BF16),
            *[pltpu.VMEM((3, tokens, w), BF16) for w in cols],
            pltpu.VMEM((3, 4, 2 * top, tokens), F32),
            pltpu.VMEM((max(chunks, 4), N, N, SUB, d), BF16),
            pltpu.VMEM((d, ff), BF16),
            pltpu.VMEM((d, ff), BF16),
            pltpu.VMEM((chunks, N, N, N, SUB, d), BF16),
            pltpu.VMEM((chunks, N, N, N, SUB, d), BF16),
            pltpu.VMEM((rows, ff), BF16),
            pltpu.VMEM((tokens, d), F32),
            pltpu.VMEM((2, d, u_tile), BF16),
            pltpu.VMEM((2, d, u_tile), BF16),
            pltpu.VMEM((2, u_tile, d), BF16),
            pltpu.VMEM((2, tokens, u_tile), BF16),
            dma(()), dma((3, max(chunks, 4))), dma((2, 3)), dma((3, 2)), dma(()),
            *single, *single, *single,
            *phase, dma((3, chunks)),
            *phase, dma((3, chunks)),
            *phase, dma((3, chunks)),
            *quarter, dma((3, 4)),
            *phase,
            *quarter, dma((3, 4)),
            dma((3, chunks, 4)), *single,
        ],
        compiler_params=pltpu.CompilerParams(collective_id=0, has_side_effects=True, vmem_limit_bytes=cfg["vmem"]),
        name="moe_layer",
    )(x, expert, slot, gate, w_gate, w_up, w_down.reshape(chunks, N, N, N, SUB, d), s_gate, s_up, s_down)
    total, sums = outs[:2]
    for o in range(3):
        total += sums[o].astype(F32)
    return total.astype(BF16)


PLAN = {
    "pre": 18, "weights": 1, "gather": (8, 9, 10, 13, 15), "forward": (13, 15, 16),
    "main": (((0, 3), "C", 3), ((1, 1), "C", 4), ((2, 3), "F", 0), ((3, 3), "F", 1), ((4, 2), "F", 2)),
    "fetch": 1, "eb": 2, "ebx": (7, 8, 9, 10), "sums": 14,
}


def configure(x, expert, w_gate, s_gate):
    tokens, d = x.shape[-2:]
    top, ff, width, experts = expert.shape[-1], w_gate.shape[-1], s_gate.shape[-1], N * N * N
    slots = 5 * tokens * top // (4 * experts)
    lanes = d // 128
    cols = tuple(128 * ((lanes + 2 - r) // 3) for r in range(3))
    return dict(tokens=tokens, top=top, slots=slots, chunks=slots // SUB, cols=cols, ff=ff, f_tile=512, down=(768, 512, 512),
                units=width // 512, u_tile=512, plan=PLAN, vmem=67043328)


TEST = dict(
    cols=(256, 256, 128), down=(256, 256, 128),
    plan={"pre": 2, "weights": -9, "gather": (0, 1), "forward": (1,), "main": (((0, 1), "C", 1),),
          "fetch": 0, "eb": 0, "ebx": (1, 2, 3, 3), "sums": 4})


def solution(mesh):
    def step(x, expert, slot, gate, w_gate, w_up, w_down, s_gate, s_up, s_down):
        cfg = configure(x, expert, w_gate, s_gate)
        y = layer(x[0, 0], expert[0, 0].T, slot[0, 0].T, gate[0, 0].T, w_gate[0], w_up[0], w_down[0], s_gate, s_up, s_down, cfg)
        return y[None, None]

    tok, own, whole = P("dp", "ep", None, None), P("ep", None, None), P(None, None)
    return jax.shard_map(step, mesh=mesh, in_specs=(tok,) * 4 + (own,) * 3 + (whole,) * 3, out_specs=tok, check_vma=False)
```

```python
import functools

import jax
import jax.numpy as jnp
from jax import lax
from jax.experimental import pallas as pl
from jax.experimental.pallas import tpu as pltpu
from jax.sharding import PartitionSpec as P

MESH = pl.DeviceIdType.MESH
N = 4
STRIDE = (16, 4, 1)
TURNS = ((0, 1, 2), (1, 2, 0), (2, 0, 1))
SUB = 8
ORDER = (2, 1, 3, 0)
HOPS = tuple((r, s) for s in (1, 3, 2) for r in range(3))
F32, BF16 = jnp.float32, jnp.bfloat16


def dot(a, b):
    return jnp.dot(a, b, preferred_element_type=F32)


def any_of(i, places):
    hit = i == places[0]
    for p in places[1:]:
        hit = hit | (i == p)
    return hit


def before(i, places):
    return sum((i > p).astype(jnp.int32) for p in places)


def kernel(cfg, *refs):
    tokens, chunks, cols, ff, f_tile, units, u_tile, top, slots, plan = (
        cfg[n] for n in ("tokens", "chunks", "cols", "ff", "f_tile", "units", "u_tile", "top", "slots", "plan"))
    it = iter(refs)
    take = lambda n: [next(it) for _ in range(n)]
    x_hbm, expert_ref, slot_ref, gate_ref, wg_hbm, wu_hbm, wd_hbm, sg_hbm, su_hbm, sd_hbm = take(10)
    sum_hbm, eal = take(2)
    made, bl, ecl, ebl = take(3), take(3), take(3), take(3)
    (xv,) = take(1)
    al = take(3)
    met, stage, wg, wu, wd, z, h, acc, sg, su, sd, act = take(12)
    (x_sem, w_sem, s_sem, st_sem, out_sem, a_send, a_recv, m_send, m_recv, b0_send, b0_recv, b_send, b_recv, b_self,
     c_send, c_recv, c_self, ec_send, ec_recv, ec_self, ecx_send, ecx_recv, ecx_self, eb_send, eb_recv,
     ebx_send, ebx_recv, ebx_self, ld_sem, ea_send, ea_recv) = take(31)

    me = lax.axis_index("ep")
    co = (me // 16, lax.rem(me // 4, 4), lax.rem(me, 4))
    starts = [sum(cols[:r]) for r in range(3)]
    span = [pl.ds(starts[r], cols[r]) for r in range(3)]
    d, last = sum(cols), chunks - 1
    a_axis, b_axis, c_axis = ([t[i] for t in TURNS] for i in range(3))

    def hop(c, s):
        return lax.rem(c + s, N)

    def peer(axis, s):
        return {"ep": me + (hop(co[axis], s) - co[axis]) * STRIDE[axis]}

    def remote(src, dst, send, recv, to):
        return pltpu.make_async_remote_copy(
            src_ref=src, dst_ref=dst, send_sem=send, recv_sem=recv, device_id=to, device_id_type=MESH)

    def ab(ref, r, k, a, b):
        return ref.at[k, b, a] if a_axis[r] > b_axis[r] else ref.at[k, a, b]

    def at_c(ref, r, k, c):
        if c_axis[r] == 0:
            return ref.at[k, c, :, :, :, span[r]]
        if c_axis[r] == 1:
            return ref.at[k, :, c, :, :, span[r]]
        return ref.at[k, :, :, c, :, span[r]]

    def at_ca(ref, r, k, c, a):
        ix = {c_axis[r]: c, a_axis[r]: a, b_axis[r]: slice(None)}
        return ref.at[k, ix[0], ix[1], ix[2], :, span[r]]

    every, others = slice(None), pl.ds(1, 3)

    def a_copy(r, s):
        return remote(x_hbm.at[:, span[r]], al[r].at[3 - s], a_send.at[r, 3 - s], a_recv.at[r, 3 - s], peer(a_axis[r], s))

    def m_copy(axis, s):
        return remote(met.at[axis, 0], met.at[axis, N - s], m_send.at[axis, 3 - s], m_recv.at[axis, 3 - s], peer(axis, s))

    def early_copies(r):
        return [pltpu.make_async_copy(stage.at[pl.ds(0, chunks), :, :, :, span[r]], made[r].at[:, 0], st_sem.at[r, 0]),
                pltpu.make_async_copy(stage.at[pl.ds(0, chunks), 0, :, :, span[r]], ab(bl[r], r, every, 0, 0), st_sem.at[r, 1])]

    def b0_copy(r, s):
        return remote(made[r].at[:, 0, s], ab(bl[r], r, every, 0, N - s), b0_send.at[r, s - 1], b0_recv.at[r, s - 1], peer(b_axis[r], s))

    def stage_copies(r, k):
        return [pltpu.make_async_copy(stage.at[others, :, :, :, span[r]], made[r].at[k, others], st_sem.at[r, 0]),
                pltpu.make_async_copy(stage.at[others, 0, :, :, span[r]], ab(bl[r], r, k, others, 0), st_sem.at[r, 1])]

    def b_copy(r, k, s):
        return remote(made[r].at[k, others, s], ab(bl[r], r, k, others, N - s), b_send.at[r, k, s - 1], b_recv.at[r, k, s - 1],
                      peer(b_axis[r], s))

    def c_own(r, k):
        return pltpu.make_async_copy(bl[r].at[k, :, :, 0], at_c(z, r, k, 0), c_self.at[r, k])

    def c_copy(r, k, s):
        return remote(bl[r].at[k, :, :, s], at_c(z, r, k, N - s), c_send.at[r, k, s - 1], c_recv.at[r, k, s - 1], peer(c_axis[r], s))

    def ec_own(r, k):
        return pltpu.make_async_copy(at_c(z, r, k, 0), ecl[r].at[k, :, :, 0], ec_self.at[r, k])

    def ec_copy(r, k, s):
        return remote(at_c(z, r, k, s), ecl[r].at[k, :, :, N - s], ec_send.at[r, k, s - 1], ec_recv.at[r, k, s - 1], peer(c_axis[r], s))

    def ecx_own(r, o):
        return pltpu.make_async_copy(at_ca(z, r, last, 0, o), ab(ecl[r], r, last, o, every).at[:, 0], ecx_self.at[r, o])

    def ecx_copy(r, o, s):
        return remote(at_ca(z, r, last, s, o), ab(ecl[r], r, last, o, every).at[:, N - s], ecx_send.at[r, o, s - 1],
                      ecx_recv.at[r, o, s - 1], peer(c_axis[r], s))

    def eb_copy(r, k, s):
        return remote(ab(ecl[r], r, k, every, s), ebl[r].at[k, :, N - s], eb_send.at[r, k, s - 1], eb_recv.at[r, k, s - 1],
                      peer(b_axis[r], s))

    def ebx_own(r, o):
        return pltpu.make_async_copy(ab(ecl[r], r, last, o, 0), stage.at[o, 0, :, :, span[r]], ebx_self.at[r, o])

    def ebx_copy(r, o, s):
        return remote(ab(ecl[r], r, last, o, s), stage.at[o, N - s, :, :, span[r]], ebx_send.at[r, o, s - 1], ebx_recv.at[r, o, s - 1],
                      peer(b_axis[r], s))

    def ea_copy(r, o):
        return remote(al[r].at[o - 1], eal.at[3 - o, :, span[r]], ea_send.at[r, 3 - o], ea_recv.at[r, 3 - o], peer(a_axis[r], o))

    def load(r, k, b):
        src = ab(ecl[r], r, k, every, 0) if b == 0 else ebl[r].at[k, :, b]
        return pltpu.make_async_copy(src, wd.at[k, :, b, :, :, span[r]], ld_sem.at[r, k, b])

    def up_copies(u):
        i, w = lax.rem(u, 3), pl.ds(pl.multiple_of(u * u_tile, u_tile), u_tile)
        return [pltpu.make_async_copy(sg_hbm.at[:, w], sg.at[i], s_sem.at[i, 0]),
                pltpu.make_async_copy(su_hbm.at[:, w], su.at[i], s_sem.at[i, 1])]

    def down_copy(u):
        i, w = lax.rem(u, 2), pl.ds(pl.multiple_of(u * u_tile, u_tile), u_tile)
        return pltpu.make_async_copy(sd_hbm.at[w, :], sd.at[i], s_sem.at[i, 2])

    def shared(u):
        down_copy(u).start()
        @pl.when(u + 2 < units)
        def _():
            for c in up_copies(u + 2):
                c.start()
        for c in up_copies(u):
            c.wait()
        @pl.when(u > 0)
        def _():
            down_copy(u - 1).wait()
        i, old = lax.rem(u, 3), lax.rem(u + 1, 2)
        g = dot(xv[...], sg[i])
        up = dot(xv[...], su[i])
        acc[...] += dot(act[...], sd[old])
        act[...] = (jax.nn.silu(g) * up).astype(BF16)

    def matches(r, o, first, count, weight):
        wide = min(tokens, 128)
        i = lax.broadcasted_iota(jnp.int32, (128, wide), 0)
        b, c = (co[b_axis[r]] + (i >> 5)) & 3, (co[c_axis[r]] + (i >> 3)) & 3
        expert = co[a_axis[r]] * STRIDE[a_axis[r]] + b * STRIDE[b_axis[r]] + c * STRIDE[c_axis[r]]
        base = (expert * slots + first * SUB + (i & 7)).astype(F32)
        m = met.at[a_axis[r], o]
        out = []
        for k in range(count):
            code, line = base + float(k * SUB), []
            for t in range(0, tokens, wide):
                hit = jnp.zeros((128, wide), F32)
                for j in range(top):
                    new = m[top + j : top + j + 1, t : t + wide] if weight else 1.0
                    hit = jnp.where(m[j : j + 1, t : t + wide] == code, new, hit)
                line.append(hit.astype(BF16))
            out.append(jnp.concatenate(line, axis=1))
        return jnp.concatenate(out)

    def dispatch(k):
        for r in range(3):
            for o in (1, 3, 2):
                rows = dot(matches(r, o, k, 1, False), al[r][o - 1]).astype(BF16)
                stage[o, :, :, :, span[r]] = rows.reshape(N, N, SUB, cols[r])
        for r in range(3):
            for c in stage_copies(r, k):
                c.start()
        for r in range(3):
            for c in stage_copies(r, k):
                c.wait()
        for r, s in HOPS:
            b_copy(r, k, s).start()

    def forward_c(k):
        for r in range(3):
            for s in (1, 2, 3):
                b_copy(r, k, s).wait_recv()
        for r, s in HOPS:
            c_copy(r, k, s).start()
        for r in range(3):
            c_own(r, k).start()

    def forward_eb(k):
        for r in range(3):
            for s in (1, 2, 3):
                ec_copy(r, k, s).wait_recv()
            ec_own(r, k).wait()
        for r, s in HOPS:
            eb_copy(r, k, s).start()

    def forward_ebx(o):
        for r in range(3):
            for s in (1, 2, 3):
                ecx_copy(r, o, s).wait_recv()
            ecx_own(r, o).wait()
        for r, s in HOPS:
            ebx_copy(r, o, s).start()
        for r in range(3):
            ebx_own(r, o).start()

    rows = N * N * N * SUB

    def expert(k):
        for r in range(3):
            for s in (1, 2, 3):
                c_copy(r, k, s).wait_recv()
            c_own(r, k).wait()

        def up(f, _):
            for (ek, ef), event, arg in plan["main"]:
                pl.when((k == ek) & (f == ef))(functools.partial({"C": forward_c, "F": forward_eb}[event], arg))
            w = pl.ds(pl.multiple_of(f * f_tile, f_tile), f_tile)
            zk = z[k].reshape(rows, d)
            h[:, w] = (jax.nn.silu(dot(zk, wg[:, w])) * dot(zk, wu[:, w])).astype(BF16)
            return 0
        lax.fori_loop(0, ff // f_tile, up, 0)

        at = 0
        for r in range(3):
            w = pl.ds(at, cfg["down"][r])
            at += cfg["down"][r]
            out = dot(h[...], wd[:, :, :, :, :, w].reshape(ff, cfg["down"][r]))
            z[k, :, :, :, :, w] = out.astype(BF16).reshape(N, N, N, SUB, cfg["down"][r])

            @pl.when(k < last)
            def _():
                for s in (1, 3, 2):
                    ec_copy(r, k, s).start()
                ec_own(r, k).start()

            @pl.when(k == last)
            def _():
                for o in ORDER:
                    for s in (1, 3, 2):
                        ecx_copy(r, o, s).start()
                    ecx_own(r, o).start()

    def held(r, o):
        return (pl.ds(pl.multiple_of(lax.rem(o, 2) * (128 * chunks), 128), 128 * chunks),
                pl.ds(pl.multiple_of((2 * r + o // 2) * tokens, 128 if tokens % 128 == 0 else tokens), tokens))

    def weigh(i):
        o = ordered(i)
        for r in range(3):
            wg[held(r, o)] = matches(r, o, 0, chunks, True)

    def ordered(i):
        return jnp.where(i == 0, ORDER[0], jnp.where(i == 1, ORDER[1], jnp.where(i == 2, ORDER[2], ORDER[3])))

    def combine(i, _):
        o = ordered(i)
        for r in range(3):
            for s in (1, 2, 3):
                ebx_copy(r, o, s).wait_recv()
            ebx_own(r, o).wait()
        for r in range(3):
            weight = wg[held(r, o)]
            early = wd[0:last, pl.ds(o, 1), :, :, :, span[r]].reshape(128 * last, cols[r])
            late = stage[pl.ds(o, 1), :, :, :, span[r]].reshape(128, cols[r])
            across = (((0,), (0,)), ((), ()))
            part = lax.dot_general(weight[: 128 * last], early, across, preferred_element_type=F32)
            part += lax.dot_general(weight[128 * last :], late, across, preferred_element_type=F32)

            @pl.when(o == 0)
            def _():
                acc[:, span[r]] += part

            @pl.when(o > 0)
            def _():
                al[r][pl.ds(o - 1, 1)] = part.astype(BF16)[None]
                ea_copy(r, o).start()
        return 0

    x_in = pltpu.make_async_copy(x_hbm, xv, x_sem)
    x_in.start()
    for u in range(2):
        for c in up_copies(u):
            c.start()
    code = jnp.where(slot_ref[...] < slots, expert_ref[...] * slots + slot_ref[...], -1).astype(F32)
    for axis in range(3):
        met[axis, 0, :top] = code
        met[axis, 0, top:] = gate_ref[...]
    barrier = pltpu.get_barrier_semaphore()
    for axis in range(3):
        for s in (1, 2, 3):
            pl.semaphore_signal(barrier, inc=1, device_id=peer(axis, s), device_id_type=MESH)
    acc[...] = jnp.zeros_like(acc)
    act[...] = jnp.zeros_like(act)
    sd[1] = jnp.zeros_like(sd[1])
    pl.semaphore_wait(barrier, 9)
    for s in (1, 3, 2):
        for axis in range(3):
            m_copy(axis, s).start()
        for r in range(3):
            a_copy(r, s).start()
    x_in.wait()
    for r in range(3):
        mine = dot(matches(r, 0, 0, chunks, False), xv[:, span[r]]).astype(BF16)
        stage[0:chunks, :, :, :, span[r]] = mine.reshape(chunks, N, N, SUB, cols[r])
    for r in range(3):
        for c in early_copies(r):
            c.start()
    for r in range(3):
        for c in early_copies(r):
            c.wait()
    for r, s in HOPS:
        b0_copy(r, s).start()

    def weight_copy(which, k):
        if which == 2:
            return pltpu.make_async_copy(wd_hbm.at[k], wd.at[k], w_sem.at[2, k])
        w = pl.ds(pl.multiple_of(k * (d // 4), d // 4), d // 4)
        return pltpu.make_async_copy((wg_hbm, wu_hbm)[which].at[w], (wg, wu)[which].at[w], w_sem.at[which, k])

    pieces = (4, 4, chunks)
    if plan["weights"] < 0:
        for which in range(3):
            for k in range(pieces[which]):
                weight_copy(which, k).start()

    def pre(i, _):
        first, gathers, forwards = plan["weights"], plan["gather"], plan["forward"]
        if first >= 0:
            for which in range(3):
                at = first + sum(pieces[:which])

                @pl.when((i >= at) & (i < at + pieces[which]))
                def _():
                    weight_copy(which, i - at).start()

        @pl.when(i == gathers[0])
        def _():
            for axis in range(3):
                for s in (1, 2, 3):
                    m_copy(axis, s).wait_recv()
            for r, s in HOPS:
                a_copy(r, s).wait_recv()

        @pl.when(i == forwards[0])
        def _():
            for r, s in HOPS:
                b0_copy(r, s).wait_recv()

        @pl.when(any_of(i, forwards))
        def _():
            forward_c(before(i, forwards))

        @pl.when(any_of(i, gathers))
        def _():
            dispatch(before(i, gathers))

        shared(i)
        return 0
    lax.fori_loop(0, plan["pre"], pre, 0)
    for which in range(3):
        for k in range(pieces[which]):
            weight_copy(which, k).wait()
    lax.fori_loop(0, chunks, lambda k, _: (expert(k), 0)[1], 0)

    def fetch(ks):
        for k in ks:
            for r in range(3):
                for s in (1, 2, 3):
                    eb_copy(r, k, s).wait_recv()
                for b in range(4):
                    load(r, k, b).start()

    def tail(i, _):
        @pl.when(i < 4)
        def _():
            weigh(i)

        @pl.when(i == plan["eb"])
        def _():
            forward_eb(last - 1)

        @pl.when(i == plan["fetch"])
        def _():
            fetch(range(last - 1))

        for p, o in zip(plan["ebx"], ORDER, strict=True):
            pl.when(i == p)(functools.partial(forward_ebx, o))

        @pl.when(i == plan["sums"])
        def _():
            fetch([last - 1])
            for k in range(last):
                for r in range(3):
                    for b in range(4):
                        load(r, k, b).wait()
            lax.fori_loop(0, 4, combine, 0)

        shared(i + plan["pre"])
        return 0
    lax.fori_loop(0, units - plan["pre"], tail, 0)
    down_copy(units - 1).wait()
    acc[...] += dot(act[...], sd[(units - 1) % 2])
    out = pltpu.make_async_copy(acc, sum_hbm, out_sem)
    out.start()
    for r, s in HOPS:
        ea_copy(r, s).wait_recv()

    for axis in range(3):
        for s in (1, 2, 3):
            m_copy(axis, s).wait_send()
    for r, s in HOPS:
        a_copy(r, s).wait_send()
        b0_copy(r, s).wait_send()
        ea_copy(r, s).wait_send()
        for o in range(4):
            ecx_copy(r, o, s).wait_send()
            ebx_copy(r, o, s).wait_send()

    def drain(k, _):
        for r, s in HOPS:
            b_copy(r, k, s).wait_send()
            c_copy(r, k, s).wait_send()
            @pl.when(k < last)
            def _():
                ec_copy(r, k, s).wait_send()
                eb_copy(r, k, s).wait_send()
        return 0
    lax.fori_loop(0, chunks, drain, 0)
    out.wait()


def layer(x, expert, slot, gate, w_gate, w_up, w_down, s_gate, s_up, s_down, cfg):
    tokens, chunks, cols, ff, u_tile, top = (cfg[n] for n in ("tokens", "chunks", "cols", "ff", "u_tile", "top"))
    d, rows = sum(cols), N * N * N * SUB
    hbm, vm = pl.BlockSpec(memory_space=pl.ANY), pl.BlockSpec(memory_space=pltpu.VMEM)
    block = lambda w: jax.ShapeDtypeStruct((chunks, N, N, N, SUB, w), BF16)
    dma = pltpu.SemaphoreType.DMA
    phase, single, quarter = [dma((3, chunks, 3))] * 2, [dma((3, 3))] * 2, [dma((3, 4, 3))] * 2
    outs = pl.pallas_call(
        functools.partial(kernel, cfg),
        out_shape=[jax.ShapeDtypeStruct((tokens, d), F32), jax.ShapeDtypeStruct((3, tokens, d), BF16)]
        + [block(w) for _ in range(4) for w in cols],
        in_specs=[hbm] + [vm] * 3 + [hbm] * 6,
        out_specs=[hbm] * 14,
        scratch_shapes=[
            pltpu.VMEM((tokens, d), BF16),
            *[pltpu.VMEM((3, tokens, w), BF16) for w in cols],
            pltpu.VMEM((3, 4, 2 * top, tokens), F32),
            pltpu.VMEM((max(chunks, 4), N, N, SUB, d), BF16),
            pltpu.VMEM((d, ff), BF16),
            pltpu.VMEM((d, ff), BF16),
            pltpu.VMEM((chunks, N, N, N, SUB, d), BF16),
            pltpu.VMEM((chunks, N, N, N, SUB, d), BF16),
            pltpu.VMEM((rows, ff), BF16),
            pltpu.VMEM((tokens, d), F32),
            pltpu.VMEM((3, d, u_tile), BF16),
            pltpu.VMEM((3, d, u_tile), BF16),
            pltpu.VMEM((2, u_tile, d), BF16),
            pltpu.VMEM((tokens, u_tile), BF16),
            dma(()), dma((3, max(chunks, 4))), dma((3, 3)), dma((3, 2)), dma(()),
            *single, *single, *single,
            *phase, dma((3, chunks)),
            *phase, dma((3, chunks)),
            *phase, dma((3, chunks)),
            *quarter, dma((3, 4)),
            *phase,
            *quarter, dma((3, 4)),
            dma((3, chunks, 4)), *single,
        ],
        compiler_params=pltpu.CompilerParams(collective_id=0, has_side_effects=True, vmem_limit_bytes=cfg["vmem"]),
        name="moe_layer",
    )(x, expert, slot, gate, w_gate, w_up, w_down.reshape(chunks, N, N, N, SUB, d), s_gate, s_up, s_down)
    total, sums = outs[:2]
    for o in range(3):
        total += sums[o].astype(F32)
    return total.astype(BF16)


PLAN = {
    "pre": 18, "weights": 1, "gather": (8, 9, 10, 13, 15), "forward": (13, 15, 16),
    "main": (((0, 3), "C", 3), ((1, 1), "C", 4), ((2, 3), "F", 0), ((3, 3), "F", 1), ((4, 2), "F", 2)),
    "fetch": 1, "eb": 2, "ebx": (7, 8, 9, 10), "sums": 14,
}


def configure(x, expert, w_gate, s_gate):
    tokens, d = x.shape[-2:]
    top, ff, width, experts = expert.shape[-1], w_gate.shape[-1], s_gate.shape[-1], N * N * N
    slots = 5 * tokens * top // (4 * experts)
    lanes = d // 128
    cols = tuple(128 * ((lanes + 2 - r) // 3) for r in range(3))
    return dict(tokens=tokens, top=top, slots=slots, chunks=slots // SUB, cols=cols, ff=ff, f_tile=512, down=(768, 512, 512),
                units=width // 512, u_tile=512, plan=PLAN, vmem=67043328)


TEST = dict(
    cols=(256, 256, 128), down=(256, 256, 128),
    plan={"pre": 2, "weights": -9, "gather": (0, 1), "forward": (1,), "main": (((0, 1), "C", 1),),
          "fetch": 0, "eb": 0, "ebx": (1, 2, 3, 3), "sums": 4})


def solution(mesh):
    def step(x, expert, slot, gate, w_gate, w_up, w_down, s_gate, s_up, s_down):
        cfg = configure(x, expert, w_gate, s_gate)
        y = layer(x[0, 0], expert[0, 0].T, slot[0, 0].T, gate[0, 0].T, w_gate[0], w_up[0], w_down[0], s_gate, s_up, s_down, cfg)
        return y[None, None]

    tok, own, whole = P("dp", "ep", None, None), P("ep", None, None), P(None, None)
    return jax.shard_map(step, mesh=mesh, in_specs=(tok,) * 4 + (own,) * 3 + (whole,) * 3, out_specs=tok, check_vma=False)
```

```python
import functools

import jax
import jax.numpy as jnp
from jax import lax
from jax.experimental import pallas as pl
from jax.experimental.pallas import tpu as pltpu
from jax.sharding import PartitionSpec as P

MESH = pl.DeviceIdType.MESH
N = 4
STRIDE = (16, 4, 1)
TURNS = ((0, 1, 2), (1, 2, 0), (2, 0, 1))
SUB = 8
ORDER = (2, 1, 3, 0)
HOPS = tuple((r, s) for s in (1, 3, 2) for r in range(3))
F32, BF16 = jnp.float32, jnp.bfloat16


def dot(a, b):
    return jnp.dot(a, b, preferred_element_type=F32)


def any_of(i, places):
    hit = i == places[0]
    for p in places[1:]:
        hit = hit | (i == p)
    return hit


def before(i, places):
    return sum((i > p).astype(jnp.int32) for p in places)


def kernel(cfg, *refs):
    tokens, chunks, cols, ff, f_tile, units, u_tile, top, slots, plan = (
        cfg[n] for n in ("tokens", "chunks", "cols", "ff", "f_tile", "units", "u_tile", "top", "slots", "plan"))
    it = iter(refs)
    take = lambda n: [next(it) for _ in range(n)]
    x_hbm, expert_ref, slot_ref, gate_ref, wg_hbm, wu_hbm, wd_hbm, sg_hbm, su_hbm, sd_hbm = take(10)
    sum_hbm, eal = take(2)
    made, bl, ecl, ebl = take(3), take(3), take(3), take(3)
    (xv,) = take(1)
    al = take(3)
    met, stage, wg, wu, wd, z, h, acc, sg, su, sd, act = take(12)
    (x_sem, w_sem, s_sem, st_sem, out_sem, a_send, a_recv, m_send, m_recv, b0_send, b0_recv, b_send, b_recv, b_self,
     c_send, c_recv, c_self, ec_send, ec_recv, ec_self, ecx_send, ecx_recv, ecx_self, eb_send, eb_recv,
     ebx_send, ebx_recv, ebx_self, ld_sem, ea_send, ea_recv) = take(31)

    me = lax.axis_index("ep")
    co = (me // 16, lax.rem(me // 4, 4), lax.rem(me, 4))
    starts = [sum(cols[:r]) for r in range(3)]
    span = [pl.ds(starts[r], cols[r]) for r in range(3)]
    d, last = sum(cols), chunks - 1
    a_axis, b_axis, c_axis = ([t[i] for t in TURNS] for i in range(3))

    def hop(c, s):
        return lax.rem(c + s, N)

    def peer(axis, s):
        return {"ep": me + (hop(co[axis], s) - co[axis]) * STRIDE[axis]}

    def remote(src, dst, send, recv, to):
        return pltpu.make_async_remote_copy(
            src_ref=src, dst_ref=dst, send_sem=send, recv_sem=recv, device_id=to, device_id_type=MESH)

    def ab(ref, r, k, a, b):
        return ref.at[k, b, a] if a_axis[r] > b_axis[r] else ref.at[k, a, b]

    def at_c(ref, r, k, c):
        if c_axis[r] == 0:
            return ref.at[k, c, :, :, :, span[r]]
        if c_axis[r] == 1:
            return ref.at[k, :, c, :, :, span[r]]
        return ref.at[k, :, :, c, :, span[r]]

    def at_ca(ref, r, k, c, a):
        ix = {c_axis[r]: c, a_axis[r]: a, b_axis[r]: slice(None)}
        return ref.at[k, ix[0], ix[1], ix[2], :, span[r]]

    every, others = slice(None), pl.ds(1, 3)

    def a_copy(r, s):
        return remote(x_hbm.at[:, span[r]], al[r].at[3 - s], a_send.at[r, 3 - s], a_recv.at[r, 3 - s], peer(a_axis[r], s))

    def m_copy(axis, s):
        return remote(met.at[axis, 0], met.at[axis, N - s], m_send.at[axis, 3 - s], m_recv.at[axis, 3 - s], peer(axis, s))

    def early_copies(r):
        return [pltpu.make_async_copy(wd.at[:, 0, :, :, :, span[r]], made[r].at[:, 0], st_sem.at[r, 0]),
                pltpu.make_async_copy(wd.at[:, 0, 0, :, :, span[r]], ab(bl[r], r, every, 0, 0), st_sem.at[r, 1])]

    def b0_copy(r, s):
        return remote(made[r].at[:, 0, s], ab(bl[r], r, every, 0, N - s), b0_send.at[r, s - 1], b0_recv.at[r, s - 1], peer(b_axis[r], s))

    def stage_copies(r, k):
        return [pltpu.make_async_copy(stage.at[others, :, :, :, span[r]], made[r].at[k, others], st_sem.at[r, 0]),
                pltpu.make_async_copy(stage.at[others, 0, :, :, span[r]], ab(bl[r], r, k, others, 0), st_sem.at[r, 1])]

    def b_copy(r, k, s):
        return remote(made[r].at[k, others, s], ab(bl[r], r, k, others, N - s), b_send.at[r, k, s - 1], b_recv.at[r, k, s - 1],
                      peer(b_axis[r], s))

    def c_own(r, k):
        return pltpu.make_async_copy(bl[r].at[k, :, :, 0], at_c(z, r, k, 0), c_self.at[r, k])

    def c_copy(r, k, s):
        return remote(bl[r].at[k, :, :, s], at_c(z, r, k, N - s), c_send.at[r, k, s - 1], c_recv.at[r, k, s - 1], peer(c_axis[r], s))

    def ec_own(r, k):
        return pltpu.make_async_copy(at_c(z, r, k, 0), ecl[r].at[k, :, :, 0], ec_self.at[r, k])

    def ec_copy(r, k, s):
        return remote(at_c(z, r, k, s), ecl[r].at[k, :, :, N - s], ec_send.at[r, k, s - 1], ec_recv.at[r, k, s - 1], peer(c_axis[r], s))

    def ecx_own(r, o):
        return pltpu.make_async_copy(at_ca(z, r, last, 0, o), ab(ecl[r], r, last, o, every).at[:, 0], ecx_self.at[r, o])

    def ecx_copy(r, o, s):
        return remote(at_ca(z, r, last, s, o), ab(ecl[r], r, last, o, every).at[:, N - s], ecx_send.at[r, o, s - 1],
                      ecx_recv.at[r, o, s - 1], peer(c_axis[r], s))

    def eb_copy(r, k, s):
        return remote(ab(ecl[r], r, k, every, s), ebl[r].at[k, :, N - s], eb_send.at[r, k, s - 1], eb_recv.at[r, k, s - 1],
                      peer(b_axis[r], s))

    def ebx_own(r, o):
        return pltpu.make_async_copy(ab(ecl[r], r, last, o, 0), stage.at[o, 0, :, :, span[r]], ebx_self.at[r, o])

    def ebx_copy(r, o, s):
        return remote(ab(ecl[r], r, last, o, s), stage.at[o, N - s, :, :, span[r]], ebx_send.at[r, o, s - 1], ebx_recv.at[r, o, s - 1],
                      peer(b_axis[r], s))

    def ea_copy(r, o):
        return remote(al[r].at[o - 1], eal.at[3 - o, :, span[r]], ea_send.at[r, 3 - o], ea_recv.at[r, 3 - o], peer(a_axis[r], o))

    def load(r, k, b):
        src = ab(ecl[r], r, k, every, 0) if b == 0 else ebl[r].at[k, :, b]
        return pltpu.make_async_copy(src, wd.at[k, :, b, :, :, span[r]], ld_sem.at[r, k, b])

    def up_copies(u):
        i, w = lax.rem(u, 3), pl.ds(pl.multiple_of(u * u_tile, u_tile), u_tile)
        return [pltpu.make_async_copy(sg_hbm.at[:, w], sg.at[i], s_sem.at[i, 0]),
                pltpu.make_async_copy(su_hbm.at[:, w], su.at[i], s_sem.at[i, 1])]

    def down_copy(u):
        i, w = lax.rem(u, 2), pl.ds(pl.multiple_of(u * u_tile, u_tile), u_tile)
        return pltpu.make_async_copy(sd_hbm.at[w, :], sd.at[i], s_sem.at[i, 2])

    def shared(u, beside=None):
        down_copy(u).start()
        @pl.when(u + 2 < units)
        def _():
            for c in up_copies(u + 2):
                c.start()
        for c in up_copies(u):
            c.wait()
        @pl.when(u > 0)
        def _():
            down_copy(u - 1).wait()
        i, old = lax.rem(u, 3), lax.rem(u + 1, 2)
        beside = beside or (lambda r: None)
        g = dot(xv[...], sg[i])
        beside(0)
        up = dot(xv[...], su[i])
        beside(1)
        acc[...] += dot(act[...], sd[old])
        act[...] = (jax.nn.silu(g) * up).astype(BF16)
        beside(2)

    def matches(r, o, first, count, weight):
        m = met.at[a_axis[r], o]
        code = m[:top].astype(jnp.int32)
        at = [(code >> (10 - 2 * axis)) & 3 for axis in range(3)]
        here = (code >= 0) & (at[a_axis[r]] == co[a_axis[r]])
        place = ((at[b_axis[r]] - co[b_axis[r]]) & 3) * 32 + ((at[c_axis[r]] - co[c_axis[r]]) & 3) * 8 + (code & 7)
        chunk = jnp.where(here, (code & 63) >> 3, -1)
        spread = lambda v, j: jnp.broadcast_to(v[j : j + 1], (16, tokens)).astype(BF16)[None]
        given = [spread(m[top:], j) for j in range(top)] if weight else [jnp.ones((1, 16, tokens), BF16)] * top
        row = (lax.broadcasted_iota(jnp.int32, (8, 16, tokens), 0) * 16 + lax.broadcasted_iota(jnp.int32, (8, 16, tokens), 1))
        row = row.astype(F32).astype(BF16)
        out = []
        for k in range(count):
            mine = jnp.where(chunk == first + k, place, -1).astype(F32)
            hit = jnp.zeros((8, 16, tokens), BF16)
            for j in range(top):
                hit = jnp.where(spread(mine, j) == row, given[j], hit)
            out.append(hit.reshape(128, tokens))
        return jnp.concatenate(out) if count > 1 else out[0]

    def gather(k, r):
        for o in (1, 3, 2):
            rows = dot(matches(r, o, k, 1, False), al[r][o - 1]).astype(BF16)
            stage[o, :, :, :, span[r]] = rows.reshape(N, N, SUB, cols[r])

    def keep(k):
        for r in range(3):
            for c in stage_copies(r, k):
                c.start()

    def dispatch(k):
        for r in range(3):
            for c in stage_copies(r, k):
                c.wait()
        for r, s in HOPS:
            b_copy(r, k, s).start()

    def forward_c(k):
        for r in range(3):
            for s in (1, 2, 3):
                b_copy(r, k, s).wait_recv()
        for r, s in HOPS:
            c_copy(r, k, s).start()
        for r in range(3):
            c_own(r, k).start()

    def forward_eb(k):
        for r in range(3):
            for s in (1, 2, 3):
                ec_copy(r, k, s).wait_recv()
            ec_own(r, k).wait()
        for r, s in HOPS:
            eb_copy(r, k, s).start()

    def forward_ebx(o):
        for r in range(3):
            for s in (1, 2, 3):
                ecx_copy(r, o, s).wait_recv()
            ecx_own(r, o).wait()
        for r, s in HOPS:
            ebx_copy(r, o, s).start()
        for r in range(3):
            ebx_own(r, o).start()

    rows = N * N * N * SUB

    def expert(k):
        for r in range(3):
            for s in (1, 2, 3):
                c_copy(r, k, s).wait_recv()
            c_own(r, k).wait()

        def up(f, _):
            for (ek, ef), event, arg in plan["main"]:
                pl.when((k == ek) & (f == ef))(functools.partial({"C": forward_c, "F": forward_eb}[event], arg))
            w = pl.ds(pl.multiple_of(f * f_tile, f_tile), f_tile)
            zk = z[k].reshape(rows, d)
            h[:, w] = (jax.nn.silu(dot(zk, wg[:, w])) * dot(zk, wu[:, w])).astype(BF16)
            return 0
        lax.fori_loop(0, ff // f_tile, up, 0)

        at = 0
        for r in range(3):
            w = pl.ds(at, cfg["down"][r])
            at += cfg["down"][r]
            out = dot(h[...], wd[:, :, :, :, :, w].reshape(ff, cfg["down"][r]))
            z[k, :, :, :, :, w] = out.astype(BF16).reshape(N, N, N, SUB, cfg["down"][r])

            @pl.when(k < last)
            def _():
                for s in (1, 3, 2):
                    ec_copy(r, k, s).start()
                ec_own(r, k).start()

            @pl.when(k == last)
            def _():
                for o in ORDER:
                    for s in (1, 3, 2):
                        ecx_copy(r, o, s).start()
                    ecx_own(r, o).start()

    def held(r, o):
        wide = 128 * chunks
        return pl.ds(r * tokens, tokens), pl.ds(pl.multiple_of(o * wide, wide), wide)

    def weigh(i, r):
        o = ordered(i)
        wg[held(r, o)] = matches(r, o, 0, chunks, True).T

    def ordered(i):
        return jnp.where(i == 0, ORDER[0], jnp.where(i == 1, ORDER[1], jnp.where(i == 2, ORDER[2], ORDER[3])))

    def combine(i, _):
        o = ordered(i)
        for r in range(3):
            for s in (1, 2, 3):
                ebx_copy(r, o, s).wait_recv()
            ebx_own(r, o).wait()
        for r in range(3):
            weight = wg[held(r, o)]
            early = wd[0:last, pl.ds(o, 1), :, :, :, span[r]].reshape(128 * last, cols[r])
            late = stage[pl.ds(o, 1), :, :, :, span[r]].reshape(128, cols[r])
            part = dot(weight[:, : 128 * last], early) + dot(weight[:, 128 * last :], late)

            @pl.when(o == 0)
            def _():
                acc[:, span[r]] += part

            @pl.when(o > 0)
            def _():
                al[r][pl.ds(o - 1, 1)] = part.astype(BF16)[None]
                ea_copy(r, o).start()
        return 0

    x_in = pltpu.make_async_copy(x_hbm, xv, x_sem)
    x_in.start()
    for u in range(2):
        for c in up_copies(u):
            c.start()
    code = jnp.where(slot_ref[...] < slots, expert_ref[...] * 64 + slot_ref[...], -1).astype(F32)
    for axis in range(3):
        met[axis, 0, :top] = code
        met[axis, 0, top:] = gate_ref[...]
    barrier = pltpu.get_barrier_semaphore()
    for axis in range(3):
        for s in (1, 2, 3):
            pl.semaphore_signal(barrier, inc=1, device_id=peer(axis, s), device_id_type=MESH)
    acc[...] = jnp.zeros_like(acc)
    act[...] = jnp.zeros_like(act)
    sd[1] = jnp.zeros_like(sd[1])
    pl.semaphore_wait(barrier, 9)
    for s in (1, 3, 2):
        for axis in range(3):
            m_copy(axis, s).start()
        for r in range(3):
            a_copy(r, s).start()
    x_in.wait()
    for r in range(3):
        mine = dot(matches(r, 0, 0, chunks, False), xv[:, span[r]]).astype(BF16)
        wd[:, 0, :, :, :, span[r]] = mine.reshape(chunks, N, N, SUB, cols[r])
    for r in range(3):
        for c in early_copies(r):
            c.start()
    for r in range(3):
        for c in early_copies(r):
            c.wait()
    for r, s in HOPS:
        b0_copy(r, s).start()

    def weight_copy(which, k):
        if which == 2:
            return pltpu.make_async_copy(wd_hbm.at[k], wd.at[k], w_sem.at[2, k])
        w = pl.ds(pl.multiple_of(k * (d // 4), d // 4), d // 4)
        return pltpu.make_async_copy((wg_hbm, wu_hbm)[which].at[w], (wg, wu)[which].at[w], w_sem.at[which, k])

    pieces = (4, 4, chunks)
    if plan["weights"] < 0:
        for which in range(3):
            for k in range(pieces[which]):
                weight_copy(which, k).start()

    def pre(i, _):
        first, gathers, forwards = plan["weights"], plan["gather"], plan["forward"]
        if first >= 0:
            for which in range(3):
                at = first + sum(pieces[:which])

                @pl.when((i >= at) & (i < at + pieces[which]))
                def _():
                    weight_copy(which, i - at).start()

        @pl.when(any_of(i - 1, gathers))
        def _():
            dispatch(before(i - 1, gathers))

        @pl.when(i == gathers[0])
        def _():
            for axis in range(3):
                for s in (1, 2, 3):
                    m_copy(axis, s).wait_recv()
            for r, s in HOPS:
                a_copy(r, s).wait_recv()

        @pl.when(i == forwards[0])
        def _():
            for r, s in HOPS:
                b0_copy(r, s).wait_recv()

        @pl.when(any_of(i, forwards))
        def _():
            forward_c(before(i, forwards))

        gathering = any_of(i, gathers)

        @pl.when(gathering)
        def _():
            k = before(i, gathers)
            shared(i, lambda r: gather(k, r))
            keep(k)

        @pl.when(jnp.logical_not(gathering))
        def _():
            shared(i)
        return 0
    lax.fori_loop(0, plan["pre"], pre, 0)
    for which in range(3):
        for k in range(pieces[which]):
            weight_copy(which, k).wait()
    lax.fori_loop(0, chunks, lambda k, _: (expert(k), 0)[1], 0)

    def fetch(ks):
        for k in ks:
            for r in range(3):
                for s in (1, 2, 3):
                    eb_copy(r, k, s).wait_recv()
                for b in range(4):
                    load(r, k, b).start()

    def masks(i, _):
        @pl.when(i == plan["eb"])
        def _():
            forward_eb(last - 1)

        shared(i + plan["pre"], lambda r: weigh(i, r))
        return 0
    lax.fori_loop(0, 4, masks, 0)

    def tail(i, _):
        @pl.when(i == plan["fetch"])
        def _():
            fetch(range(last - 1))

        for p, o in zip(plan["ebx"], ORDER, strict=True):
            pl.when(i == p)(functools.partial(forward_ebx, o))

        @pl.when(i == plan["sums"])
        def _():
            fetch([last - 1])
            for k in range(last):
                for r in range(3):
                    for b in range(4):
                        load(r, k, b).wait()
            lax.fori_loop(0, 4, combine, 0)

        shared(i + plan["pre"])
        return 0
    lax.fori_loop(4, units - plan["pre"], tail, 0)
    down_copy(units - 1).wait()
    acc[...] += dot(act[...], sd[(units - 1) % 2])
    out = pltpu.make_async_copy(acc, sum_hbm, out_sem)
    out.start()
    for r, s in HOPS:
        ea_copy(r, s).wait_recv()

    for axis in range(3):
        for s in (1, 2, 3):
            m_copy(axis, s).wait_send()
    for r, s in HOPS:
        a_copy(r, s).wait_send()
        b0_copy(r, s).wait_send()
        ea_copy(r, s).wait_send()
        for o in range(4):
            ecx_copy(r, o, s).wait_send()
            ebx_copy(r, o, s).wait_send()

    def drain(k, _):
        for r, s in HOPS:
            b_copy(r, k, s).wait_send()
            c_copy(r, k, s).wait_send()
            @pl.when(k < last)
            def _():
                ec_copy(r, k, s).wait_send()
                eb_copy(r, k, s).wait_send()
        return 0
    lax.fori_loop(0, chunks, drain, 0)
    out.wait()


def layer(x, expert, slot, gate, w_gate, w_up, w_down, s_gate, s_up, s_down, cfg):
    tokens, chunks, cols, ff, u_tile, top = (cfg[n] for n in ("tokens", "chunks", "cols", "ff", "u_tile", "top"))
    d, rows = sum(cols), N * N * N * SUB
    hbm, vm = pl.BlockSpec(memory_space=pl.ANY), pl.BlockSpec(memory_space=pltpu.VMEM)
    block = lambda w: jax.ShapeDtypeStruct((chunks, N, N, N, SUB, w), BF16)
    dma = pltpu.SemaphoreType.DMA
    phase, single, quarter = [dma((3, chunks, 3))] * 2, [dma((3, 3))] * 2, [dma((3, 4, 3))] * 2
    outs = pl.pallas_call(
        functools.partial(kernel, cfg),
        out_shape=[jax.ShapeDtypeStruct((tokens, d), F32), jax.ShapeDtypeStruct((3, tokens, d), BF16)]
        + [block(w) for _ in range(4) for w in cols],
        in_specs=[hbm] + [vm] * 3 + [hbm] * 6,
        out_specs=[hbm] * 14,
        scratch_shapes=[
            pltpu.VMEM((tokens, d), BF16),
            *[pltpu.VMEM((3, tokens, w), BF16) for w in cols],
            pltpu.VMEM((3, 4, 2 * top, tokens), F32),
            pltpu.VMEM((N, N, N, SUB, d), BF16),
            pltpu.VMEM((d, ff), BF16),
            pltpu.VMEM((d, ff), BF16),
            pltpu.VMEM((chunks, N, N, N, SUB, d), BF16),
            pltpu.VMEM((chunks, N, N, N, SUB, d), BF16),
            pltpu.VMEM((rows, ff), BF16),
            pltpu.VMEM((tokens, d), F32),
            pltpu.VMEM((3, d, u_tile), BF16),
            pltpu.VMEM((3, d, u_tile), BF16),
            pltpu.VMEM((2, u_tile, d), BF16),
            pltpu.VMEM((tokens, u_tile), BF16),
            dma(()), dma((3, max(chunks, 4))), dma((3, 3)), dma((3, 2)), dma(()),
            *single, *single, *single,
            *phase, dma((3, chunks)),
            *phase, dma((3, chunks)),
            *phase, dma((3, chunks)),
            *quarter, dma((3, 4)),
            *phase,
            *quarter, dma((3, 4)),
            dma((3, chunks, 4)), *single,
        ],
        compiler_params=pltpu.CompilerParams(collective_id=0, has_side_effects=True, vmem_limit_bytes=cfg["vmem"]),
        name="moe_layer",
    )(x, expert, slot, gate, w_gate, w_up, w_down.reshape(chunks, N, N, N, SUB, d), s_gate, s_up, s_down)
    total, sums = outs[:2]
    for o in range(3):
        total += sums[o].astype(F32)
    return total.astype(BF16)


PLAN = {
    "pre": 21, "weights": 1, "gather": (7, 8, 9, 13, 16), "forward": (12, 16, 18),
    "main": (((0, 3), "C", 3), ((1, 2), "C", 4), ((2, 3), "F", 0), ((3, 3), "F", 1), ((4, 3), "F", 2)),
    "eb": 3, "ebx": (6, 8, 9, 9), "fetch": 12, "sums": 13,
}


def configure(x, expert, w_gate, s_gate):
    tokens, d = x.shape[-2:]
    top, ff, width, experts = expert.shape[-1], w_gate.shape[-1], s_gate.shape[-1], N * N * N
    slots = 5 * tokens * top // (4 * experts)
    lanes = d // 128
    cols = tuple(128 * ((lanes + 2 - r) // 3) for r in range(3))
    return dict(tokens=tokens, top=top, slots=slots, chunks=slots // SUB, cols=cols, ff=ff, f_tile=512, down=(768, 512, 512),
                units=width // 512, u_tile=512, plan=PLAN, vmem=67043328)


TEST = dict(
    cols=(256, 256, 128), down=(256, 256, 128),
    plan={"pre": 3, "weights": -9, "gather": (0, 1), "forward": (2,), "main": (((0, 1), "C", 1),),
          "eb": 0, "ebx": (4, 4, 5, 5), "fetch": 5, "sums": 6})


def solution(mesh):
    def step(x, expert, slot, gate, w_gate, w_up, w_down, s_gate, s_up, s_down):
        cfg = configure(x, expert, w_gate, s_gate)
        y = layer(x[0, 0], expert[0, 0].T, slot[0, 0].T, gate[0, 0].T, w_gate[0], w_up[0], w_down[0], s_gate, s_up, s_down, cfg)
        return y[None, None]

    tok, own, whole = P("dp", "ep", None, None), P("ep", None, None), P(None, None)
    return jax.shard_map(step, mesh=mesh, in_specs=(tok,) * 4 + (own,) * 3 + (whole,) * 3, out_specs=tok, check_vma=False)
```

```python
import functools

import jax
import jax.numpy as jnp
from jax import lax
from jax.experimental import pallas as pl
from jax.experimental.pallas import tpu as pltpu
from jax.sharding import PartitionSpec as P

MESH = pl.DeviceIdType.MESH
N = 4
STRIDE = (16, 4, 1)
TURNS = ((0, 1, 2), (1, 2, 0), (2, 0, 1))
SUB = 8
ORDER = (2, 1, 3, 0)
HOPS = tuple((r, s) for s in (1, 3, 2) for r in range(3))
SIDES = tuple((r, s) for s in (1, 3) for r in range(3))
F32, BF16 = jnp.float32, jnp.bfloat16


def dot(a, b):
    return jnp.dot(a, b, preferred_element_type=F32)


def any_of(i, places):
    hit = i == places[0]
    for p in places[1:]:
        hit = hit | (i == p)
    return hit


def before(i, places):
    return sum((i > p).astype(jnp.int32) for p in places)


def kernel(cfg, *refs):
    tokens, chunks, cols, ff, f_tile, units, u_tile, top, slots, plan = (
        cfg[n] for n in ("tokens", "chunks", "cols", "ff", "f_tile", "units", "u_tile", "top", "slots", "plan"))
    it = iter(refs)
    take = lambda n: [next(it) for _ in range(n)]
    x_hbm, expert_ref, slot_ref, gate_ref, wg_hbm, wu_hbm, wd_hbm, sg_hbm, su_hbm, sd_hbm = take(10)
    sum_hbm, eal = take(2)
    made, bl, ecl, ebl = take(3), take(3), take(3), take(3)
    (xv,) = take(1)
    al = take(3)
    met, stage, wg, wu, wd, z, h, acc, sg, su, sd, act = take(12)
    (x_sem, w_sem, s_sem, st_sem, out_sem, a_send, a_recv, r_send, r_recv, m_send, m_recv, b0_send, b0_recv, b_send, b_recv,
     c_send, c_recv, ec_send, ec_recv, ecx_send, ecx_recv, eb_send, eb_recv,
     ebx_send, ebx_recv, ld_sem, ea_send, ea_recv) = take(28)

    me = lax.axis_index("ep")
    co = (me // 16, lax.rem(me // 4, 4), lax.rem(me, 4))
    starts = [sum(cols[:r]) for r in range(3)]
    span = [pl.ds(starts[r], cols[r]) for r in range(3)]
    d, last = sum(cols), chunks - 1
    a_axis, b_axis, c_axis = ([t[i] for t in TURNS] for i in range(3))

    def hop(c, s):
        return lax.rem(c + s, N)

    def peer(axis, s):
        return {"ep": me + (hop(co[axis], s) - co[axis]) * STRIDE[axis]}

    def remote(src, dst, send, recv, to):
        return pltpu.make_async_remote_copy(
            src_ref=src, dst_ref=dst, send_sem=send, recv_sem=recv, device_id=to, device_id_type=MESH)

    def ab(ref, r, k, a, b):
        return ref.at[k, b, a] if a_axis[r] > b_axis[r] else ref.at[k, a, b]

    def at_c(ref, r, k, c):
        if c_axis[r] == 0:
            return ref.at[k, c, :, :, :, span[r]]
        if c_axis[r] == 1:
            return ref.at[k, :, c, :, :, span[r]]
        return ref.at[k, :, :, c, :, span[r]]

    def at_ca(ref, r, k, c, a):
        ix = {c_axis[r]: c, a_axis[r]: a, b_axis[r]: slice(None)}
        return ref.at[k, ix[0], ix[1], ix[2], :, span[r]]

    every, others = slice(None), pl.ds(1, 3)

    def a_copy(r, s):
        return remote(x_hbm.at[:, span[r]], al[r].at[3 - s], a_send, a_recv, peer(a_axis[r], s))

    def relay(r, s):
        half = pl.ds(0 if s == 1 else tokens // 2, tokens // 2)
        return remote(al[r].at[3 - s, half], al[r].at[1, half], r_send, r_recv, peer(a_axis[r], s))

    def m_copy(axis, s):
        return remote(met.at[axis, 0], met.at[axis, N - s], m_send, m_recv, peer(axis, s))

    def early_copies(r):
        return [pltpu.make_async_copy(wd.at[:, 0, :, :, :, span[r]], made[r].at[:, 0], st_sem.at[0]),
                pltpu.make_async_copy(wd.at[:, 0, 0, :, :, span[r]], ab(bl[r], r, every, 0, 0), st_sem.at[1])]

    parts = (pl.ds(0, chunks // 2), pl.ds(chunks // 2, chunks - chunks // 2))

    def b0_copy(r, part, s):
        k = parts[part]
        return remote(made[r].at[k, 0, s], ab(bl[r], r, k, 0, N - s), b0_send, b0_recv, peer(b_axis[r], s))

    def stage_copies(r, k):
        return [pltpu.make_async_copy(stage.at[others, :, :, :, span[r]], made[r].at[k, others], st_sem.at[0]),
                pltpu.make_async_copy(stage.at[others, 0, :, :, span[r]], ab(bl[r], r, k, others, 0), st_sem.at[1])]

    def b_copy(r, k, s):
        return remote(made[r].at[k, others, s], ab(bl[r], r, k, others, N - s), b_send, b_recv.at[k], peer(b_axis[r], s))

    def c_own(r, k):
        return pltpu.make_async_copy(bl[r].at[k, :, :, 0], at_c(z, r, k, 0), c_recv.at[k])

    def c_copy(r, k, s):
        return remote(bl[r].at[k, :, :, s], at_c(z, r, k, N - s), c_send, c_recv.at[k], peer(c_axis[r], s))

    def ec_own(r, k):
        return pltpu.make_async_copy(at_c(z, r, k, 0), ecl[r].at[k, :, :, 0], ec_recv.at[k])

    def ec_copy(r, k, s):
        return remote(at_c(z, r, k, s), ecl[r].at[k, :, :, N - s], ec_send, ec_recv.at[k], peer(c_axis[r], s))

    def ecx_own(r, o):
        return pltpu.make_async_copy(at_ca(z, r, last, 0, o), ab(ecl[r], r, last, o, every).at[:, 0], ecx_recv.at[o])

    def ecx_copy(r, o, s):
        return remote(at_ca(z, r, last, s, o), ab(ecl[r], r, last, o, every).at[:, N - s], ecx_send,
                      ecx_recv.at[o], peer(c_axis[r], s))

    def eb_copy(r, k, s):
        return remote(ab(ecl[r], r, k, every, s), ebl[r].at[k, :, N - s], eb_send, eb_recv.at[k], peer(b_axis[r], s))

    def ebx_own(r, o):
        return pltpu.make_async_copy(ab(ecl[r], r, last, o, 0), stage.at[o, 0, :, :, span[r]], ebx_recv.at[o])

    def ebx_copy(r, o, s):
        return remote(ab(ecl[r], r, last, o, s), stage.at[o, N - s, :, :, span[r]], ebx_send, ebx_recv.at[o], peer(b_axis[r], s))

    def ea_copy(r, o):
        return remote(al[r].at[o - 1], eal.at[3 - o, :, span[r]], ea_send, ea_recv, peer(a_axis[r], o))

    def load(r, k, b):
        src = ab(ecl[r], r, k, every, 0) if b == 0 else ebl[r].at[k, :, b]
        return pltpu.make_async_copy(src, wd.at[k, :, b, :, :, span[r]], ld_sem)

    def arrived(like, sem):
        remote(like, like, out_sem, sem, peer(0, 1)).wait_recv()

    def left(like, sem):
        remote(like, like, sem, out_sem, peer(0, 1)).wait_send()

    def up_copies(u):
        i, w = lax.rem(u, 3), pl.ds(pl.multiple_of(u * u_tile, u_tile), u_tile)
        return [pltpu.make_async_copy(sg_hbm.at[:, w], sg.at[i], s_sem.at[i, 0]),
                pltpu.make_async_copy(su_hbm.at[:, w], su.at[i], s_sem.at[i, 1])]

    def down_copy(u):
        i, w = lax.rem(u, 2), pl.ds(pl.multiple_of(u * u_tile, u_tile), u_tile)
        return pltpu.make_async_copy(sd_hbm.at[w, :], sd.at[i], s_sem.at[i, 2])

    def shared(u, beside=None):
        down_copy(u).start()
        @pl.when(u + 2 < units)
        def _():
            for c in up_copies(u + 2):
                c.start()
        with jax.named_scope("w_tile"):
            for c in up_copies(u):
                c.wait()
            @pl.when(u > 0)
            def _():
                down_copy(u - 1).wait()
        with jax.named_scope("tile"):
            i, old = lax.rem(u, 3), lax.rem(u + 1, 2)
            beside = beside or (lambda r: None)
            g = dot(xv[...], sg[i])
            beside(0)
            up = dot(xv[...], su[i])
            beside(1)
            acc[...] += dot(act[...], sd[old])
            act[...] = (jax.nn.silu(g) * up).astype(BF16)
            beside(2)

    def matches(r, o, first, count, weight):
        m = met.at[a_axis[r], o]
        code = m[:top].astype(jnp.int32)
        at = [(code >> (10 - 2 * axis)) & 3 for axis in range(3)]
        here = (code >= 0) & (at[a_axis[r]] == co[a_axis[r]])
        place = ((at[b_axis[r]] - co[b_axis[r]]) & 3) * 32 + ((at[c_axis[r]] - co[c_axis[r]]) & 3) * 8 + (code & 7)
        chunk = jnp.where(here, (code & 63) >> 3, -1)
        spread = lambda v, j: jnp.broadcast_to(v[j : j + 1], (16, tokens)).astype(BF16)[None]
        given = [spread(m[top:], j) for j in range(top)] if weight else [jnp.ones((1, 16, tokens), BF16)] * top
        row = (lax.broadcasted_iota(jnp.int32, (8, 16, tokens), 0) * 16 + lax.broadcasted_iota(jnp.int32, (8, 16, tokens), 1))
        row = row.astype(F32).astype(BF16)
        out = []
        for k in range(count):
            mine = jnp.where(chunk == first + k, place, -1).astype(F32)
            hit = jnp.zeros((8, 16, tokens), BF16)
            for j in range(top):
                hit = jnp.where(spread(mine, j) == row, given[j], hit)
            out.append(hit.reshape(128, tokens))
        return jnp.concatenate(out) if count > 1 else out[0]

    def gather(k, r):
        for o in (1, 3, 2):
            rows = dot(matches(r, o, k, 1, False), al[r][o - 1]).astype(BF16)
            stage[o, :, :, :, span[r]] = rows.reshape(N, N, SUB, cols[r])

    def keep(k):
        for r in range(3):
            for c in stage_copies(r, k):
                c.start()

    def dispatch(k):
        with jax.named_scope("w_stage"):
            for n, like in enumerate((stage.at[others], stage.at[others, 0])):
                pltpu.make_async_copy(like, like, st_sem.at[n]).wait()
        for r, s in HOPS:
            b_copy(r, k, s).start()

    def forward_c(k):
        with jax.named_scope("w_b"):
            arrived(z.at[k, others, others], b_recv.at[k])
        for r, s in HOPS:
            c_copy(r, k, s).start()
        for r in range(3):
            c_own(r, k).start()

    def forward_eb(k):
        with jax.named_scope("w_ec"):
            arrived(z.at[k], ec_recv.at[k])
        for r, s in HOPS:
            eb_copy(r, k, s).start()

    def forward_ebx(o):
        with jax.named_scope("w_ecx"):
            arrived(z.at[last, 0], ecx_recv.at[o])
        for r, s in HOPS:
            ebx_copy(r, o, s).start()
        for r in range(3):
            ebx_own(r, o).start()

    def weight_copy(which, k):
        if which == 2:
            return pltpu.make_async_copy(wd_hbm.at[k], wd.at[k], w_sem.at[2])
        w = pl.ds(pl.multiple_of(k * (d // 4), d // 4), d // 4)
        return pltpu.make_async_copy((wg_hbm, wu_hbm)[which].at[w], (wg, wu)[which].at[w], w_sem.at[which])

    pieces = (4, 4, chunks)
    rows = N * N * N * SUB

    def expert(k):
        with jax.named_scope("w_c"):
            arrived(z.at[k], c_recv.at[k])

        def up(f, _):
            for (ek, ef), event, arg in plan["main"]:
                pl.when((k == ek) & (f == ef))(functools.partial({"C": forward_c, "F": forward_eb}[event], arg))
            with jax.named_scope("up"):
                w = pl.ds(pl.multiple_of(f * f_tile, f_tile), f_tile)
                zk = z[k].reshape(rows, d)
                h[:, w] = (jax.nn.silu(dot(zk, wg[:, w])) * dot(zk, wu[:, w])).astype(BF16)
            return 0
        lax.fori_loop(0, ff // f_tile, up, 0)

        if plan["mid"]:
            @pl.when(any_of(k, plan["mid"]))
            def _():
                shared(plan["pre"] + before(k, plan["mid"]))

        @pl.when(k == 0)
        def _():
            with jax.named_scope("w_wd"):
                pltpu.make_async_copy(wd_hbm, wd, w_sem.at[2]).wait()

        at = 0
        for r in range(3):
            w = pl.ds(at, cfg["down"][r])
            at += cfg["down"][r]
            with jax.named_scope("down"):
                out = dot(h[...], wd[:, :, :, :, :, w].reshape(ff, cfg["down"][r]))
                z[k, :, :, :, :, w] = out.astype(BF16).reshape(N, N, N, SUB, cfg["down"][r])

            @pl.when(k < last)
            def _():
                for s in (1, 3, 2):
                    ec_copy(r, k, s).start()
                ec_own(r, k).start()

            @pl.when(k == last)
            def _():
                for o in ORDER:
                    for s in (1, 3, 2):
                        ecx_copy(r, o, s).start()
                    ecx_own(r, o).start()

    def held(r, o):
        wide = 128 * chunks
        return pl.ds(r * tokens, tokens), pl.ds(pl.multiple_of(o * wide, wide), wide)

    def weigh(i, r):
        o = ordered(i)
        wg[held(r, o)] = matches(r, o, 0, chunks, True).T

    def ordered(i):
        return jnp.where(i == 0, ORDER[0], jnp.where(i == 1, ORDER[1], jnp.where(i == 2, ORDER[2], ORDER[3])))

    def combine(i, _):
        o = ordered(i)
        with jax.named_scope("w_ebx"):
            arrived(stage.at[o], ebx_recv.at[o])
        for r in range(3):
            weight = wg[held(r, o)]
            early = wd[0:last, pl.ds(o, 1), :, :, :, span[r]].reshape(128 * last, cols[r])
            late = stage[pl.ds(o, 1), :, :, :, span[r]].reshape(128, cols[r])
            with jax.named_scope("m"):
                part = dot(weight[:, : 128 * last], early) + dot(weight[:, 128 * last :], late)

            @pl.when(o == 0)
            def _():
                acc[:, span[r]] += part

            @pl.when(o > 0)
            def _():
                al[r][pl.ds(o - 1, 1)] = part.astype(BF16)[None]
                ea_copy(r, o).start()
        return 0

    x_in = pltpu.make_async_copy(x_hbm, xv, x_sem)
    x_in.start()
    for u in range(2):
        for c in up_copies(u):
            c.start()
    code = jnp.where(slot_ref[...] < slots, expert_ref[...] * 64 + slot_ref[...], -1).astype(F32)
    for axis in range(3):
        met[axis, 0, :top] = code
        met[axis, 0, top:] = gate_ref[...]
    barrier = pltpu.get_barrier_semaphore()
    for axis in range(3):
        for s in (1, 2, 3):
            pl.semaphore_signal(barrier, inc=1, device_id=peer(axis, s), device_id_type=MESH)
    acc[...] = jnp.zeros_like(acc)
    act[...] = jnp.zeros_like(act)
    sd[1] = jnp.zeros_like(sd[1])
    with jax.named_scope("w_barrier"):
        pl.semaphore_wait(barrier, 9)
    for s in (1, 3, 2):
        for axis in range(3):
            m_copy(axis, s).start()
        for r in range(3 if s != 2 else 0):
            a_copy(r, s).start()
    x_in.wait()
    for r in range(3):
        mine = dot(matches(r, 0, 0, chunks, False), xv[:, span[r]]).astype(BF16)
        wd[:, 0, :, :, :, span[r]] = mine.reshape(chunks, N, N, SUB, cols[r])
    for r in range(3):
        for c in early_copies(r):
            c.start()

    pieces = (4, 4, chunks)

    def pre(i, _):
        gathers, forwards = plan["gather"], plan["forward"]
        for which, (at, each) in enumerate(plan["weights"]):
            @pl.when((i >= at) & (i < at + pieces[which] // each))
            def _():
                for n in range(each):
                    weight_copy(which, (i - at) * each + n).start()

        @pl.when(i == 1)
        def _():
            for n, like in enumerate((wd.at[:, 0], wd.at[:, 0, 0])):
                pltpu.make_async_copy(like, like, st_sem.at[n]).wait()
            for r, s in HOPS:
                b0_copy(r, 0, s).start()

        @pl.when(i == plan["relay"])
        def _():
            with jax.named_scope("w_a1"):
                arrived(eal.at[pl.ds(0, 2)], a_recv)
            for r, s in SIDES:
                relay(r, s).start()
            for r, s in HOPS:
                b0_copy(r, 1, s).start()

        @pl.when(any_of(i - 2, gathers))
        def _():
            dispatch(before(i - 2, gathers))

        @pl.when(i == gathers[0])
        def _():
            with jax.named_scope("w_a2"):
                arrived(met.at[:, others], m_recv)
                arrived(xv, r_recv)

        @pl.when(i == forwards[0])
        def _():
            with jax.named_scope("w_b0"):
                arrived(z.at[:, 0, others], b0_recv)
            left(xv, r_send)

        @pl.when(any_of(i, forwards))
        def _():
            forward_c(before(i, forwards))

        gathering = any_of(i, gathers)

        @pl.when(gathering)
        def _():
            k = before(i, gathers)
            shared(i, lambda r: gather(k, r))
            keep(k)

        @pl.when(jnp.logical_not(gathering))
        def _():
            shared(i)
        return 0
    lax.fori_loop(0, plan["pre"], pre, 0)
    pltpu.make_async_copy(wg_hbm, wg, w_sem.at[0]).wait()
    pltpu.make_async_copy(wu_hbm, wu, w_sem.at[1]).wait()
    lax.fori_loop(0, chunks, lambda k, _: (expert(k), 0)[1], 0)

    def fetch(ks):
        for k in ks:
            with jax.named_scope("w_eb"):
                arrived(z.at[k, :, others], eb_recv.at[k])
            for r in range(3):
                for b in range(4):
                    load(r, k, b).start()

    done = plan["pre"] + len(plan["mid"])

    def masks(i, _):
        @pl.when(i == plan["eb"])
        def _():
            forward_eb(last - 1)

        shared(i + done, lambda r: weigh(i, r))
        return 0
    lax.fori_loop(0, 4, masks, 0)

    def tail(i, _):
        @pl.when(i == plan["fetch"])
        def _():
            fetch(range(last - 1))

        @pl.when(i == plan["late"])
        def _():
            fetch([last - 1])

        for p, o in zip(plan["ebx"], ORDER, strict=True):
            pl.when(i == p)(functools.partial(forward_ebx, o))

        @pl.when(i == plan["sums"])
        def _():
            with jax.named_scope("w_load"):
                whole = wd.at[pl.ds(0, last)]
                pltpu.make_async_copy(whole, whole, ld_sem).wait()
            lax.fori_loop(0, 4, combine, 0)

        shared(i + done)
        return 0
    lax.fori_loop(4, units - done, tail, 0)
    down_copy(units - 1).wait()
    acc[...] += dot(act[...], sd[(units - 1) % 2])
    out = pltpu.make_async_copy(acc, sum_hbm, out_sem)
    out.start()
    with jax.named_scope("w_ea"):
        arrived(eal, ea_recv)

    early, end = pl.ds(0, last), pl.ds(last, 1)
    left(met.at[:, others], m_send)
    left(eal.at[pl.ds(0, 2)], a_send)
    left(z.at[:, 0, others], b0_send)
    left(z.at[:, others, others], b_send)
    left(z.at[:, :, :, others], c_send)
    left(z.at[early, :, :, others], ec_send)
    left(z.at[end, :, :, others], ecx_send)
    left(z.at[early, :, others], eb_send)
    left(z.at[end, :, others], ebx_send)
    left(eal, ea_send)
    with jax.named_scope("w_out"):
        out.wait()


def layer(x, expert, slot, gate, w_gate, w_up, w_down, s_gate, s_up, s_down, cfg):
    tokens, chunks, cols, ff, u_tile, top = (cfg[n] for n in ("tokens", "chunks", "cols", "ff", "u_tile", "top"))
    d, rows = sum(cols), N * N * N * SUB
    hbm, vm = pl.BlockSpec(memory_space=pl.ANY), pl.BlockSpec(memory_space=pltpu.VMEM)
    block = lambda w: jax.ShapeDtypeStruct((chunks, N, N, N, SUB, w), BF16)
    dma = pltpu.SemaphoreType.DMA
    outs = pl.pallas_call(
        functools.partial(kernel, cfg),
        out_shape=[jax.ShapeDtypeStruct((tokens, d), F32), jax.ShapeDtypeStruct((3, tokens, d), BF16)]
        + [block(w) for _ in range(4) for w in cols],
        in_specs=[hbm] + [vm] * 3 + [hbm] * 6,
        out_specs=[hbm] * 14,
        scratch_shapes=[
            pltpu.VMEM((tokens, d), BF16),
            *[pltpu.VMEM((3, tokens, w), BF16) for w in cols],
            pltpu.VMEM((3, 4, 2 * top, tokens), F32),
            pltpu.VMEM((N, N, N, SUB, d), BF16),
            pltpu.VMEM((d, ff), BF16),
            pltpu.VMEM((d, ff), BF16),
            pltpu.VMEM((chunks, N, N, N, SUB, d), BF16),
            pltpu.VMEM((chunks, N, N, N, SUB, d), BF16),
            pltpu.VMEM((rows, ff), BF16),
            pltpu.VMEM((tokens, d), F32),
            pltpu.VMEM((3, d, u_tile), BF16),
            pltpu.VMEM((3, d, u_tile), BF16),
            pltpu.VMEM((2, u_tile, d), BF16),
            pltpu.VMEM((tokens, u_tile), BF16),
            dma(()), dma((3,)), dma((3, 3)), dma((2,)), dma(()),
            *[dma(())] * 8,
            *[dma(()), dma((chunks,))] * 3,
            dma(()), dma((4,)), dma(()), dma((chunks,)), dma(()), dma((4,)),
            *[dma(())] * 3,
        ],
        compiler_params=pltpu.CompilerParams(collective_id=0, has_side_effects=True, vmem_limit_bytes=cfg["vmem"]),
        name="moe_layer",
    )(x, expert, slot, gate, w_gate, w_up, w_down.reshape(chunks, N, N, N, SUB, d), s_gate, s_up, s_down)
    total, sums = outs[:2]
    for o in range(3):
        total += sums[o].astype(F32)
    return total.astype(BF16)


PLAN = {
    "pre": 19, "relay": 5, "gather": (8, 10, 12, 14, 16), "forward": (13, 16, 18), "mid": (0, 2),
    "weights": ((3, 1), (8, 1), (14, 1)),
    "main": (((0, 3), "C", 3), ((1, 1), "C", 4), ((2, 2), "F", 0), ((3, 1), "F", 1), ((4, 1), "F", 2)),
    "eb": 0, "ebx": (5, 6, 7, 8), "fetch": 8, "late": 9, "sums": 10,
}


def configure(x, expert, w_gate, s_gate):
    tokens, d = x.shape[-2:]
    top, ff, width, experts = expert.shape[-1], w_gate.shape[-1], s_gate.shape[-1], N * N * N
    slots = 5 * tokens * top // (4 * experts)
    lanes = d // 128
    cols = tuple(128 * ((lanes + 2 - r) // 3) for r in range(3))
    return dict(tokens=tokens, top=top, slots=slots, chunks=slots // SUB, cols=cols, ff=ff, f_tile=512, down=(768, 512, 512),
                units=width // 512, u_tile=512, plan=PLAN, vmem=67043328)


TEST = dict(
    cols=(256, 256, 128), down=(256, 256, 128),
    plan={"pre": 7, "relay": 1, "weights": ((0, 4), (1, 4), (2, 2)), "gather": (2, 4), "forward": (6,), "mid": (0,),
          "main": (((0, 1), "C", 1),), "eb": 0, "ebx": (4, 4, 4, 4), "fetch": 4, "late": 4, "sums": 4})


def solution(mesh):
    def step(x, expert, slot, gate, w_gate, w_up, w_down, s_gate, s_up, s_down):
        cfg = configure(x, expert, w_gate, s_gate)
        y = layer(x[0, 0], expert[0, 0].T, slot[0, 0].T, gate[0, 0].T, w_gate[0], w_up[0], w_down[0], s_gate, s_up, s_down, cfg)
        return y[None, None]

    tok, own, whole = P("dp", "ep", None, None), P("ep", None, None), P(None, None)
    return jax.shard_map(step, mesh=mesh, in_specs=(tok,) * 4 + (own,) * 3 + (whole,) * 3, out_specs=tok, check_vma=False)
```

```python
import functools

import jax
import jax.numpy as jnp
from jax import lax
from jax.experimental import pallas as pl
from jax.experimental.pallas import tpu as pltpu
from jax.sharding import PartitionSpec as P

MESH = pl.DeviceIdType.MESH
N = 4
STRIDE = (16, 4, 1)
TURNS = ((0, 1, 2), (1, 2, 0), (2, 0, 1))
SUB = 8
ORDER = (2, 1, 3, 0)
HOPS = tuple((r, s) for s in (1, 3, 2) for r in range(3))
SIDES = tuple((r, s) for s in (1, 3) for r in range(3))
F32, BF16 = jnp.float32, jnp.bfloat16


def dot(a, b):
    return jnp.dot(a, b, preferred_element_type=F32)


def any_of(i, places):
    hit = i == places[0]
    for p in places[1:]:
        hit = hit | (i == p)
    return hit


def before(i, places):
    return sum((i > p).astype(jnp.int32) for p in places)


def kernel(cfg, *refs):
    tokens, chunks, cols, ff, f_tile, units, u_tile, top, slots, plan = (
        cfg[n] for n in ("tokens", "chunks", "cols", "ff", "f_tile", "units", "u_tile", "top", "slots", "plan"))
    it = iter(refs)
    take = lambda n: [next(it) for _ in range(n)]
    x_hbm, expert_hbm, slot_hbm, gate_hbm, wg_hbm, wu_hbm, wd_hbm, sg_hbm, su_hbm, sd_hbm = take(10)
    sum_hbm, eal = take(2)
    made, bl, ecl, ebl = take(3), take(3), take(3), take(3)
    (xv,) = take(1)
    al = take(3)
    met, stage, wg, wu, wd, z, h, acc, sg, su, sd, act, expert_ref, slot_ref, gate_ref = take(15)
    (x_sem, w_sem, s_sem, st_sem, out_sem, a_send, a_recv, r_send, r_recv, m_send, m_recv, b0_send, b0_recv, b_send, b_recv,
     c_send, c_recv, ec_send, ec_recv, ecx_send, ecx_recv, eb_send, eb_recv,
     ebx_send, ebx_recv, ld_sem, ea_send, ea_recv) = take(28)

    me = lax.axis_index("ep")
    co = (me // 16, lax.rem(me // 4, 4), lax.rem(me, 4))
    starts = [sum(cols[:r]) for r in range(3)]
    span = [pl.ds(starts[r], cols[r]) for r in range(3)]
    d, last = sum(cols), chunks - 1
    a_axis, b_axis, c_axis = ([t[i] for t in TURNS] for i in range(3))

    def hop(c, s):
        return lax.rem(c + s, N)

    def peer(axis, s):
        return {"ep": me + (hop(co[axis], s) - co[axis]) * STRIDE[axis]}

    def remote(src, dst, send, recv, to):
        return pltpu.make_async_remote_copy(
            src_ref=src, dst_ref=dst, send_sem=send, recv_sem=recv, device_id=to, device_id_type=MESH)

    def ab(ref, r, k, a, b):
        return ref.at[k, b, a] if a_axis[r] > b_axis[r] else ref.at[k, a, b]

    def at_c(ref, r, k, c):
        if c_axis[r] == 0:
            return ref.at[k, c, :, :, :, span[r]]
        if c_axis[r] == 1:
            return ref.at[k, :, c, :, :, span[r]]
        return ref.at[k, :, :, c, :, span[r]]

    def at_ca(ref, r, k, c, a):
        ix = {c_axis[r]: c, a_axis[r]: a, b_axis[r]: slice(None)}
        return ref.at[k, ix[0], ix[1], ix[2], :, span[r]]

    every, others = slice(None), pl.ds(1, 3)

    def a_copy(r, s):
        return remote(x_hbm.at[:, span[r]], al[r].at[3 - s], a_send, a_recv, peer(a_axis[r], s))

    def relay(r, s):
        half = pl.ds(0 if s == 1 else tokens // 2, tokens // 2)
        return remote(al[r].at[3 - s, half], al[r].at[1, half], r_send, r_recv, peer(a_axis[r], s))

    def m_copy(axis, s):
        return remote(met.at[axis, 0], met.at[axis, N - s], m_send, m_recv, peer(axis, s))

    def early_copies(r):
        return [pltpu.make_async_copy(wd.at[:, 0, :, :, :, span[r]], made[r].at[:, 0], st_sem.at[0]),
                pltpu.make_async_copy(wd.at[:, 0, 0, :, :, span[r]], ab(bl[r], r, every, 0, 0), st_sem.at[1])]

    parts = (pl.ds(0, chunks // 2), pl.ds(chunks // 2, chunks - chunks // 2))

    def b0_copy(r, part, s):
        k = parts[part]
        return remote(made[r].at[k, 0, s], ab(bl[r], r, k, 0, N - s), b0_send, b0_recv, peer(b_axis[r], s))

    def stage_copies(r, k):
        return [pltpu.make_async_copy(stage.at[others, :, :, :, span[r]], made[r].at[k, others], st_sem.at[0]),
                pltpu.make_async_copy(stage.at[others, 0, :, :, span[r]], ab(bl[r], r, k, others, 0), st_sem.at[1])]

    def b_copy(r, k, s):
        return remote(made[r].at[k, others, s], ab(bl[r], r, k, others, N - s), b_send, b_recv.at[k], peer(b_axis[r], s))

    def c_own(r, k):
        return pltpu.make_async_copy(bl[r].at[k, :, :, 0], at_c(z, r, k, 0), c_recv.at[k])

    def c_copy(r, k, s):
        return remote(bl[r].at[k, :, :, s], at_c(z, r, k, N - s), c_send, c_recv.at[k], peer(c_axis[r], s))

    def ec_own(r, k):
        return pltpu.make_async_copy(at_c(z, r, k, 0), ecl[r].at[k, :, :, 0], ec_recv.at[k])

    def ec_copy(r, k, s):
        return remote(at_c(z, r, k, s), ecl[r].at[k, :, :, N - s], ec_send, ec_recv.at[k], peer(c_axis[r], s))

    def ecx_own(r, o):
        return pltpu.make_async_copy(at_ca(z, r, last, 0, o), ab(ecl[r], r, last, o, every).at[:, 0], ecx_recv.at[o])

    def ecx_copy(r, o, s):
        return remote(at_ca(z, r, last, s, o), ab(ecl[r], r, last, o, every).at[:, N - s], ecx_send,
                      ecx_recv.at[o], peer(c_axis[r], s))

    def eb_copy(r, k, s):
        return remote(ab(ecl[r], r, k, every, s), ebl[r].at[k, :, N - s], eb_send, eb_recv.at[k], peer(b_axis[r], s))

    def ebx_own(r, o):
        return pltpu.make_async_copy(ab(ecl[r], r, last, o, 0), stage.at[o, 0, :, :, span[r]], ebx_recv.at[o])

    def ebx_copy(r, o, s):
        return remote(ab(ecl[r], r, last, o, s), stage.at[o, N - s, :, :, span[r]], ebx_send, ebx_recv.at[o], peer(b_axis[r], s))

    def ea_copy(r, o):
        return remote(al[r].at[o - 1], eal.at[3 - o, :, span[r]], ea_send, ea_recv, peer(a_axis[r], o))

    def load(r, k, b):
        src = ab(ecl[r], r, k, every, 0) if b == 0 else ebl[r].at[k, :, b]
        return pltpu.make_async_copy(src, wd.at[k, :, b, :, :, span[r]], ld_sem)

    def arrived(like, sem):
        remote(like, like, out_sem, sem, peer(0, 1)).wait_recv()

    def left(like, sem):
        remote(like, like, sem, out_sem, peer(0, 1)).wait_send()

    def up_copies(u):
        i, w = lax.rem(u, 3), pl.ds(pl.multiple_of(u * u_tile, u_tile), u_tile)
        return [pltpu.make_async_copy(sg_hbm.at[:, w], sg.at[i], s_sem.at[i, 0]),
                pltpu.make_async_copy(su_hbm.at[:, w], su.at[i], s_sem.at[i, 1])]

    def down_copy(u):
        i, w = lax.rem(u, 2), pl.ds(pl.multiple_of(u * u_tile, u_tile), u_tile)
        return pltpu.make_async_copy(sd_hbm.at[w, :], sd.at[i], s_sem.at[i, 2])

    def shared(u, beside=None):
        down_copy(u).start()
        @pl.when(u + 2 < units)
        def _():
            for c in up_copies(u + 2):
                c.start()
        with jax.named_scope("w_tile"):
            for c in up_copies(u):
                c.wait()
            @pl.when(u > 0)
            def _():
                down_copy(u - 1).wait()
        with jax.named_scope("tile"):
            i, old = lax.rem(u, 3), lax.rem(u + 1, 2)
            beside = beside or (lambda r: None)
            g = dot(xv[...], sg[i])
            beside(0)
            up = dot(xv[...], su[i])
            beside(1)
            acc[...] += dot(act[...], sd[old])
            act[...] = (jax.nn.silu(g) * up).astype(BF16)
            beside(2)

    def matches(r, o, first, count, weight):
        m = met.at[a_axis[r], o]
        code = m[:top].astype(jnp.int32)
        at = [(code >> (10 - 2 * axis)) & 3 for axis in range(3)]
        here = (code >= 0) & (at[a_axis[r]] == co[a_axis[r]])
        place = ((at[b_axis[r]] - co[b_axis[r]]) & 3) * 32 + ((at[c_axis[r]] - co[c_axis[r]]) & 3) * 8 + (code & 7)
        chunk = jnp.where(here, (code & 63) >> 3, -1)
        spread = lambda v, j: jnp.broadcast_to(v[j : j + 1], (16, tokens)).astype(BF16)[None]
        given = [spread(m[top:], j) for j in range(top)] if weight else [jnp.ones((1, 16, tokens), BF16)] * top
        row = (lax.broadcasted_iota(jnp.int32, (8, 16, tokens), 0) * 16 + lax.broadcasted_iota(jnp.int32, (8, 16, tokens), 1))
        row = row.astype(F32).astype(BF16)
        out = []
        for k in range(count):
            mine = jnp.where(chunk == first + k, place, -1).astype(F32)
            hit = jnp.zeros((8, 16, tokens), BF16)
            for j in range(top):
                hit = jnp.where(spread(mine, j) == row, given[j], hit)
            out.append(hit.reshape(128, tokens))
        return jnp.concatenate(out) if count > 1 else out[0]

    def gather(k, r):
        for o in (1, 3, 2):
            rows = dot(matches(r, o, k, 1, False), al[r][o - 1]).astype(BF16)
            stage[o, :, :, :, span[r]] = rows.reshape(N, N, SUB, cols[r])

    def keep(k):
        for r in range(3):
            for c in stage_copies(r, k):
                c.start()

    def dispatch(k):
        with jax.named_scope("w_stage"):
            for n, like in enumerate((stage.at[others], stage.at[others, 0])):
                pltpu.make_async_copy(like, like, st_sem.at[n]).wait()
        for r, s in HOPS:
            b_copy(r, k, s).start()

    def forward_c(k):
        with jax.named_scope("w_b"):
            arrived(z.at[k, others, others], b_recv.at[k])
        for r, s in HOPS:
            c_copy(r, k, s).start()
        for r in range(3):
            c_own(r, k).start()

    def forward_eb(k):
        with jax.named_scope("w_ec"):
            arrived(z.at[k], ec_recv.at[k])
        for r, s in HOPS:
            eb_copy(r, k, s).start()

    def forward_ebx(o):
        with jax.named_scope("w_ecx"):
            arrived(z.at[last, 0], ecx_recv.at[o])
        for r, s in HOPS:
            ebx_copy(r, o, s).start()
        for r in range(3):
            ebx_own(r, o).start()

    f_tiles = ff // f_tile

    def tile_copies(f):
        w = pl.ds(pl.multiple_of(f * f_tile, f_tile), f_tile)
        return [pltpu.make_async_copy(wg_hbm.at[:, w], wg.at[:, w], w_sem.at[f]), pltpu.make_async_copy(wu_hbm.at[:, w], wu.at[:, w], w_sem.at[f])]

    def wd_copy(k):
        return pltpu.make_async_copy(wd_hbm.at[k], wd.at[k], w_sem.at[f_tiles])

    rows = N * N * N * SUB

    def expert(k):
        with jax.named_scope("w_c"):
            arrived(z.at[k], c_recv.at[k])

        def up(f, _):
            @pl.when(k == 0)
            def _():
                @pl.when(f + 2 < f_tiles)
                def _():
                    for c in tile_copies(f + 2):
                        c.start()

                @pl.when(f < chunks)
                def _():
                    wd_copy(f).start()
                like = wg.at[:, pl.ds(0, 2 * f_tile)]
                with jax.named_scope("w_wgu"):
                    pltpu.make_async_copy(like, like, w_sem.at[f]).wait()
            for (ek, ef), event, arg in plan["main"]:
                pl.when((k == ek) & (f == ef))(functools.partial({"C": forward_c, "F": forward_eb}[event], arg))
            with jax.named_scope("up"):
                w = pl.ds(pl.multiple_of(f * f_tile, f_tile), f_tile)
                zk = z[k].reshape(rows, d)
                h[:, w] = (jax.nn.silu(dot(zk, wg[:, w])) * dot(zk, wu[:, w])).astype(BF16)
            return 0
        lax.fori_loop(0, ff // f_tile, up, 0)

        if plan["mid"]:
            @pl.when(any_of(k, plan["mid"]))
            def _():
                shared(plan["pre"] + before(k, plan["mid"]))

        @pl.when(k == 0)
        def _():
            with jax.named_scope("w_wd"):
                pltpu.make_async_copy(wd_hbm, wd, w_sem.at[f_tiles]).wait()

        at = 0
        for r in range(3):
            w = pl.ds(at, cfg["down"][r])
            at += cfg["down"][r]
            with jax.named_scope("down"):
                out = dot(h[...], wd[:, :, :, :, :, w].reshape(ff, cfg["down"][r]))
                z[k, :, :, :, :, w] = out.astype(BF16).reshape(N, N, N, SUB, cfg["down"][r])

            @pl.when(k < last)
            def _():
                for s in (1, 3, 2):
                    ec_copy(r, k, s).start()
                ec_own(r, k).start()

            @pl.when(k == last)
            def _():
                for o in ORDER:
                    for s in (1, 3, 2):
                        ecx_copy(r, o, s).start()
                    ecx_own(r, o).start()

    def held(r, o):
        wide = 128 * chunks
        return pl.ds(r * tokens, tokens), pl.ds(pl.multiple_of(o * wide, wide), wide)

    def weigh(i, r):
        o = ordered(i)
        wg[held(r, o)] = matches(r, o, 0, chunks, True).T

    def ordered(i):
        return jnp.where(i == 0, ORDER[0], jnp.where(i == 1, ORDER[1], jnp.where(i == 2, ORDER[2], ORDER[3])))

    def combine(i, _):
        o = ordered(i)
        with jax.named_scope("w_ebx"):
            arrived(stage.at[o], ebx_recv.at[o])
        for r in range(3):
            weight = wg[held(r, o)]
            early = wd[0:last, pl.ds(o, 1), :, :, :, span[r]].reshape(128 * last, cols[r])
            late = stage[pl.ds(o, 1), :, :, :, span[r]].reshape(128, cols[r])
            with jax.named_scope("m"):
                part = dot(weight[:, : 128 * last], early) + dot(weight[:, 128 * last :], late)

            @pl.when(o == 0)
            def _():
                acc[:, span[r]] += part

            @pl.when(o > 0)
            def _():
                al[r][pl.ds(o - 1, 1)] = part.astype(BF16)[None]
                ea_copy(r, o).start()
        return 0

    barrier = pltpu.get_barrier_semaphore()
    for axis in range(3):
        for s in (1, 2, 3):
            pl.semaphore_signal(barrier, inc=1, device_id=peer(axis, s), device_id_type=MESH)
    routing = [pltpu.make_async_copy(a, b, x_sem.at[1]) for a, b in ((expert_hbm, expert_ref), (slot_hbm, slot_ref), (gate_hbm, gate_ref))]
    x_in = pltpu.make_async_copy(x_hbm, xv, x_sem.at[0])
    for c in (*routing, x_in):
        c.start()
    for u in range(2):
        for c in up_copies(u):
            c.start()
    acc[...] = jnp.zeros_like(acc)
    act[...] = jnp.zeros_like(act)
    sd[1] = jnp.zeros_like(sd[1])
    for c in routing:
        c.wait()
    code = jnp.where(slot_ref[...] < slots, expert_ref[...] * 64 + slot_ref[...], -1).astype(F32)
    for axis in range(3):
        met[axis, 0, :top] = code
        met[axis, 0, top:] = gate_ref[...]
    x_in.wait()
    with jax.named_scope("w_barrier"):
        pl.semaphore_wait(barrier, 9)
    for r, s in SIDES:
        a_copy(r, s).start()
    for s in (1, 3, 2):
        for axis in range(3):
            m_copy(axis, s).start()

    def own_rows(r):
        mine = dot(matches(r, 0, 0, chunks, False), xv[:, span[r]]).astype(BF16)
        wd[:, 0, :, :, :, span[r]] = mine.reshape(chunks, N, N, SUB, cols[r])

    shared(0, own_rows)
    for r in range(3):
        for c in early_copies(r):
            c.start()

    def pre(i, _):
        gathers, forwards = plan["gather"], plan["forward"]
        for f, at in enumerate(plan["weights"]):
            @pl.when(i == at)
            def _():
                for c in tile_copies(f):
                    c.start()

        @pl.when(i == 2)
        def _():
            for n, like in enumerate((wd.at[:, 0], wd.at[:, 0, 0])):
                pltpu.make_async_copy(like, like, st_sem.at[n]).wait()
            for r, s in HOPS:
                b0_copy(r, 0, s).start()

        @pl.when(i == plan["relay"])
        def _():
            with jax.named_scope("w_a1"):
                arrived(eal.at[pl.ds(0, 2)], a_recv)
            for r, s in SIDES:
                relay(r, s).start()
            for r, s in HOPS:
                b0_copy(r, 1, s).start()

        @pl.when(any_of(i - 2, gathers))
        def _():
            dispatch(before(i - 2, gathers))

        @pl.when(i == gathers[0])
        def _():
            with jax.named_scope("w_a2"):
                arrived(met.at[:, others], m_recv)
                arrived(xv, r_recv)

        @pl.when(i == forwards[0])
        def _():
            with jax.named_scope("w_b0"):
                arrived(z.at[:, 0, others], b0_recv)
            left(xv, r_send)

        @pl.when(any_of(i, forwards))
        def _():
            forward_c(before(i, forwards))

        gathering = any_of(i, gathers)

        @pl.when(gathering)
        def _():
            k = before(i, gathers)
            shared(i, lambda r: gather(k, r))
            keep(k)

        @pl.when(jnp.logical_not(gathering))
        def _():
            shared(i)
        return 0
    lax.fori_loop(1, plan["pre"], pre, 0)
    lax.fori_loop(0, chunks, lambda k, _: (expert(k), 0)[1], 0)

    def fetch(ks):
        for k in ks:
            with jax.named_scope("w_eb"):
                arrived(z.at[k, :, others], eb_recv.at[k])
            for r in range(3):
                for b in range(4):
                    load(r, k, b).start()

    done = plan["pre"] + len(plan["mid"])

    def masks(i, _):
        @pl.when(i == plan["eb"])
        def _():
            forward_eb(last - 1)

        shared(i + done, lambda r: weigh(i, r))
        return 0
    lax.fori_loop(0, 4, masks, 0)

    def tail(i, _):
        @pl.when(i == plan["fetch"])
        def _():
            fetch(range(last - 1))

        @pl.when(i == plan["late"])
        def _():
            fetch([last - 1])

        for p, o in zip(plan["ebx"], ORDER, strict=True):
            pl.when(i == p)(functools.partial(forward_ebx, o))

        @pl.when(i == plan["sums"])
        def _():
            with jax.named_scope("w_load"):
                whole = wd.at[pl.ds(0, last)]
                pltpu.make_async_copy(whole, whole, ld_sem).wait()
            lax.fori_loop(0, 4, combine, 0)

        shared(i + done)
        return 0
    lax.fori_loop(4, units - done, tail, 0)
    down_copy(units - 1).wait()
    outs = [pltpu.make_async_copy(acc.at[:, span[r]], sum_hbm.at[:, span[r]], out_sem) for r in range(3)]
    for r in range(3):
        acc[:, span[r]] += dot(act[...], sd[(units - 1) % 2, :, span[r]])
        outs[r].start()
    with jax.named_scope("w_ea"):
        arrived(eal, ea_recv)

    early, end = pl.ds(0, last), pl.ds(last, 1)
    left(met.at[:, others], m_send)
    left(eal.at[pl.ds(0, 2)], a_send)
    left(z.at[:, 0, others], b0_send)
    left(z.at[:, others, others], b_send)
    left(z.at[:, :, :, others], c_send)
    left(z.at[early, :, :, others], ec_send)
    left(z.at[end, :, :, others], ecx_send)
    left(z.at[early, :, others], eb_send)
    left(z.at[end, :, others], ebx_send)
    left(eal, ea_send)
    with jax.named_scope("w_out"):
        pltpu.make_async_copy(acc, sum_hbm, out_sem).wait()


def layer(x, expert, slot, gate, w_gate, w_up, w_down, s_gate, s_up, s_down, cfg):
    tokens, chunks, cols, ff, u_tile, top = (cfg[n] for n in ("tokens", "chunks", "cols", "ff", "u_tile", "top"))
    d, rows = sum(cols), N * N * N * SUB
    hbm = pl.BlockSpec(memory_space=pl.ANY)
    block = lambda w: jax.ShapeDtypeStruct((chunks, N, N, N, SUB, w), BF16)
    dma = pltpu.SemaphoreType.DMA
    outs = pl.pallas_call(
        functools.partial(kernel, cfg),
        out_shape=[jax.ShapeDtypeStruct((tokens, d), F32), jax.ShapeDtypeStruct((3, tokens, d), BF16)]
        + [block(w) for _ in range(4) for w in cols],
        in_specs=[hbm] * 10,
        out_specs=[hbm] * 14,
        scratch_shapes=[
            pltpu.VMEM((tokens, d), BF16),
            *[pltpu.VMEM((3, tokens, w), BF16) for w in cols],
            pltpu.VMEM((3, 4, 2 * top, tokens), F32),
            pltpu.VMEM((N, N, N, SUB, d), BF16),
            pltpu.VMEM((d, ff), BF16),
            pltpu.VMEM((d, ff), BF16),
            pltpu.VMEM((chunks, N, N, N, SUB, d), BF16),
            pltpu.VMEM((chunks, N, N, N, SUB, d), BF16),
            pltpu.VMEM((rows, ff), BF16),
            pltpu.VMEM((tokens, d), F32),
            pltpu.VMEM((3, d, u_tile), BF16),
            pltpu.VMEM((3, d, u_tile), BF16),
            pltpu.VMEM((2, u_tile, d), BF16),
            pltpu.VMEM((tokens, u_tile), BF16),
            pltpu.VMEM((top, tokens), jnp.int32),
            pltpu.VMEM((top, tokens), jnp.int32),
            pltpu.VMEM((top, tokens), F32),
            dma((2,)), dma((ff // cfg["f_tile"] + 1,)), dma((3, 3)), dma((2,)), dma(()),
            *[dma(())] * 8,
            *[dma(()), dma((chunks,))] * 3,
            dma(()), dma((4,)), dma(()), dma((chunks,)), dma(()), dma((4,)),
            *[dma(())] * 3,
        ],
        compiler_params=pltpu.CompilerParams(collective_id=0, has_side_effects=True, vmem_limit_bytes=cfg["vmem"]),
        name="moe_layer",
    )(x, expert, slot, gate, w_gate, w_up, w_down.reshape(chunks, N, N, N, SUB, d), s_gate, s_up, s_down)
    total, sums = outs[:2]
    for o in range(3):
        total += sums[o].astype(F32)
    return total.astype(BF16)


PLAN = {
    "pre": 22, "relay": 4, "gather": (9, 11, 13, 15, 17), "forward": (15,), "mid": (),
    "weights": (17, 19),
    "main": (((0, 0), "C", 1), ((0, 3), "C", 2), ((1, 2), "C", 3), ((2, 0), "C", 4),
             ((2, 2), "F", 0), ((3, 1), "F", 1), ((4, 1), "F", 2)),
    "eb": 0, "ebx": (5, 5, 6, 7), "fetch": 7, "late": 8, "sums": 10,
}


def configure(x, expert, w_gate, s_gate):
    tokens, d = x.shape[-2:]
    top, ff, width, experts = expert.shape[-1], w_gate.shape[-1], s_gate.shape[-1], N * N * N
    slots = 5 * tokens * top // (4 * experts)
    lanes = d // 128
    cols = tuple(128 * ((lanes + 2 - r) // 3) for r in range(3))
    return dict(tokens=tokens, top=top, slots=slots, chunks=slots // SUB, cols=cols, ff=ff, f_tile=512, down=(768, 512, 512),
                units=width // 512, u_tile=512, plan=PLAN, vmem=67043328)


TEST = dict(
    cols=(256, 256, 128), down=(256, 256, 128),
    plan={"pre": 7, "relay": 2, "weights": (3, 4), "gather": (2, 4), "forward": (6,), "mid": (0,),
          "main": (((0, 3), "C", 1),), "eb": 0, "ebx": (4, 4, 4, 4), "fetch": 4, "late": 4, "sums": 4})


def solution(mesh):
    def step(x, expert, slot, gate, w_gate, w_up, w_down, s_gate, s_up, s_down):
        cfg = configure(x, expert, w_gate, s_gate)
        y = layer(x[0, 0], expert[0, 0].T, slot[0, 0].T, gate[0, 0].T, w_gate[0], w_up[0], w_down[0], s_gate, s_up, s_down, cfg)
        return y[None, None]

    tok, own, whole = P("dp", "ep", None, None), P("ep", None, None), P(None, None)
    return jax.shard_map(step, mesh=mesh, in_specs=(tok,) * 4 + (own,) * 3 + (whole,) * 3, out_specs=tok, check_vma=False)
```

```python
import functools

import jax
import jax.numpy as jnp
from jax import lax
from jax.experimental import pallas as pl
from jax.experimental.pallas import tpu as pltpu
from jax.sharding import PartitionSpec as P

MESH = pl.DeviceIdType.MESH
N = 4
STRIDE = (16, 4, 1)
TURNS = ((0, 1, 2), (1, 2, 0), (2, 0, 1))
SUB = 8
ORDER = (2, 1, 3, 0)
HOPS = tuple((r, s) for s in (1, 3, 2) for r in range(3))
SIDES = tuple((r, s) for s in (1, 3) for r in range(3))
F32, BF16 = jnp.float32, jnp.bfloat16


def dot(a, b):
    return jnp.dot(a, b, preferred_element_type=F32)


def any_of(i, places):
    hit = i == places[0]
    for p in places[1:]:
        hit = hit | (i == p)
    return hit


def before(i, places):
    return sum((i > p).astype(jnp.int32) for p in places)


def kernel(cfg, *refs):
    tokens, chunks, cols, ff, f_tile, units, u_tile, top, slots, plan = (
        cfg[n] for n in ("tokens", "chunks", "cols", "ff", "f_tile", "units", "u_tile", "top", "slots", "plan"))
    it = iter(refs)
    take = lambda n: [next(it) for _ in range(n)]
    x_hbm, expert_hbm, slot_hbm, gate_hbm, wg_hbm, wu_hbm, wd_hbm, sg_hbm, su_hbm, sd_hbm = take(10)
    sum_hbm, eal = take(2)
    made, bl, ecl, ebl = take(3), take(3), take(3), take(3)
    (xv,) = take(1)
    al = take(3)
    met, stage, wg, wu, wd, z, h, acc, sg, su, sd, act, expert_ref, slot_ref, gate_ref = take(15)
    (x_sem, w_sem, s_sem, st_sem, out_sem, a_send, a_recv, r_send, r_recv, m_send, m_recv, b0_send, b0_recv, b_send, b_recv,
     c_send, c_recv, ec_send, ec_recv, ecx_send, ecx_recv, eb_send, eb_recv,
     ebx_send, ebx_recv, ld_sem, ea_send, ea_recv) = take(28)

    me = lax.axis_index("ep")
    co = (me // 16, lax.rem(me // 4, 4), lax.rem(me, 4))
    starts = [sum(cols[:r]) for r in range(3)]
    span = [pl.ds(starts[r], cols[r]) for r in range(3)]
    d, last = sum(cols), chunks - 1
    a_axis, b_axis, c_axis = ([t[i] for t in TURNS] for i in range(3))

    def hop(c, s):
        return lax.rem(c + s, N)

    def peer(axis, s):
        return {"ep": me + (hop(co[axis], s) - co[axis]) * STRIDE[axis]}

    def remote(src, dst, send, recv, to):
        return pltpu.make_async_remote_copy(
            src_ref=src, dst_ref=dst, send_sem=send, recv_sem=recv, device_id=to, device_id_type=MESH)

    def ab(ref, r, k, a, b):
        return ref.at[k, b, a] if a_axis[r] > b_axis[r] else ref.at[k, a, b]

    def at_c(ref, r, k, c):
        if c_axis[r] == 0:
            return ref.at[k, c, :, :, :, span[r]]
        if c_axis[r] == 1:
            return ref.at[k, :, c, :, :, span[r]]
        return ref.at[k, :, :, c, :, span[r]]

    def at_ca(ref, r, k, c, a):
        ix = {c_axis[r]: c, a_axis[r]: a, b_axis[r]: slice(None)}
        return ref.at[k, ix[0], ix[1], ix[2], :, span[r]]

    every, others = slice(None), pl.ds(1, 3)

    def a_copy(r, s):
        return remote(x_hbm.at[:, span[r]], al[r].at[3 - s], a_send, a_recv, peer(a_axis[r], s))

    def relay(r, s):
        half = pl.ds(0 if s == 1 else tokens // 2, tokens // 2)
        return remote(al[r].at[3 - s, half], al[r].at[1, half], r_send, r_recv, peer(a_axis[r], s))

    def m_copy(axis, s):
        return remote(met.at[axis, 0], met.at[axis, N - s], m_send, m_recv, peer(axis, s))

    def early_copies(r):
        return [pltpu.make_async_copy(wd.at[:, 0, :, :, :, span[r]], made[r].at[:, 0], st_sem.at[0]),
                pltpu.make_async_copy(wd.at[:, 0, 0, :, :, span[r]], ab(bl[r], r, every, 0, 0), st_sem.at[1])]

    parts = (pl.ds(0, 1), pl.ds(1, chunks - 1))

    def b0_copy(r, part, s):
        k = parts[part]
        return remote(made[r].at[k, 0, s], ab(bl[r], r, k, 0, N - s), b0_send.at[part], b0_recv.at[part], peer(b_axis[r], s))

    def stage_copies(r, k):
        return [pltpu.make_async_copy(stage.at[others, :, :, :, span[r]], made[r].at[k, others], st_sem.at[0]),
                pltpu.make_async_copy(stage.at[others, 0, :, :, span[r]], ab(bl[r], r, k, others, 0), st_sem.at[1])]

    def b_copy(r, k, s):
        return remote(made[r].at[k, others, s], ab(bl[r], r, k, others, N - s), b_send, b_recv.at[k], peer(b_axis[r], s))

    def c_own(r, k):
        return pltpu.make_async_copy(bl[r].at[k, :, :, 0], at_c(z, r, k, 0), c_recv.at[k])

    def c_copy(r, k, s):
        return remote(bl[r].at[k, :, :, s], at_c(z, r, k, N - s), c_send, c_recv.at[k], peer(c_axis[r], s))

    def ec_own(r, k):
        return pltpu.make_async_copy(at_c(z, r, k, 0), ecl[r].at[k, :, :, 0], ec_recv.at[k])

    def ec_copy(r, k, s):
        return remote(at_c(z, r, k, s), ecl[r].at[k, :, :, N - s], ec_send, ec_recv.at[k], peer(c_axis[r], s))

    def ecx_own(r, o):
        return pltpu.make_async_copy(at_ca(z, r, last, 0, o), ab(ecl[r], r, last, o, every).at[:, 0], ecx_recv.at[o])

    def ecx_copy(r, o, s):
        return remote(at_ca(z, r, last, s, o), ab(ecl[r], r, last, o, every).at[:, N - s], ecx_send,
                      ecx_recv.at[o], peer(c_axis[r], s))

    def eb_copy(r, k, s):
        return remote(ab(ecl[r], r, k, every, s), ebl[r].at[k, :, N - s], eb_send, eb_recv.at[k], peer(b_axis[r], s))

    def ebx_own(r, o):
        return pltpu.make_async_copy(ab(ecl[r], r, last, o, 0), stage.at[o, 0, :, :, span[r]], ebx_recv.at[o])

    def ebx_copy(r, o, s):
        return remote(ab(ecl[r], r, last, o, s), stage.at[o, N - s, :, :, span[r]], ebx_send, ebx_recv.at[o], peer(b_axis[r], s))

    def ea_copy(r, o):
        return remote(al[r].at[o - 1], eal.at[3 - o, :, span[r]], ea_send, ea_recv, peer(a_axis[r], o))

    def load(r, k, b):
        src = ab(ecl[r], r, k, every, 0) if b == 0 else ebl[r].at[k, :, b]
        return pltpu.make_async_copy(src, wd.at[k, :, b, :, :, span[r]], ld_sem)

    def arrived(like, sem):
        remote(like, like, out_sem, sem, peer(0, 1)).wait_recv()

    def left(like, sem):
        remote(like, like, sem, out_sem, peer(0, 1)).wait_send()

    def up_copies(u):
        i, w = lax.rem(u, 3), pl.ds(pl.multiple_of(u * u_tile, u_tile), u_tile)
        return [pltpu.make_async_copy(sg_hbm.at[:, w], sg.at[i], s_sem.at[i, 0]),
                pltpu.make_async_copy(su_hbm.at[:, w], su.at[i], s_sem.at[i, 1])]

    def down_copy(u):
        i, w = lax.rem(u, 2), pl.ds(pl.multiple_of(u * u_tile, u_tile), u_tile)
        return pltpu.make_async_copy(sd_hbm.at[w, :], sd.at[i], s_sem.at[i, 2])

    def shared(u, beside=None):
        down_copy(u).start()
        @pl.when(u + 2 < units)
        def _():
            for c in up_copies(u + 2):
                c.start()
        with jax.named_scope("w_tile"):
            for c in up_copies(u):
                c.wait()
            @pl.when(u > 0)
            def _():
                down_copy(u - 1).wait()
        with jax.named_scope("tile"):
            i, old = lax.rem(u, 3), lax.rem(u + 1, 2)
            beside = beside or (lambda r: None)
            g = dot(xv[...], sg[i])
            beside(0)
            up = dot(xv[...], su[i])
            beside(1)
            acc[...] += dot(act[...], sd[old])
            act[...] = (jax.nn.silu(g) * up).astype(BF16)
            beside(2)

    def matches(r, o, first, count, weight):
        m = met.at[a_axis[r], o]
        code = m[:top].astype(jnp.int32)
        at = [(code >> (10 - 2 * axis)) & 3 for axis in range(3)]
        here = (code >= 0) & (at[a_axis[r]] == co[a_axis[r]])
        place = ((at[b_axis[r]] - co[b_axis[r]]) & 3) * 32 + ((at[c_axis[r]] - co[c_axis[r]]) & 3) * 8 + (code & 7)
        chunk = jnp.where(here, (code & 63) >> 3, -1)
        spread = lambda v, j: jnp.broadcast_to(v[j : j + 1], (16, tokens)).astype(BF16)[None]
        given = [spread(m[top:], j) for j in range(top)] if weight else [jnp.ones((1, 16, tokens), BF16)] * top
        row = (lax.broadcasted_iota(jnp.int32, (8, 16, tokens), 0) * 16 + lax.broadcasted_iota(jnp.int32, (8, 16, tokens), 1))
        row = row.astype(F32).astype(BF16)
        out = []
        for k in range(count):
            mine = jnp.where(chunk == first + k, place, -1).astype(F32)
            hit = jnp.zeros((8, 16, tokens), BF16)
            for j in range(top):
                hit = jnp.where(spread(mine, j) == row, given[j], hit)
            out.append(hit.reshape(128, tokens))
        return jnp.concatenate(out) if count > 1 else out[0]

    def gather(k, r):
        for o in (1, 3, 2):
            rows = dot(matches(r, o, k, 1, False), al[r][o - 1]).astype(BF16)
            stage[o, :, :, :, span[r]] = rows.reshape(N, N, SUB, cols[r])

    def keep(k):
        for r in range(3):
            for c in stage_copies(r, k):
                c.start()

    def dispatch(k):
        with jax.named_scope("w_stage"):
            for n, like in enumerate((stage.at[others], stage.at[others, 0])):
                pltpu.make_async_copy(like, like, st_sem.at[n]).wait()
        for r, s in HOPS:
            b_copy(r, k, s).start()

    def forward_c(k):
        if k == 1:
            arrived(z.at[pl.ds(1, last), 0, others], b0_recv.at[1])
        with jax.named_scope("w_b"):
            arrived(z.at[k, others, others], b_recv.at[k])
        for r, s in HOPS:
            c_copy(r, k, s).start()
        for r in range(3):
            c_own(r, k).start()

    def forward_eb(k):
        with jax.named_scope("w_ec"):
            arrived(z.at[k], ec_recv.at[k])
        for r, s in HOPS:
            eb_copy(r, k, s).start()

    def forward_ebx(o):
        with jax.named_scope("w_ecx"):
            arrived(z.at[last, 0], ecx_recv.at[o])
        for r, s in HOPS:
            ebx_copy(r, o, s).start()
        for r in range(3):
            ebx_own(r, o).start()

    f_tiles = ff // f_tile

    def tile_copies(f):
        w = pl.ds(pl.multiple_of(f * f_tile, f_tile), f_tile)
        return [pltpu.make_async_copy(wg_hbm.at[:, w], wg.at[:, w], w_sem.at[f]), pltpu.make_async_copy(wu_hbm.at[:, w], wu.at[:, w], w_sem.at[f])]

    def wd_copy(k):
        return pltpu.make_async_copy(wd_hbm.at[k], wd.at[k], w_sem.at[f_tiles])

    rows = N * N * N * SUB

    def expert(k):
        with jax.named_scope("w_c"):
            arrived(z.at[k], c_recv.at[k])

        def up(f, _):
            @pl.when(k == 0)
            def _():
                @pl.when(f + 2 < f_tiles)
                def _():
                    for c in tile_copies(f + 2):
                        c.start()

                @pl.when(f < chunks)
                def _():
                    wd_copy(f).start()
                like = wg.at[:, pl.ds(0, 2 * f_tile)]
                with jax.named_scope("w_wgu"):
                    pltpu.make_async_copy(like, like, w_sem.at[f]).wait()
            for (ek, ef), event, arg in plan["main"]:
                pl.when((k == ek) & (f == ef))(functools.partial({"C": forward_c, "F": forward_eb}[event], arg))
            with jax.named_scope("up"):
                w = pl.ds(pl.multiple_of(f * f_tile, f_tile), f_tile)
                zk = z[k].reshape(rows, d)
                h[:, w] = (jax.nn.silu(dot(zk, wg[:, w])) * dot(zk, wu[:, w])).astype(BF16)
            return 0
        lax.fori_loop(0, ff // f_tile, up, 0)

        if plan["mid"]:
            @pl.when(any_of(k, plan["mid"]))
            def _():
                shared(plan["pre"] + before(k, plan["mid"]))

        @pl.when(k == 0)
        def _():
            with jax.named_scope("w_wd"):
                pltpu.make_async_copy(wd_hbm, wd, w_sem.at[f_tiles]).wait()

        at = 0
        for r in range(3):
            w = pl.ds(at, cfg["down"][r])
            at += cfg["down"][r]
            with jax.named_scope("down"):
                out = dot(h[...], wd[:, :, :, :, :, w].reshape(ff, cfg["down"][r]))
                z[k, :, :, :, :, w] = out.astype(BF16).reshape(N, N, N, SUB, cfg["down"][r])

            @pl.when(k < last)
            def _():
                for s in (1, 3, 2):
                    ec_copy(r, k, s).start()
                ec_own(r, k).start()

            @pl.when(k == last)
            def _():
                for o in ORDER:
                    for s in (1, 3, 2):
                        ecx_copy(r, o, s).start()
                    ecx_own(r, o).start()

    def held(r, o):
        wide = 128 * chunks
        return pl.ds(r * tokens, tokens), pl.ds(pl.multiple_of(o * wide, wide), wide)

    def weigh(i, r):
        o = ordered(i)
        wg[held(r, o)] = matches(r, o, 0, chunks, True).T

    def ordered(i):
        return jnp.where(i == 0, ORDER[0], jnp.where(i == 1, ORDER[1], jnp.where(i == 2, ORDER[2], ORDER[3])))

    def combine(i, _):
        o = ordered(i)
        with jax.named_scope("w_ebx"):
            arrived(stage.at[o], ebx_recv.at[o])
        for r in range(3):
            weight = wg[held(r, o)]
            early = wd[0:last, pl.ds(o, 1), :, :, :, span[r]].reshape(128 * last, cols[r])
            late = stage[pl.ds(o, 1), :, :, :, span[r]].reshape(128, cols[r])
            with jax.named_scope("m"):
                part = dot(weight[:, : 128 * last], early) + dot(weight[:, 128 * last :], late)

            @pl.when(o == 0)
            def _():
                acc[:, span[r]] += part

            @pl.when(o > 0)
            def _():
                al[r][pl.ds(o - 1, 1)] = part.astype(BF16)[None]
                ea_copy(r, o).start()
        return 0

    barrier = pltpu.get_barrier_semaphore()
    for axis in range(3):
        for s in (1, 2, 3):
            pl.semaphore_signal(barrier, inc=1, device_id=peer(axis, s), device_id_type=MESH)
    routing = [pltpu.make_async_copy(a, b, x_sem.at[1]) for a, b in ((expert_hbm, expert_ref), (slot_hbm, slot_ref), (gate_hbm, gate_ref))]
    x_in = pltpu.make_async_copy(x_hbm, xv, x_sem.at[0])
    for c in (*routing, x_in):
        c.start()
    for u in range(2):
        for c in up_copies(u):
            c.start()
    acc[...] = jnp.zeros_like(acc)
    act[...] = jnp.zeros_like(act)
    sd[1] = jnp.zeros_like(sd[1])
    for c in routing:
        c.wait()
    code = jnp.where(slot_ref[...] < slots, expert_ref[...] * 64 + slot_ref[...], -1).astype(F32)
    for axis in range(3):
        met[axis, 0, :top] = code
        met[axis, 0, top:] = gate_ref[...]
    x_in.wait()
    with jax.named_scope("w_barrier"):
        pl.semaphore_wait(barrier, 9)
    for r, s in SIDES:
        a_copy(r, s).start()
    for s in (1, 3, 2):
        for axis in range(3):
            m_copy(axis, s).start()

    def own_rows(r):
        mine = dot(matches(r, 0, 0, chunks, False), xv[:, span[r]]).astype(BF16)
        wd[:, 0, :, :, :, span[r]] = mine.reshape(chunks, N, N, SUB, cols[r])

    shared(0, own_rows)
    for r in range(3):
        for c in early_copies(r):
            c.start()

    def pre(i, _):
        gathers = plan["gather"]
        for f, at in enumerate(plan["weights"]):
            @pl.when(i == at)
            def _():
                for c in tile_copies(f):
                    c.start()

        @pl.when(i == plan["relay"])
        def _():
            for n, like in enumerate((wd.at[:, 0], wd.at[:, 0, 0])):
                pltpu.make_async_copy(like, like, st_sem.at[n]).wait()
            with jax.named_scope("w_a1"):
                arrived(eal.at[pl.ds(0, 2)], a_recv)
            for r, s in SIDES:
                relay(r, s).start()
            for r, s in HOPS:
                b0_copy(r, 0, s).start()

        @pl.when(i == plan["own"])
        def _():
            for r, s in HOPS:
                b0_copy(r, 1, s).start()

        @pl.when(i == gathers[0])
        def _():
            with jax.named_scope("w_a2"):
                arrived(met.at[:, others], m_recv)
                arrived(xv, r_recv)

        @pl.when(i == plan["forward"])
        def _():
            with jax.named_scope("w_b0"):
                arrived(z.at[0, 0, others], b0_recv.at[0])
            left(xv, r_send)
            forward_c(0)

        @pl.when(any_of(i - 2, gathers))
        def _():
            dispatch(before(i - 2, gathers))

        gathering = any_of(i, gathers)

        @pl.when(gathering)
        def _():
            k = before(i, gathers)
            shared(i, lambda r: gather(k, r))
            keep(k)

        @pl.when(jnp.logical_not(gathering))
        def _():
            shared(i)
        return 0
    lax.fori_loop(1, plan["pre"], pre, 0)
    lax.fori_loop(0, chunks, lambda k, _: (expert(k), 0)[1], 0)

    def fetch(ks):
        for k in ks:
            with jax.named_scope("w_eb"):
                arrived(z.at[k, :, others], eb_recv.at[k])
            for r in range(3):
                for b in range(4):
                    load(r, k, b).start()

    done = plan["pre"] + len(plan["mid"])

    def masks(i, _):
        @pl.when(i == plan["eb"])
        def _():
            forward_eb(last - 1)

        shared(i + done, lambda r: weigh(i, r))
        return 0
    lax.fori_loop(0, 4, masks, 0)

    def tail(i, _):
        @pl.when(i == plan["fetch"])
        def _():
            fetch(range(last - 1))

        @pl.when(i == plan["late"])
        def _():
            fetch([last - 1])

        for p, o in zip(plan["ebx"], ORDER, strict=True):
            pl.when(i == p)(functools.partial(forward_ebx, o))

        @pl.when(i == plan["sums"])
        def _():
            with jax.named_scope("w_load"):
                whole = wd.at[pl.ds(0, last)]
                pltpu.make_async_copy(whole, whole, ld_sem).wait()
            lax.fori_loop(0, 4, combine, 0)

        shared(i + done)
        return 0
    lax.fori_loop(4, units - done, tail, 0)
    down_copy(units - 1).wait()
    outs = [pltpu.make_async_copy(acc.at[:, span[r]], sum_hbm.at[:, span[r]], out_sem) for r in range(3)]
    for r in range(3):
        acc[:, span[r]] += dot(act[...], sd[(units - 1) % 2, :, span[r]])
        outs[r].start()
    with jax.named_scope("w_ea"):
        arrived(eal, ea_recv)

    early, end = pl.ds(0, last), pl.ds(last, 1)
    left(met.at[:, others], m_send)
    left(eal.at[pl.ds(0, 2)], a_send)
    left(z.at[0, 0, others], b0_send.at[0])
    left(z.at[pl.ds(1, last), 0, others], b0_send.at[1])
    left(z.at[:, others, others], b_send)
    left(z.at[:, :, :, others], c_send)
    left(z.at[early, :, :, others], ec_send)
    left(z.at[end, :, :, others], ecx_send)
    left(z.at[early, :, others], eb_send)
    left(z.at[end, :, others], ebx_send)
    left(eal, ea_send)
    with jax.named_scope("w_out"):
        pltpu.make_async_copy(acc, sum_hbm, out_sem).wait()


def layer(x, expert, slot, gate, w_gate, w_up, w_down, s_gate, s_up, s_down, cfg):
    tokens, chunks, cols, ff, u_tile, top = (cfg[n] for n in ("tokens", "chunks", "cols", "ff", "u_tile", "top"))
    d, rows = sum(cols), N * N * N * SUB
    hbm = pl.BlockSpec(memory_space=pl.ANY)
    block = lambda w: jax.ShapeDtypeStruct((chunks, N, N, N, SUB, w), BF16)
    dma = pltpu.SemaphoreType.DMA
    outs = pl.pallas_call(
        functools.partial(kernel, cfg),
        out_shape=[jax.ShapeDtypeStruct((tokens, d), F32), jax.ShapeDtypeStruct((3, tokens, d), BF16)]
        + [block(w) for _ in range(4) for w in cols],
        in_specs=[hbm] * 10,
        out_specs=[hbm] * 14,
        scratch_shapes=[
            pltpu.VMEM((tokens, d), BF16),
            *[pltpu.VMEM((3, tokens, w), BF16) for w in cols],
            pltpu.VMEM((3, 4, 2 * top, tokens), F32),
            pltpu.VMEM((N, N, N, SUB, d), BF16),
            pltpu.VMEM((d, ff), BF16),
            pltpu.VMEM((d, ff), BF16),
            pltpu.VMEM((chunks, N, N, N, SUB, d), BF16),
            pltpu.VMEM((chunks, N, N, N, SUB, d), BF16),
            pltpu.VMEM((rows, ff), BF16),
            pltpu.VMEM((tokens, d), F32),
            pltpu.VMEM((3, d, u_tile), BF16),
            pltpu.VMEM((3, d, u_tile), BF16),
            pltpu.VMEM((2, u_tile, d), BF16),
            pltpu.VMEM((tokens, u_tile), BF16),
            pltpu.VMEM((top, tokens), jnp.int32),
            pltpu.VMEM((top, tokens), jnp.int32),
            pltpu.VMEM((top, tokens), F32),
            dma((2,)), dma((ff // cfg["f_tile"] + 1,)), dma((3, 3)), dma((2,)), dma(()),
            *[dma(())] * 6, *[dma((2,))] * 2,
            *[dma(()), dma((chunks,))] * 3,
            dma(()), dma((4,)), dma(()), dma((chunks,)), dma(()), dma((4,)),
            *[dma(())] * 3,
        ],
        compiler_params=pltpu.CompilerParams(collective_id=0, has_side_effects=True, vmem_limit_bytes=cfg["vmem"]),
        name="moe_layer",
    )(x, expert, slot, gate, w_gate, w_up, w_down.reshape(chunks, N, N, N, SUB, d), s_gate, s_up, s_down)
    total, sums = outs[:2]
    for o in range(3):
        total += sums[o].astype(F32)
    return total.astype(BF16)


PLAN = {
    "pre": 21, "relay": 4, "own": 15, "gather": (8, 12, 14, 16, 18), "forward": 14, "mid": (),
    "weights": (17, 19),
    "main": (((0, 1), "C", 1), ((0, 4), "C", 2), ((1, 1), "C", 3), ((1, 4), "C", 4),
             ((2, 0), "F", 0), ((3, 0), "F", 1), ((4, 0), "F", 2)),
    "eb": 0, "ebx": (4, 5, 6, 7), "fetch": 8, "late": 10, "sums": 11,
}


def configure(x, expert, w_gate, s_gate):
    tokens, d = x.shape[-2:]
    top, ff, width, experts = expert.shape[-1], w_gate.shape[-1], s_gate.shape[-1], N * N * N
    slots = 5 * tokens * top // (4 * experts)
    lanes = d // 128
    cols = tuple(128 * ((lanes + 2 - r) // 3) for r in range(3))
    return dict(tokens=tokens, top=top, slots=slots, chunks=slots // SUB, cols=cols, ff=ff, f_tile=512, down=(768, 512, 512),
                units=width // 512, u_tile=512, plan=PLAN, vmem=67043328)


TEST = dict(
    cols=(256, 256, 128), down=(256, 256, 128),
    plan={"pre": 7, "relay": 1, "own": 3, "weights": (3, 4), "gather": (2, 4), "forward": 6, "mid": (0,),
          "main": (((0, 3), "C", 1),), "eb": 0, "ebx": (4, 4, 4, 4), "fetch": 4, "late": 4, "sums": 4})


def solution(mesh):
    def step(x, expert, slot, gate, w_gate, w_up, w_down, s_gate, s_up, s_down):
        cfg = configure(x, expert, w_gate, s_gate)
        y = layer(x[0, 0], expert[0, 0].T, slot[0, 0].T, gate[0, 0].T, w_gate[0], w_up[0], w_down[0], s_gate, s_up, s_down, cfg)
        return y[None, None]

    tok, own, whole = P("dp", "ep", None, None), P("ep", None, None), P(None, None)
    return jax.shard_map(step, mesh=mesh, in_specs=(tok,) * 4 + (own,) * 3 + (whole,) * 3, out_specs=tok, check_vma=False)
```

```python
import functools

import jax
import jax.numpy as jnp
from jax import lax
from jax.experimental import pallas as pl
from jax.experimental.pallas import tpu as pltpu
from jax.sharding import PartitionSpec as P

MESH = pl.DeviceIdType.MESH
N = 4
STRIDE = (16, 4, 1)
TURNS = ((0, 1, 2), (1, 2, 0), (2, 0, 1))
SUB = 8
ORDER = (2, 1, 3, 0)
HOPS = tuple((r, s) for s in (1, 3, 2) for r in range(3))
SIDES = tuple((r, s) for s in (1, 3) for r in range(3))
F32, BF16 = jnp.float32, jnp.bfloat16


def dot(a, b):
    return jnp.dot(a, b, preferred_element_type=F32)


def any_of(i, places):
    hit = i == places[0]
    for p in places[1:]:
        hit = hit | (i == p)
    return hit


def before(i, places):
    return sum((i > p).astype(jnp.int32) for p in places)


def kernel(cfg, *refs):
    tokens, chunks, cols, ff, f_tile, units, u_tile, top, slots, plan = (
        cfg[n] for n in ("tokens", "chunks", "cols", "ff", "f_tile", "units", "u_tile", "top", "slots", "plan"))
    it = iter(refs)
    take = lambda n: [next(it) for _ in range(n)]
    x_hbm, expert_hbm, slot_hbm, gate_hbm, wg_hbm, wu_hbm, wd_hbm, sg_hbm, su_hbm, sd_hbm = take(10)
    sum_hbm, eal = take(2)
    made, bl, ecl, ebl = take(3), take(3), take(3), take(3)
    (xv,) = take(1)
    al = take(3)
    met, stage, wg, wu, wd, z, h, acc, sg, su, sd, act, expert_ref, slot_ref, gate_ref = take(15)
    (x_sem, w_sem, s_sem, st_sem, out_sem, a_send, a_recv, r_send, r_recv, m_send, m_recv, b0_send, b0_recv, b_send, b_recv,
     c_send, c_recv, ec_send, ec_recv, ecx_send, ecx_recv, eb_send, eb_recv,
     ebx_send, ebx_recv, ld_sem, ea_send, ea_recv) = take(28)

    me = lax.axis_index("ep")
    co = (me // 16, lax.rem(me // 4, 4), lax.rem(me, 4))
    starts = [sum(cols[:r]) for r in range(3)]
    span = [pl.ds(starts[r], cols[r]) for r in range(3)]
    d, last = sum(cols), chunks - 1
    a_axis, b_axis, c_axis = ([t[i] for t in TURNS] for i in range(3))

    def hop(c, s):
        return lax.rem(c + s, N)

    def peer(axis, s):
        return {"ep": me + (hop(co[axis], s) - co[axis]) * STRIDE[axis]}

    def remote(src, dst, send, recv, to):
        return pltpu.make_async_remote_copy(
            src_ref=src, dst_ref=dst, send_sem=send, recv_sem=recv, device_id=to, device_id_type=MESH)

    def ab(ref, r, k, a, b):
        return ref.at[k, b, a] if a_axis[r] > b_axis[r] else ref.at[k, a, b]

    def at_c(ref, r, k, c):
        if c_axis[r] == 0:
            return ref.at[k, c, :, :, :, span[r]]
        if c_axis[r] == 1:
            return ref.at[k, :, c, :, :, span[r]]
        return ref.at[k, :, :, c, :, span[r]]

    def at_ca(ref, r, k, c, a):
        ix = {c_axis[r]: c, a_axis[r]: a, b_axis[r]: slice(None)}
        return ref.at[k, ix[0], ix[1], ix[2], :, span[r]]

    every, others = slice(None), pl.ds(1, 3)

    def a_copy(r, s):
        return remote(x_hbm.at[:, span[r]], al[r].at[3 - s], a_send, a_recv, peer(a_axis[r], s))

    def relay(r, s):
        half = pl.ds(0 if s == 1 else tokens // 2, tokens // 2)
        return remote(al[r].at[3 - s, half], al[r].at[1, half], r_send, r_recv, peer(a_axis[r], s))

    def m_copy(axis, s):
        return remote(met.at[axis, 0], met.at[axis, N - s], m_send, m_recv, peer(axis, s))

    def early_copies(r):
        return [pltpu.make_async_copy(wd.at[:, 0, :, :, :, span[r]], made[r].at[:, 0], st_sem.at[0]),
                pltpu.make_async_copy(wd.at[:, 0, 0, :, :, span[r]], ab(bl[r], r, every, 0, 0), st_sem.at[1])]

    parts = (pl.ds(0, 1), pl.ds(1, chunks - 1))

    def b0_copy(r, part, s):
        k = parts[part]
        return remote(made[r].at[k, 0, s], ab(bl[r], r, k, 0, N - s), b0_send.at[part], b0_recv.at[part], peer(b_axis[r], s))

    def stage_copies(r, k):
        return [pltpu.make_async_copy(stage.at[others, :, :, :, span[r]], made[r].at[k, others], st_sem.at[0]),
                pltpu.make_async_copy(stage.at[others, 0, :, :, span[r]], ab(bl[r], r, k, others, 0), st_sem.at[1])]

    def b_copy(r, k, s):
        return remote(made[r].at[k, others, s], ab(bl[r], r, k, others, N - s), b_send, b_recv.at[k], peer(b_axis[r], s))

    def c_own(r, k):
        return pltpu.make_async_copy(bl[r].at[k, :, :, 0], at_c(z, r, k, 0), c_recv.at[k])

    def c_copy(r, k, s):
        return remote(bl[r].at[k, :, :, s], at_c(z, r, k, N - s), c_send, c_recv.at[k], peer(c_axis[r], s))

    def ec_own(r, k):
        return pltpu.make_async_copy(at_c(z, r, k, 0), ecl[r].at[k, :, :, 0], ec_recv.at[k])

    def ec_copy(r, k, s):
        return remote(at_c(z, r, k, s), ecl[r].at[k, :, :, N - s], ec_send, ec_recv.at[k], peer(c_axis[r], s))

    def ecx_own(r, o):
        return pltpu.make_async_copy(at_ca(z, r, last, 0, o), ab(ecl[r], r, last, o, every).at[:, 0], ecx_recv.at[o])

    def ecx_copy(r, o, s):
        return remote(at_ca(z, r, last, s, o), ab(ecl[r], r, last, o, every).at[:, N - s], ecx_send,
                      ecx_recv.at[o], peer(c_axis[r], s))

    def eb_copy(r, k, s):
        return remote(ab(ecl[r], r, k, every, s), ebl[r].at[k, :, N - s], eb_send, eb_recv.at[k], peer(b_axis[r], s))

    def ebx_own(r, o):
        return pltpu.make_async_copy(ab(ecl[r], r, last, o, 0), stage.at[o, 0, :, :, span[r]], ebx_recv.at[o])

    def ebx_copy(r, o, s):
        return remote(ab(ecl[r], r, last, o, s), stage.at[o, N - s, :, :, span[r]], ebx_send, ebx_recv.at[o], peer(b_axis[r], s))

    def ea_copy(r, o):
        return remote(al[r].at[o - 1], eal.at[3 - o, :, span[r]], ea_send, ea_recv, peer(a_axis[r], o))

    def load(r, k, b):
        src = ab(ecl[r], r, k, every, 0) if b == 0 else ebl[r].at[k, :, b]
        return pltpu.make_async_copy(src, wd.at[k, :, b, :, :, span[r]], ld_sem)

    def arrived(like, sem):
        remote(like, like, out_sem, sem, peer(0, 1)).wait_recv()

    def left(like, sem):
        remote(like, like, sem, out_sem, peer(0, 1)).wait_send()

    def up_copies(u):
        i, w = lax.rem(u, 3), pl.ds(pl.multiple_of(u * u_tile, u_tile), u_tile)
        return [pltpu.make_async_copy(sg_hbm.at[:, w], sg.at[i], s_sem.at[i, 0]),
                pltpu.make_async_copy(su_hbm.at[:, w], su.at[i], s_sem.at[i, 1])]

    def down_copy(u):
        i, w = lax.rem(u, 2), pl.ds(pl.multiple_of(u * u_tile, u_tile), u_tile)
        return pltpu.make_async_copy(sd_hbm.at[w, :], sd.at[i], s_sem.at[i, 2])

    def shared(u, beside=None):
        down_copy(u).start()
        @pl.when(u + 2 < units)
        def _():
            for c in up_copies(u + 2):
                c.start()
        with jax.named_scope("w_tile"):
            for c in up_copies(u):
                c.wait()
            @pl.when(u > 0)
            def _():
                down_copy(u - 1).wait()
        with jax.named_scope("tile"):
            i, old = lax.rem(u, 3), lax.rem(u + 1, 2)
            beside = beside or (lambda r: None)
            g = dot(xv[...], sg[i])
            beside(0)
            up = dot(xv[...], su[i])
            beside(1)
            acc[...] += dot(act[...], sd[old])
            act[...] = (jax.nn.silu(g) * up).astype(BF16)
            beside(2)

    def matches(r, o, first, count, weight):
        m = met.at[a_axis[r], o]
        code = m[:top].astype(jnp.int32)
        at = [(code >> (10 - 2 * axis)) & 3 for axis in range(3)]
        here = (code >= 0) & (at[a_axis[r]] == co[a_axis[r]])
        place = ((at[b_axis[r]] - co[b_axis[r]]) & 3) * 32 + ((at[c_axis[r]] - co[c_axis[r]]) & 3) * 8 + (code & 7)
        chunk = jnp.where(here, (code & 63) >> 3, -1)
        spread = lambda v, j: jnp.broadcast_to(v[j : j + 1], (16, tokens)).astype(BF16)[None]
        given = [spread(m[top:], j) for j in range(top)] if weight else [jnp.ones((1, 16, tokens), BF16)] * top
        row = (lax.broadcasted_iota(jnp.int32, (8, 16, tokens), 0) * 16 + lax.broadcasted_iota(jnp.int32, (8, 16, tokens), 1))
        row = row.astype(F32).astype(BF16)
        out = []
        for k in range(count):
            mine = jnp.where(chunk == first + k, place, -1).astype(F32)
            hit = jnp.zeros((8, 16, tokens), BF16)
            for j in range(top):
                hit = jnp.where(spread(mine, j) == row, given[j], hit)
            out.append(hit.reshape(128, tokens))
        return jnp.concatenate(out) if count > 1 else out[0]

    def gather(k, r):
        for o in (1, 3, 2):
            rows = dot(matches(r, o, k, 1, False), al[r][o - 1]).astype(BF16)
            stage[o, :, :, :, span[r]] = rows.reshape(N, N, SUB, cols[r])

    def keep(k):
        for r in range(3):
            for c in stage_copies(r, k):
                c.start()

    def dispatch(k):
        with jax.named_scope("w_stage"):
            for n, like in enumerate((stage.at[others], stage.at[others, 0])):
                pltpu.make_async_copy(like, like, st_sem.at[n]).wait()
        for r, s in HOPS:
            b_copy(r, k, s).start()

    def forward_c(k):
        if k == 1:
            arrived(z.at[pl.ds(1, last), 0, others], b0_recv.at[1])
        with jax.named_scope("w_b"):
            arrived(z.at[k, others, others], b_recv.at[k])
        for r, s in HOPS:
            c_copy(r, k, s).start()
        for r in range(3):
            c_own(r, k).start()

    def forward_eb(k):
        with jax.named_scope("w_ec"):
            arrived(z.at[k], ec_recv.at[k])
        for r, s in HOPS:
            eb_copy(r, k, s).start()

    def forward_ebx(o):
        with jax.named_scope("w_ecx"):
            arrived(z.at[last, 0], ecx_recv.at[o])
        for r, s in HOPS:
            ebx_copy(r, o, s).start()
        for r in range(3):
            ebx_own(r, o).start()

    f_tiles = ff // f_tile

    def tile_copies(f):
        w = pl.ds(pl.multiple_of(f * f_tile, f_tile), f_tile)
        return [pltpu.make_async_copy(wg_hbm.at[:, w], wg.at[:, w], w_sem.at[f]), pltpu.make_async_copy(wu_hbm.at[:, w], wu.at[:, w], w_sem.at[f])]

    def wd_copy(k):
        return pltpu.make_async_copy(wd_hbm.at[k], wd.at[k], w_sem.at[f_tiles])

    rows = N * N * N * SUB

    def expert(k):
        with jax.named_scope("w_c"):
            arrived(z.at[k], c_recv.at[k])

        def up(f, _):
            @pl.when(k == 0)
            def _():
                @pl.when(f + 2 < f_tiles)
                def _():
                    for c in tile_copies(f + 2):
                        c.start()

                @pl.when(f < chunks)
                def _():
                    wd_copy(f).start()
                like = wg.at[:, pl.ds(0, 2 * f_tile)]
                with jax.named_scope("w_wgu"):
                    pltpu.make_async_copy(like, like, w_sem.at[f]).wait()
            for (ek, ef), event, arg in plan["main"]:
                pl.when((k == ek) & (f == ef))(functools.partial({"C": forward_c, "F": forward_eb}[event], arg))
            with jax.named_scope("up"):
                w = pl.ds(pl.multiple_of(f * f_tile, f_tile), f_tile)
                zk = z[k].reshape(rows, d)
                h[:, w] = (jax.nn.silu(dot(zk, wg[:, w])) * dot(zk, wu[:, w])).astype(BF16)
            return 0
        lax.fori_loop(0, ff // f_tile, up, 0)

        if plan["mid"]:
            @pl.when(any_of(k, plan["mid"]))
            def _():
                shared(plan["pre"] + before(k, plan["mid"]))

        @pl.when(k == 0)
        def _():
            with jax.named_scope("w_wd"):
                pltpu.make_async_copy(wd_hbm, wd, w_sem.at[f_tiles]).wait()

        at = 0
        for r in range(3):
            w = pl.ds(at, cfg["down"][r])
            at += cfg["down"][r]
            with jax.named_scope("down"):
                out = dot(h[...], wd[:, :, :, :, :, w].reshape(ff, cfg["down"][r]))
                z[k, :, :, :, :, w] = out.astype(BF16).reshape(N, N, N, SUB, cfg["down"][r])

            @pl.when(k < last)
            def _():
                for s in (1, 3, 2):
                    ec_copy(r, k, s).start()
                ec_own(r, k).start()

            @pl.when(k == last)
            def _():
                for o in ORDER:
                    for s in (1, 3, 2):
                        ecx_copy(r, o, s).start()
                    ecx_own(r, o).start()

    def held(r, o):
        wide = 128 * chunks
        return pl.ds(r * tokens, tokens), pl.ds(pl.multiple_of(o * wide, wide), wide)

    def weigh(i, r):
        o = ordered(i)
        wg[held(r, o)] = matches(r, o, 0, chunks, True).T

    def ordered(i):
        return jnp.where(i == 0, ORDER[0], jnp.where(i == 1, ORDER[1], jnp.where(i == 2, ORDER[2], ORDER[3])))

    def combine(i, _):
        o = ordered(i)
        with jax.named_scope("w_ebx"):
            arrived(stage.at[o], ebx_recv.at[o])
        for r in range(3):
            weight = wg[held(r, o)]
            early = wd[0:last, pl.ds(o, 1), :, :, :, span[r]].reshape(128 * last, cols[r])
            late = stage[pl.ds(o, 1), :, :, :, span[r]].reshape(128, cols[r])
            with jax.named_scope("m"):
                part = dot(weight[:, : 128 * last], early) + dot(weight[:, 128 * last :], late)

            @pl.when(o == 0)
            def _():
                acc[:, span[r]] += part

            @pl.when(o > 0)
            def _():
                al[r][pl.ds(o - 1, 1)] = part.astype(BF16)[None]
                ea_copy(r, o).start()
        return 0

    barrier = pltpu.get_barrier_semaphore()
    for axis in range(3):
        for s in (1, 2, 3):
            pl.semaphore_signal(barrier, inc=1, device_id=peer(axis, s), device_id_type=MESH)
    routing = [pltpu.make_async_copy(a, b, x_sem.at[1]) for a, b in ((expert_hbm, expert_ref), (slot_hbm, slot_ref), (gate_hbm, gate_ref))]
    x_in = pltpu.make_async_copy(x_hbm, xv, x_sem.at[0])
    for c in (*routing, x_in):
        c.start()
    for u in range(2):
        for c in up_copies(u):
            c.start()
    acc[...] = jnp.zeros_like(acc)
    act[...] = jnp.zeros_like(act)
    sd[1] = jnp.zeros_like(sd[1])
    for c in routing:
        c.wait()
    code = jnp.where(slot_ref[...] < slots, expert_ref[...] * 64 + slot_ref[...], -1).astype(F32)
    for axis in range(3):
        met[axis, 0, :top] = code
        met[axis, 0, top:] = gate_ref[...]
    x_in.wait()
    with jax.named_scope("w_barrier"):
        pl.semaphore_wait(barrier, 9)
    for r, s in SIDES:
        a_copy(r, s).start()
    for s in (1, 3, 2):
        for axis in range(3):
            m_copy(axis, s).start()

    def own_rows(r):
        mine = dot(matches(r, 0, 0, chunks, False), xv[:, span[r]]).astype(BF16)
        wd[:, 0, :, :, :, span[r]] = mine.reshape(chunks, N, N, SUB, cols[r])

    shared(0, own_rows)
    for r in range(3):
        for c in early_copies(r):
            c.start()

    def pre(i, _):
        gathers = plan["gather"]
        for f, at in enumerate(plan["weights"]):
            @pl.when(i == at)
            def _():
                for c in tile_copies(f):
                    c.start()

        @pl.when(i == plan["relay"])
        def _():
            for n, like in enumerate((wd.at[:, 0], wd.at[:, 0, 0])):
                pltpu.make_async_copy(like, like, st_sem.at[n]).wait()
            with jax.named_scope("w_a1"):
                arrived(eal.at[pl.ds(0, 2)], a_recv)
            for r, s in SIDES:
                relay(r, s).start()
            for r, s in HOPS:
                b0_copy(r, 0, s).start()

        @pl.when(i == plan["own"])
        def _():
            for r, s in HOPS:
                b0_copy(r, 1, s).start()

        @pl.when(i == gathers[0])
        def _():
            with jax.named_scope("w_a2"):
                arrived(met.at[:, others], m_recv)
                arrived(xv, r_recv)

        @pl.when(i == plan["forward"])
        def _():
            with jax.named_scope("w_b0"):
                arrived(z.at[0, 0, others], b0_recv.at[0])
            left(xv, r_send)
            forward_c(0)

        @pl.when(any_of(i - 2, gathers))
        def _():
            dispatch(before(i - 2, gathers))

        gathering = any_of(i, gathers)

        @pl.when(gathering)
        def _():
            k = before(i, gathers)
            shared(i, lambda r: gather(k, r))
            keep(k)

        @pl.when(jnp.logical_not(gathering))
        def _():
            shared(i)
        return 0
    lax.fori_loop(1, plan["pre"], pre, 0)
    lax.fori_loop(0, chunks, lambda k, _: (expert(k), 0)[1], 0)

    def fetch(ks):
        for k in ks:
            with jax.named_scope("w_eb"):
                arrived(z.at[k, :, others], eb_recv.at[k])
            for r in range(3):
                for b in range(4):
                    load(r, k, b).start()

    done = plan["pre"] + len(plan["mid"])

    def masks(i, _):
        @pl.when(i == plan["eb"])
        def _():
            forward_eb(last - 1)

        shared(i + done, lambda r: weigh(i, r))
        return 0
    lax.fori_loop(0, 4, masks, 0)

    def tail(i, _):
        @pl.when(i == plan["fetch"])
        def _():
            fetch(range(last - 1))

        @pl.when(i == plan["late"])
        def _():
            fetch([last - 1])

        for p, o in zip(plan["ebx"], ORDER, strict=True):
            pl.when(i == p)(functools.partial(forward_ebx, o))

        @pl.when(i == plan["sums"])
        def _():
            with jax.named_scope("w_load"):
                whole = wd.at[pl.ds(0, last)]
                pltpu.make_async_copy(whole, whole, ld_sem).wait()
            lax.fori_loop(0, 4, combine, 0)

        shared(i + done)
        return 0
    lax.fori_loop(4, units - done, tail, 0)
    down_copy(units - 1).wait()
    outs = [pltpu.make_async_copy(acc.at[:, span[r]], sum_hbm.at[:, span[r]], out_sem) for r in range(3)]
    for r in range(3):
        acc[:, span[r]] += dot(act[...], sd[(units - 1) % 2, :, span[r]])
        outs[r].start()
    with jax.named_scope("w_ea"):
        arrived(eal, ea_recv)

    early, end = pl.ds(0, last), pl.ds(last, 1)
    left(met.at[:, others], m_send)
    left(eal.at[pl.ds(0, 2)], a_send)
    left(z.at[0, 0, others], b0_send.at[0])
    left(z.at[pl.ds(1, last), 0, others], b0_send.at[1])
    left(z.at[:, others, others], b_send)
    left(z.at[:, :, :, others], c_send)
    left(z.at[early, :, :, others], ec_send)
    left(z.at[end, :, :, others], ecx_send)
    left(z.at[early, :, others], eb_send)
    left(z.at[end, :, others], ebx_send)
    left(eal, ea_send)
    with jax.named_scope("w_out"):
        pltpu.make_async_copy(acc, sum_hbm, out_sem).wait()


def layer(x, expert, slot, gate, w_gate, w_up, w_down, s_gate, s_up, s_down, cfg):
    tokens, chunks, cols, ff, u_tile, top = (cfg[n] for n in ("tokens", "chunks", "cols", "ff", "u_tile", "top"))
    d, rows = sum(cols), N * N * N * SUB
    hbm = pl.BlockSpec(memory_space=pl.ANY)
    block = lambda w: jax.ShapeDtypeStruct((chunks, N, N, N, SUB, w), BF16)
    dma = pltpu.SemaphoreType.DMA
    outs = pl.pallas_call(
        functools.partial(kernel, cfg),
        out_shape=[jax.ShapeDtypeStruct((tokens, d), F32), jax.ShapeDtypeStruct((3, tokens, d), BF16)]
        + [block(w) for _ in range(4) for w in cols],
        in_specs=[hbm] * 10,
        out_specs=[hbm] * 14,
        scratch_shapes=[
            pltpu.VMEM((tokens, d), BF16),
            *[pltpu.VMEM((3, tokens, w), BF16) for w in cols],
            pltpu.VMEM((3, 4, 2 * top, tokens), F32),
            pltpu.VMEM((N, N, N, SUB, d), BF16),
            pltpu.VMEM((d, ff), BF16),
            pltpu.VMEM((d, ff), BF16),
            pltpu.VMEM((chunks, N, N, N, SUB, d), BF16),
            pltpu.VMEM((chunks, N, N, N, SUB, d), BF16),
            pltpu.VMEM((rows, ff), BF16),
            pltpu.VMEM((tokens, d), F32),
            pltpu.VMEM((3, d, u_tile), BF16),
            pltpu.VMEM((3, d, u_tile), BF16),
            pltpu.VMEM((2, u_tile, d), BF16),
            pltpu.VMEM((tokens, u_tile), BF16),
            pltpu.VMEM((top, tokens), jnp.int32),
            pltpu.VMEM((top, tokens), jnp.int32),
            pltpu.VMEM((top, tokens), F32),
            dma((2,)), dma((ff // cfg["f_tile"] + 1,)), dma((3, 3)), dma((2,)), dma(()),
            *[dma(())] * 6, *[dma((2,))] * 2,
            *[dma(()), dma((chunks,))] * 3,
            dma(()), dma((4,)), dma(()), dma((chunks,)), dma(()), dma((4,)),
            *[dma(())] * 3,
        ],
        compiler_params=pltpu.CompilerParams(collective_id=0, has_side_effects=True, vmem_limit_bytes=cfg["vmem"]),
        name="moe_layer",
    )(x, expert, slot, gate, w_gate, w_up, w_down.reshape(chunks, N, N, N, SUB, d), s_gate, s_up, s_down)
    total, sums = outs[:2]
    for o in range(3):
        total += sums[o].astype(F32)
    return total.astype(BF16)


PLAN = {
    "pre": 21, "relay": 4, "own": 6, "gather": (8, 10, 12, 14, 16), "forward": 14, "mid": (),
    "weights": (16, 20),
    "main": (((0, 0), "C", 1), ((0, 3), "C", 2), ((1, 2), "C", 3), ((2, 0), "C", 4),
             ((2, 1), "F", 0), ((3, 1), "F", 1), ((4, 0), "F", 2)),
    "eb": 0, "ebx": (4, 5, 6, 7), "fetch": 8, "late": 10, "sums": 11,
}


def configure(x, expert, w_gate, s_gate):
    tokens, d = x.shape[-2:]
    top, ff, width, experts = expert.shape[-1], w_gate.shape[-1], s_gate.shape[-1], N * N * N
    slots = 5 * tokens * top // (4 * experts)
    lanes = d // 128
    cols = tuple(128 * ((lanes + 2 - r) // 3) for r in range(3))
    return dict(tokens=tokens, top=top, slots=slots, chunks=slots // SUB, cols=cols, ff=ff, f_tile=512, down=(768, 512, 512),
                units=width // 512, u_tile=512, plan=PLAN, vmem=67043328)


TEST = dict(
    cols=(256, 256, 128), down=(256, 256, 128),
    plan={"pre": 7, "relay": 1, "own": 3, "weights": (3, 4), "gather": (2, 4), "forward": 6, "mid": (0,),
          "main": (((0, 3), "C", 1),), "eb": 0, "ebx": (4, 4, 4, 4), "fetch": 4, "late": 4, "sums": 4})


def solution(mesh):
    def step(x, expert, slot, gate, w_gate, w_up, w_down, s_gate, s_up, s_down):
        cfg = configure(x, expert, w_gate, s_gate)
        y = layer(x[0, 0], expert[0, 0].T, slot[0, 0].T, gate[0, 0].T, w_gate[0], w_up[0], w_down[0], s_gate, s_up, s_down, cfg)
        return y[None, None]

    tok, own, whole = P("dp", "ep", None, None), P("ep", None, None), P(None, None)
    return jax.shard_map(step, mesh=mesh, in_specs=(tok,) * 4 + (own,) * 3 + (whole,) * 3, out_specs=tok, check_vma=False)
```

```python
import functools

import jax
import jax.numpy as jnp
from jax import lax
from jax.experimental import pallas as pl
from jax.experimental.pallas import tpu as pltpu
from jax.sharding import PartitionSpec as P

MESH = pl.DeviceIdType.MESH
N = 4
STRIDE = (16, 4, 1)
TURNS = ((0, 1, 2), (1, 2, 0), (2, 0, 1))
SUB = 8
ORDER = (2, 1, 3, 0)
HOPS = tuple((r, s) for s in (1, 3, 2) for r in range(3))
SIDES = tuple((r, s) for s in (1, 3) for r in range(3))
F32, BF16 = jnp.float32, jnp.bfloat16


def dot(a, b):
    return jnp.dot(a, b, preferred_element_type=F32)


def any_of(i, places):
    hit = i == places[0]
    for p in places[1:]:
        hit = hit | (i == p)
    return hit


def before(i, places):
    return sum((i > p).astype(jnp.int32) for p in places)


def kernel(cfg, *refs):
    tokens, chunks, cols, ff, f_tile, units, u_tile, top, slots, plan = (
        cfg[n] for n in ("tokens", "chunks", "cols", "ff", "f_tile", "units", "u_tile", "top", "slots", "plan"))
    it = iter(refs)
    take = lambda n: [next(it) for _ in range(n)]
    x_hbm, expert_hbm, slot_hbm, gate_hbm, wg_hbm, wu_hbm, wd_hbm, sg_hbm, su_hbm, sd_hbm = take(10)
    sum_hbm, eal = take(2)
    made, bl, ecl, ebl = take(3), take(3), take(3), take(3)
    (xv,) = take(1)
    al = take(3)
    met, stage, wg, wu, wd, z, h, acc, sg, su, sd, act, expert_ref, slot_ref, gate_ref = take(15)
    (x_sem, w_sem, s_sem, st_sem, out_sem, a_send, a_recv, r_send, r_recv, m_send, m_recv, b0_send, b0_recv, b_send, b_recv,
     c_send, c_recv, ec_send, ec_recv, ecx_send, ecx_recv, eb_send, eb_recv,
     ebx_send, ebx_recv, ld_sem, ea_send, ea_recv) = take(28)

    me = lax.axis_index("ep")
    co = (me // 16, lax.rem(me // 4, 4), lax.rem(me, 4))
    starts = [sum(cols[:r]) for r in range(3)]
    span = [pl.ds(starts[r], cols[r]) for r in range(3)]
    d, last = sum(cols), chunks - 1
    a_axis, b_axis, c_axis = ([t[i] for t in TURNS] for i in range(3))

    def hop(c, s):
        return lax.rem(c + s, N)

    def peer(axis, s):
        return {"ep": me + (hop(co[axis], s) - co[axis]) * STRIDE[axis]}

    def remote(src, dst, send, recv, to):
        return pltpu.make_async_remote_copy(
            src_ref=src, dst_ref=dst, send_sem=send, recv_sem=recv, device_id=to, device_id_type=MESH)

    def ab(ref, r, k, a, b):
        return ref.at[k, b, a] if a_axis[r] > b_axis[r] else ref.at[k, a, b]

    def at_c(ref, r, k, c):
        if c_axis[r] == 0:
            return ref.at[k, c, :, :, :, span[r]]
        if c_axis[r] == 1:
            return ref.at[k, :, c, :, :, span[r]]
        return ref.at[k, :, :, c, :, span[r]]

    def at_ca(ref, r, k, c, a):
        ix = {c_axis[r]: c, a_axis[r]: a, b_axis[r]: slice(None)}
        return ref.at[k, ix[0], ix[1], ix[2], :, span[r]]

    every, others = slice(None), pl.ds(1, 3)

    def a_copy(r, s):
        return remote(x_hbm.at[:, span[r]], al[r].at[3 - s], a_send, a_recv, peer(a_axis[r], s))

    def relay(r, s):
        half = pl.ds(0 if s == 1 else tokens // 2, tokens // 2)
        return remote(al[r].at[3 - s, half], al[r].at[1, half], r_send, r_recv, peer(a_axis[r], s))

    def m_copy(axis, s):
        return remote(met.at[axis, 0], met.at[axis, N - s], m_send, m_recv, peer(axis, s))

    def early_copies(r):
        return [pltpu.make_async_copy(wd.at[:, 0, :, :, :, span[r]], made[r].at[:, 0], st_sem.at[0]),
                pltpu.make_async_copy(wd.at[:, 0, 0, :, :, span[r]], ab(bl[r], r, every, 0, 0), st_sem.at[1])]

    parts = (pl.ds(0, 1), pl.ds(1, chunks - 1))

    def b0_copy(r, part, s):
        k = parts[part]
        return remote(made[r].at[k, 0, s], ab(bl[r], r, k, 0, N - s), b0_send.at[part], b0_recv.at[part], peer(b_axis[r], s))

    def stage_copies(r, k):
        return [pltpu.make_async_copy(stage.at[others, :, :, :, span[r]], made[r].at[k, others], st_sem.at[0]),
                pltpu.make_async_copy(stage.at[others, 0, :, :, span[r]], ab(bl[r], r, k, others, 0), st_sem.at[1])]

    def b_copy(r, k, s):
        return remote(made[r].at[k, others, s], ab(bl[r], r, k, others, N - s), b_send, b_recv.at[k], peer(b_axis[r], s))

    def c_own(r, k):
        return pltpu.make_async_copy(bl[r].at[k, :, :, 0], at_c(z, r, k, 0), c_recv.at[k])

    def c_copy(r, k, s):
        return remote(bl[r].at[k, :, :, s], at_c(z, r, k, N - s), c_send, c_recv.at[k], peer(c_axis[r], s))

    def ec_own(r, k):
        return pltpu.make_async_copy(at_c(z, r, k, 0), ecl[r].at[k, :, :, 0], ec_recv.at[k])

    def ec_copy(r, k, s):
        return remote(at_c(z, r, k, s), ecl[r].at[k, :, :, N - s], ec_send, ec_recv.at[k], peer(c_axis[r], s))

    def ecx_own(r, o):
        return pltpu.make_async_copy(at_ca(z, r, last, 0, o), ab(ecl[r], r, last, o, every).at[:, 0], ecx_recv.at[o])

    def ecx_copy(r, o, s):
        return remote(at_ca(z, r, last, s, o), ab(ecl[r], r, last, o, every).at[:, N - s], ecx_send,
                      ecx_recv.at[o], peer(c_axis[r], s))

    def eb_copy(r, k, s):
        return remote(ab(ecl[r], r, k, every, s), ebl[r].at[k, :, N - s], eb_send, eb_recv.at[k], peer(b_axis[r], s))

    def ebx_own(r, o):
        return pltpu.make_async_copy(ab(ecl[r], r, last, o, 0), stage.at[o, 0, :, :, span[r]], ebx_recv.at[o])

    def ebx_copy(r, o, s):
        return remote(ab(ecl[r], r, last, o, s), stage.at[o, N - s, :, :, span[r]], ebx_send, ebx_recv.at[o], peer(b_axis[r], s))

    def ea_copy(r, o):
        return remote(al[r].at[o - 1], eal.at[3 - o, :, span[r]], ea_send, ea_recv, peer(a_axis[r], o))

    def load(r, k, b):
        src = ab(ecl[r], r, k, every, 0) if b == 0 else ebl[r].at[k, :, b]
        return pltpu.make_async_copy(src, wd.at[k, :, b, :, :, span[r]], ld_sem)

    def arrived(like, sem):
        remote(like, like, out_sem, sem, peer(0, 1)).wait_recv()

    def left(like, sem):
        remote(like, like, sem, out_sem, peer(0, 1)).wait_send()

    def up_copies(u):
        i, w = lax.rem(u, 3), pl.ds(pl.multiple_of(u * u_tile, u_tile), u_tile)
        return [pltpu.make_async_copy(sg_hbm.at[:, w], sg.at[i], s_sem.at[i, 0]),
                pltpu.make_async_copy(su_hbm.at[:, w], su.at[i], s_sem.at[i, 1])]

    def down_copy(u):
        i, w = lax.rem(u, 2), pl.ds(pl.multiple_of(u * u_tile, u_tile), u_tile)
        return pltpu.make_async_copy(sd_hbm.at[w, :], sd.at[i], s_sem.at[i, 2])

    def shared(u, beside=None):
        down_copy(u).start()
        @pl.when(u + 2 < units)
        def _():
            for c in up_copies(u + 2):
                c.start()
        for c in up_copies(u):
            c.wait()
        @pl.when(u > 0)
        def _():
            down_copy(u - 1).wait()
        i, old = lax.rem(u, 3), lax.rem(u + 1, 2)
        beside = beside or (lambda r: None)
        g = dot(xv[...], sg[i])
        beside(0)
        up = dot(xv[...], su[i])
        beside(1)
        acc[...] += dot(act[...], sd[old])
        act[...] = (jax.nn.silu(g) * up).astype(BF16)
        beside(2)

    def matches(r, o, first, count, weight):
        m = met.at[a_axis[r], o]
        code = m[:top].astype(jnp.int32)
        at = [(code >> (10 - 2 * axis)) & 3 for axis in range(3)]
        here = (code >= 0) & (at[a_axis[r]] == co[a_axis[r]])
        place = ((at[b_axis[r]] - co[b_axis[r]]) & 3) * 32 + ((at[c_axis[r]] - co[c_axis[r]]) & 3) * 8 + (code & 7)
        chunk = jnp.where(here, (code & 63) >> 3, -1)
        spread = lambda v, j: jnp.broadcast_to(v[j : j + 1], (16, tokens)).astype(BF16)[None]
        given = [spread(m[top:], j) for j in range(top)] if weight else [jnp.ones((1, 16, tokens), BF16)] * top
        row = (lax.broadcasted_iota(jnp.int32, (8, 16, tokens), 0) * 16 + lax.broadcasted_iota(jnp.int32, (8, 16, tokens), 1))
        row = row.astype(F32).astype(BF16)
        out = []
        for k in range(count):
            mine = jnp.where(chunk == first + k, place, -1).astype(F32)
            hit = jnp.zeros((8, 16, tokens), BF16)
            for j in range(top):
                hit = jnp.where(spread(mine, j) == row, given[j], hit)
            out.append(hit.reshape(128, tokens))
        return jnp.concatenate(out) if count > 1 else out[0]

    def gather(k, r):
        for o in (1, 3, 2):
            rows = dot(matches(r, o, k, 1, False), al[r][o - 1]).astype(BF16)
            stage[o, :, :, :, span[r]] = rows.reshape(N, N, SUB, cols[r])

    def keep(k):
        for r in range(3):
            for c in stage_copies(r, k):
                c.start()

    def dispatch(k):
        for n, like in enumerate((stage.at[others], stage.at[others, 0])):
            pltpu.make_async_copy(like, like, st_sem.at[n]).wait()
        for r, s in HOPS:
            b_copy(r, k, s).start()

    def forward_c(k):
        if k == 1:
            arrived(z.at[pl.ds(1, last), 0, others], b0_recv.at[1])
        arrived(z.at[k, others, others], b_recv.at[k])
        for r, s in HOPS:
            c_copy(r, k, s).start()
        for r in range(3):
            c_own(r, k).start()

    def forward_eb(k):
        arrived(z.at[k], ec_recv.at[k])
        for r, s in HOPS:
            eb_copy(r, k, s).start()

    def forward_ebx(o):
        arrived(z.at[last, 0], ecx_recv.at[o])
        for r, s in HOPS:
            ebx_copy(r, o, s).start()
        for r in range(3):
            ebx_own(r, o).start()

    f_tiles = ff // f_tile

    def tile_copies(f):
        w = pl.ds(pl.multiple_of(f * f_tile, f_tile), f_tile)
        return [pltpu.make_async_copy(wg_hbm.at[:, w], wg.at[:, w], w_sem.at[f]), pltpu.make_async_copy(wu_hbm.at[:, w], wu.at[:, w], w_sem.at[f])]

    def wd_copy(k):
        return pltpu.make_async_copy(wd_hbm.at[k], wd.at[k], w_sem.at[f_tiles])

    rows = N * N * N * SUB

    def expert(k):
        arrived(z.at[k], c_recv.at[k])

        def up(f, _):
            @pl.when(k == 0)
            def _():
                @pl.when(f + 2 < f_tiles)
                def _():
                    for c in tile_copies(f + 2):
                        c.start()

                @pl.when(f < chunks)
                def _():
                    wd_copy(f).start()
                like = wg.at[:, pl.ds(0, 2 * f_tile)]
                pltpu.make_async_copy(like, like, w_sem.at[f]).wait()
            for (ek, ef), event, arg in plan["main"]:
                pl.when((k == ek) & (f == ef))(functools.partial({"C": forward_c, "F": forward_eb}[event], arg))
            w = pl.ds(pl.multiple_of(f * f_tile, f_tile), f_tile)
            zk = z[k].reshape(rows, d)
            h[:, w] = (jax.nn.silu(dot(zk, wg[:, w])) * dot(zk, wu[:, w])).astype(BF16)
            return 0
        lax.fori_loop(0, ff // f_tile, up, 0)

        if plan["mid"]:
            @pl.when(any_of(k, plan["mid"]))
            def _():
                shared(plan["pre"] + before(k, plan["mid"]))

        @pl.when(k == 0)
        def _():
            pltpu.make_async_copy(wd_hbm, wd, w_sem.at[f_tiles]).wait()

        at = 0
        for r in range(3):
            w = pl.ds(at, cfg["down"][r])
            at += cfg["down"][r]
            out = dot(h[...], wd[:, :, :, :, :, w].reshape(ff, cfg["down"][r]))
            z[k, :, :, :, :, w] = out.astype(BF16).reshape(N, N, N, SUB, cfg["down"][r])

            @pl.when(k < last)
            def _():
                for s in (1, 3, 2):
                    ec_copy(r, k, s).start()
                ec_own(r, k).start()

            @pl.when(k == last)
            def _():
                for o in ORDER:
                    for s in (1, 3, 2):
                        ecx_copy(r, o, s).start()
                    ecx_own(r, o).start()

    def held(r, o):
        wide = 128 * chunks
        return pl.ds(r * tokens, tokens), pl.ds(pl.multiple_of(o * wide, wide), wide)

    def weigh(i, r):
        o = ordered(i)
        wg[held(r, o)] = matches(r, o, 0, chunks, True).T

    def ordered(i):
        return jnp.where(i == 0, ORDER[0], jnp.where(i == 1, ORDER[1], jnp.where(i == 2, ORDER[2], ORDER[3])))

    def combine(i, _):
        o = ordered(i)
        arrived(stage.at[o], ebx_recv.at[o])
        for r in range(3):
            weight = wg[held(r, o)]
            early = wd[0:last, pl.ds(o, 1), :, :, :, span[r]].reshape(128 * last, cols[r])
            late = stage[pl.ds(o, 1), :, :, :, span[r]].reshape(128, cols[r])
            part = dot(weight[:, : 128 * last], early) + dot(weight[:, 128 * last :], late)

            @pl.when(o == 0)
            def _():
                acc[:, span[r]] += part

            @pl.when(o > 0)
            def _():
                al[r][pl.ds(o - 1, 1)] = part.astype(BF16)[None]
                ea_copy(r, o).start()
        return 0

    barrier = pltpu.get_barrier_semaphore()
    for axis in range(3):
        for s in (1, 2, 3):
            pl.semaphore_signal(barrier, inc=1, device_id=peer(axis, s), device_id_type=MESH)
    routing = [pltpu.make_async_copy(a, b, x_sem.at[1]) for a, b in ((expert_hbm, expert_ref), (slot_hbm, slot_ref), (gate_hbm, gate_ref))]
    x_in = pltpu.make_async_copy(x_hbm, xv, x_sem.at[0])
    for c in (*routing, x_in):
        c.start()
    for u in range(2):
        for c in up_copies(u):
            c.start()
    pl.semaphore_wait(barrier, 9)
    for r, s in SIDES:
        a_copy(r, s).start()
    acc[...] = jnp.zeros_like(acc)
    act[...] = jnp.zeros_like(act)
    sd[1] = jnp.zeros_like(sd[1])
    for c in routing:
        c.wait()
    code = jnp.where(slot_ref[...] < slots, expert_ref[...] * 64 + slot_ref[...], -1).astype(F32)
    for axis in range(3):
        met[axis, 0, :top] = code
        met[axis, 0, top:] = gate_ref[...]
    for s in (1, 3, 2):
        for axis in range(3):
            m_copy(axis, s).start()
    x_in.wait()

    def own_rows(r):
        mine = dot(matches(r, 0, 0, chunks, False), xv[:, span[r]]).astype(BF16)
        wd[:, 0, :, :, :, span[r]] = mine.reshape(chunks, N, N, SUB, cols[r])

    shared(0, own_rows)
    for r in range(3):
        for c in early_copies(r):
            c.start()

    def pre(i, _):
        gathers = plan["gather"]
        for f, at in enumerate(plan["weights"]):
            @pl.when(i == at)
            def _():
                for c in tile_copies(f):
                    c.start()

        @pl.when(i == plan["relay"])
        def _():
            for n, like in enumerate((wd.at[:, 0], wd.at[:, 0, 0])):
                pltpu.make_async_copy(like, like, st_sem.at[n]).wait()
            arrived(eal.at[pl.ds(0, 2)], a_recv)
            for r, s in SIDES:
                relay(r, s).start()
            for r, s in HOPS:
                b0_copy(r, 0, s).start()

        @pl.when(i == plan["own"])
        def _():
            for r, s in HOPS:
                b0_copy(r, 1, s).start()

        @pl.when(i == gathers[0])
        def _():
            arrived(met.at[:, others], m_recv)
            arrived(xv, r_recv)

        @pl.when(i == plan["forward"])
        def _():
            arrived(z.at[0, 0, others], b0_recv.at[0])
            left(xv, r_send)
            forward_c(0)

        @pl.when(any_of(i - 2, gathers))
        def _():
            dispatch(before(i - 2, gathers))

        gathering = any_of(i, gathers)

        @pl.when(gathering)
        def _():
            k = before(i, gathers)
            shared(i, lambda r: gather(k, r))
            keep(k)

        @pl.when(jnp.logical_not(gathering))
        def _():
            shared(i)
        return 0
    lax.fori_loop(1, plan["pre"], pre, 0)
    lax.fori_loop(0, chunks, lambda k, _: (expert(k), 0)[1], 0)

    def fetch(ks):
        for k in ks:
            arrived(z.at[k, :, others], eb_recv.at[k])
            for r in range(3):
                for b in range(4):
                    load(r, k, b).start()

    done = plan["pre"] + len(plan["mid"])

    def masks(i, _):
        @pl.when(i == plan["eb"])
        def _():
            forward_eb(last - 1)

        shared(i + done, lambda r: weigh(i, r))
        return 0
    lax.fori_loop(0, 4, masks, 0)

    def tail(i, _):
        @pl.when(i == plan["fetch"])
        def _():
            fetch(range(last - 1))

        @pl.when(i == plan["late"])
        def _():
            fetch([last - 1])

        for p, o in zip(plan["ebx"], ORDER, strict=True):
            pl.when(i == p)(functools.partial(forward_ebx, o))

        @pl.when(i == plan["sums"])
        def _():
            whole = wd.at[pl.ds(0, last)]
            pltpu.make_async_copy(whole, whole, ld_sem).wait()
            lax.fori_loop(0, 4, combine, 0)

        shared(i + done)
        return 0
    lax.fori_loop(4, units - done, tail, 0)
    down_copy(units - 1).wait()
    outs = [pltpu.make_async_copy(acc.at[:, span[r]], sum_hbm.at[:, span[r]], out_sem) for r in range(3)]
    for r in range(3):
        acc[:, span[r]] += dot(act[...], sd[(units - 1) % 2, :, span[r]])
        outs[r].start()
    arrived(eal, ea_recv)

    early, end = pl.ds(0, last), pl.ds(last, 1)
    left(met.at[:, others], m_send)
    left(eal.at[pl.ds(0, 2)], a_send)
    left(z.at[0, 0, others], b0_send.at[0])
    left(z.at[pl.ds(1, last), 0, others], b0_send.at[1])
    left(z.at[:, others, others], b_send)
    left(z.at[:, :, :, others], c_send)
    left(z.at[early, :, :, others], ec_send)
    left(z.at[end, :, :, others], ecx_send)
    left(z.at[early, :, others], eb_send)
    left(z.at[end, :, others], ebx_send)
    left(eal, ea_send)
    pltpu.make_async_copy(acc, sum_hbm, out_sem).wait()


def layer(x, expert, slot, gate, w_gate, w_up, w_down, s_gate, s_up, s_down, cfg):
    tokens, chunks, cols, ff, u_tile, top = (cfg[n] for n in ("tokens", "chunks", "cols", "ff", "u_tile", "top"))
    d, rows = sum(cols), N * N * N * SUB
    hbm = pl.BlockSpec(memory_space=pl.ANY)
    block = lambda w: jax.ShapeDtypeStruct((chunks, N, N, N, SUB, w), BF16)
    dma = pltpu.SemaphoreType.DMA
    outs = pl.pallas_call(
        functools.partial(kernel, cfg),
        out_shape=[jax.ShapeDtypeStruct((tokens, d), F32), jax.ShapeDtypeStruct((3, tokens, d), BF16)]
        + [block(w) for _ in range(4) for w in cols],
        in_specs=[hbm] * 10,
        out_specs=[hbm] * 14,
        scratch_shapes=[
            pltpu.VMEM((tokens, d), BF16),
            *[pltpu.VMEM((3, tokens, w), BF16) for w in cols],
            pltpu.VMEM((3, 4, 2 * top, tokens), F32),
            pltpu.VMEM((N, N, N, SUB, d), BF16),
            pltpu.VMEM((d, ff), BF16),
            pltpu.VMEM((d, ff), BF16),
            pltpu.VMEM((chunks, N, N, N, SUB, d), BF16),
            pltpu.VMEM((chunks, N, N, N, SUB, d), BF16),
            pltpu.VMEM((rows, ff), BF16),
            pltpu.VMEM((tokens, d), F32),
            pltpu.VMEM((3, d, u_tile), BF16),
            pltpu.VMEM((3, d, u_tile), BF16),
            pltpu.VMEM((2, u_tile, d), BF16),
            pltpu.VMEM((tokens, u_tile), BF16),
            pltpu.VMEM((top, tokens), jnp.int32),
            pltpu.VMEM((top, tokens), jnp.int32),
            pltpu.VMEM((top, tokens), F32),
            dma((2,)), dma((ff // cfg["f_tile"] + 1,)), dma((3, 3)), dma((2,)), dma(()),
            *[dma(())] * 6, *[dma((2,))] * 2,
            *[dma(()), dma((chunks,))] * 3,
            dma(()), dma((4,)), dma(()), dma((chunks,)), dma(()), dma((4,)),
            *[dma(())] * 3,
        ],
        compiler_params=pltpu.CompilerParams(collective_id=0, has_side_effects=True, vmem_limit_bytes=cfg["vmem"]),
        name="moe_layer",
    )(x, expert, slot, gate, w_gate, w_up, w_down.reshape(chunks, N, N, N, SUB, d), s_gate, s_up, s_down)
    total, sums = outs[:2]
    for o in range(3):
        total += sums[o].astype(F32)
    return total.astype(BF16)


PLAN = {
    "pre": 20, "relay": 3, "own": 5, "gather": (7, 9, 11, 13, 15), "forward": 13, "mid": (),
    "weights": (15, 19),
    "main": (((0, 0), "C", 1), ((0, 4), "C", 2), ((1, 2), "C", 3), ((2, 0), "C", 4),
             ((2, 1), "F", 0), ((3, 1), "F", 1), ((4, 1), "F", 2)),
    "eb": 0, "ebx": (4, 5, 6, 7), "fetch": 8, "late": 10, "sums": 12,
}


def configure(x, expert, w_gate, s_gate):
    tokens, d = x.shape[-2:]
    top, ff, width, experts = expert.shape[-1], w_gate.shape[-1], s_gate.shape[-1], N * N * N
    slots = 5 * tokens * top // (4 * experts)
    lanes = d // 128
    cols = tuple(128 * ((lanes + 2 - r) // 3) for r in range(3))
    return dict(tokens=tokens, top=top, slots=slots, chunks=slots // SUB, cols=cols, ff=ff, f_tile=512, down=(768, 512, 512),
                units=width // 512, u_tile=512, plan=PLAN, vmem=67043328)


def solution(mesh):
    def step(x, expert, slot, gate, w_gate, w_up, w_down, s_gate, s_up, s_down):
        cfg = configure(x, expert, w_gate, s_gate)
        y = layer(x[0, 0], expert[0, 0].T, slot[0, 0].T, gate[0, 0].T, w_gate[0], w_up[0], w_down[0], s_gate, s_up, s_down, cfg)
        return y[None, None]

    tok, own, whole = P("dp", "ep", None, None), P("ep", None, None), P(None, None)
    return jax.shard_map(step, mesh=mesh, in_specs=(tok,) * 4 + (own,) * 3 + (whole,) * 3, out_specs=tok, check_vma=False)
```
